8 devices in a mesh: dp: 2 (over z, y), tp: 4 (over x, core).
Axes of the slice: x: 2, y: 2, z: 1, core: 2. Of those that a mesh axis runs over, the one named last changes fastest.
Arguments:
- x_in: bfloat16 [256, 4096], P('dp'), parts along dimension 0
- tok_pos: int32 [256], P('dp'), parts along dimension 0
- self_k: bfloat16 [256, 64, 64, 64], P('dp', None, 'tp'), parts along dimension 0
- self_v: bfloat16 [256, 64, 64, 64], P('dp', None, 'tp'), parts along dimension 0
- cross_k: bfloat16 [256, 128, 64, 64], P('dp', None, 'tp'), parts along dimension 0
- cross_v: bfloat16 [256, 128, 64, 64], P('dp', None, 'tp'), parts along dimension 0
- enc_mask: int32 [256, 128], P('dp'), parts along dimension 0
- rel_bias: float32 [32, 64], P(None, 'tp')
- w_q: bfloat16 [4096, 4096], P(None, 'tp')
- w_k: bfloat16 [4096, 4096], P(None, 'tp')
- w_v: bfloat16 [4096, 4096], P(None, 'tp')
- w_o: bfloat16 [4096, 4096], P('tp')
- cross_q: bfloat16 [4096, 4096], P(None, 'tp')
- cross_o: bfloat16 [4096, 4096], P('tp')
- w_gate: bfloat16 [4096, 10240], P(None, 'tp')
- w_up: bfloat16 [4096, 10240], P(None, 'tp')
- w_down: bfloat16 [10240, 4096], P('tp')
- norm_self: bfloat16 [4096], replicated
- norm_cross: bfloat16 [4096], replicated
- norm_mlp: bfloat16 [4096], replicated
Outputs:
- output 1: bfloat16 [256, 4096], P('dp'), parts along dimension 0
- output 2: bfloat16 [256, 64, 64, 64], P('dp', None, 'tp'), parts along dimension 0
- output 3: bfloat16 [256, 64, 64, 64], P('dp', None, 'tp'), parts along dimension 0
There are 2 independent parts. The reference program is written for one: setup_inputs(seed, part) draws one part's arguments, and reference() takes and returns one part's arrays. A program takes and returns all parts, laid end to end along the dimension named above; an argument that names none is the same for every part.
All inputs are finite; a program needn't handle non-finite values.
Results may differ from the reference program's by a relative error of at most 0.0181668.
Values are sent between devices in bfloat16 or wider.
A program may use at most 1 GiB of HBM per device.

```python
import math
import jax
import jax.numpy as jnp
from jax import lax

BATCH_ROWS = 128
T_MAX = 64
SRC_LEN = 128
D_MODEL = 4096
N_HEADS = 64
D_HEAD = 64
D_FF = 10240

INNER_DIM = N_HEADS * D_HEAD
BUCKET_EDGES = tuple(int(math.ceil(16.0 * 8.0 ** (bucket_step / 16.0))) for bucket_step in range(1, 16))
NEG_FILL = -1e30


def draw_ends(rng_key, low_end, high_end):
    key_list = jax.random.split(rng_key, 3)
    drawn_vals = jax.random.randint(key_list[0], (BATCH_ROWS,), low_end, high_end + 1)
    high_row = jax.random.randint(key_list[1], (), 0, BATCH_ROWS)
    low_row = (high_row + jax.random.randint(key_list[2], (), 1, BATCH_ROWS)) % BATCH_ROWS
    return drawn_vals.at[high_row].set(high_end).at[low_row].set(low_end).astype(jnp.int32)


def normal_bf16(rng_key, array_shape, std_dev):
    return (std_dev * jax.random.normal(rng_key, array_shape, jnp.float32)).astype(jnp.bfloat16)


def setup_inputs(seed: int = 0, part: int = 0) -> dict:
    part_keys = jax.random.split(jax.random.fold_in(jax.random.key(seed), part), 8)
    shared_keys = jax.random.split(jax.random.key(seed + 1), 16)
    cache_shape = (BATCH_ROWS, T_MAX, N_HEADS, D_HEAD)
    cross_shape = (BATCH_ROWS, SRC_LEN, N_HEADS, D_HEAD)
    src_lens = draw_ends(part_keys[2], SRC_LEN // 4, SRC_LEN)
    bias_draw = 0.7 * jax.random.normal(shared_keys[0], (32, N_HEADS), jnp.float32)
    q_scale = (D_MODEL * D_HEAD) ** -0.5
    in_scale = D_MODEL ** -0.5
    out_scale = INNER_DIM ** -0.5
    return {
        'x_in': normal_bf16(part_keys[0], (BATCH_ROWS, D_MODEL), 1.0),
        'tok_pos': draw_ends(part_keys[1], T_MAX // 8, T_MAX - 1),
        'self_k': normal_bf16(part_keys[3], cache_shape, 1.0),
        'self_v': normal_bf16(part_keys[4], cache_shape, 1.0),
        'cross_k': normal_bf16(part_keys[5], cross_shape, 1.0),
        'cross_v': normal_bf16(part_keys[6], cross_shape, 1.0),
        'enc_mask': (jnp.arange(SRC_LEN)[None, :] < src_lens[:, None]).astype(jnp.int32),
        'rel_bias': bias_draw.at[0].add(0.5 * math.log(T_MAX) - 1.0),
        'w_q': normal_bf16(shared_keys[1], (D_MODEL, INNER_DIM), q_scale),
        'w_k': normal_bf16(shared_keys[2], (D_MODEL, INNER_DIM), in_scale),
        'w_v': normal_bf16(shared_keys[3], (D_MODEL, INNER_DIM), in_scale),
        'w_o': normal_bf16(shared_keys[4], (INNER_DIM, D_MODEL), 0.4 * math.sqrt(T_MAX) * out_scale),
        'cross_q': normal_bf16(shared_keys[5], (D_MODEL, INNER_DIM), q_scale),
        'cross_o': normal_bf16(shared_keys[6], (INNER_DIM, D_MODEL), 0.5 * math.sqrt(SRC_LEN) * out_scale),
        'w_gate': normal_bf16(shared_keys[7], (D_MODEL, D_FF), in_scale),
        'w_up': normal_bf16(shared_keys[8], (D_MODEL, D_FF), in_scale),
        'w_down': normal_bf16(shared_keys[9], (D_FF, D_MODEL), 1.5 * D_FF ** -0.5),
        'norm_self': (1.0 + 0.25 * jax.random.normal(shared_keys[10], (D_MODEL,), jnp.float32)).astype(jnp.bfloat16),
        'norm_cross': (1.0 + 0.25 * jax.random.normal(shared_keys[11], (D_MODEL,), jnp.float32)).astype(jnp.bfloat16),
        'norm_mlp': (1.0 + 0.25 * jax.random.normal(shared_keys[12], (D_MODEL,), jnp.float32)).astype(jnp.bfloat16),
    }


def rms_norm(values, norm_scale):
    inv_rms = lax.rsqrt(jnp.mean(values * values, axis=-1, keepdims=True) + 1e-6)
    return (values * inv_rms * norm_scale.astype(jnp.float32)).astype(jnp.bfloat16)


def project(normed, weight):
    return jnp.dot(normed, weight, preferred_element_type=jnp.float32).astype(jnp.bfloat16)


def rel_bucket(distance):
    bucket_edges = jnp.array(BUCKET_EDGES, dtype=jnp.int32)
    far_bucket = 16 + jnp.sum((distance[..., None] >= bucket_edges).astype(jnp.int32), axis=-1)
    return jnp.where(distance < 16, distance, far_bucket)


def attend(queries, keys_all, values_all, extra):
    def one_row(operands):
        row_q, row_k, row_v, row_extra = operands
        scores = jnp.einsum('hk,thk->ht', row_q.astype(jnp.float32), row_k.astype(jnp.float32)) + row_extra
        probs_bf = jax.nn.softmax(scores, axis=-1).astype(jnp.bfloat16)
        mixed_out = jnp.einsum('ht,thk->hk', probs_bf.astype(jnp.float32), row_v.astype(jnp.float32))
        return mixed_out.astype(jnp.bfloat16)
    return lax.map(one_row, (queries, keys_all, values_all, extra))


def reference(x_in, tok_pos, self_k, self_v, cross_k, cross_v, enc_mask, rel_bias, w_q, w_k, w_v, w_o, cross_q, cross_o, w_gate, w_up, w_down, norm_self, norm_cross, norm_mlp):
    row_count = x_in.shape[0]
    head_shape = (row_count, N_HEADS, D_HEAD)
    residual = x_in.astype(jnp.float32)
    normed = rms_norm(residual, norm_self)
    queries = project(normed, w_q).reshape(head_shape)
    new_keys = project(normed, w_k).reshape(head_shape)
    new_values = project(normed, w_v).reshape(head_shape)
    key_index = jnp.arange(T_MAX)
    at_pos = (key_index[None, :] == tok_pos[:, None])[:, :, None, None]
    new_self_k = jnp.where(at_pos, new_keys[:, None], self_k)
    new_self_v = jnp.where(at_pos, new_values[:, None], self_v)
    distance = jnp.maximum(tok_pos[:, None] - key_index[None, :], 0)
    bias_rows = jnp.swapaxes(jnp.take(rel_bias, rel_bucket(distance), axis=0), 1, 2)
    causal = (key_index[None, :] <= tok_pos[:, None])[:, None, :]
    self_extra = jnp.where(causal, bias_rows, NEG_FILL)
    mixed_self = attend(queries, new_self_k, new_self_v, self_extra)
    residual = residual + jnp.dot(mixed_self.reshape(row_count, INNER_DIM), w_o, preferred_element_type=jnp.float32)
    normed = rms_norm(residual, norm_cross)
    cross_queries = project(normed, cross_q).reshape(head_shape)
    cross_extra = jnp.where(enc_mask[:, None, :] != 0, 0.0, NEG_FILL)
    mixed_cross = attend(cross_queries, cross_k, cross_v, cross_extra)
    residual = residual + jnp.dot(mixed_cross.reshape(row_count, INNER_DIM), cross_o, preferred_element_type=jnp.float32)
    normed = rms_norm(residual, norm_mlp)
    gate_pre = jnp.dot(normed, w_gate, preferred_element_type=jnp.float32)
    up_pre = jnp.dot(normed, w_up, preferred_element_type=jnp.float32)
    hidden = (jax.nn.gelu(gate_pre, approximate=True) * up_pre).astype(jnp.bfloat16)
    residual = residual + jnp.dot(hidden, w_down, preferred_element_type=jnp.float32)
    return (residual.astype(jnp.bfloat16), new_self_k, new_self_v)
```

```python
import math
import jax
import jax.numpy as jnp
from jax import lax
from jax.experimental import pallas as pl
from jax.experimental.pallas import tpu as pltpu
from jax.sharding import PartitionSpec as P

BUCKET_EDGES = tuple(int(math.ceil(16.0 * 8.0 ** (bucket_step / 16.0))) for bucket_step in range(1, 16))
NEG_FILL = -1e30
F32 = jnp.float32
BF16 = jnp.bfloat16
ANY = pl.BlockSpec(memory_space=pl.ANY)
VMEM = pl.BlockSpec(memory_space=pltpu.VMEM)
COLS = 256
T_BLOCK = 8


def self_kernel(x_hbm, norm_ref, pos_ref, rel_ref, wq_hbm, wk_hbm, wv_hbm, wo_hbm, k_hbm, v_hbm,
                part_hbm, newk_hbm, newv_hbm,
                xbuf, hbuf, wbuf, kvbuf, q_ref, kn_ref, hit_ref, score_ref, acc_ref,
                x_sem, w_sem, kv_sem, out_sem, part_sem, window):
    rows, d_model = xbuf.shape
    n_w = wbuf.shape[0]
    per_mat = n_w // 3
    n_chunk = kvbuf.shape[0] // 2
    n_head, t_len = score_ref.shape[0], score_ref.shape[1]
    inner = acc_ref.shape[0]
    d_head = inner // n_head
    chunk_rows = kvbuf.shape[1]
    sub = d_head // 16
    wo_per_slot = wbuf.shape[1] // inner
    n_wo = wo_hbm.shape[1] // COLS // wo_per_slot

    def w_copy(c):
        src = (wq_hbm, wk_hbm, wv_hbm)[c // per_mat]
        return pltpu.make_async_copy(src.at[:, pl.ds((c % per_mat) * COLS, COLS)], wbuf.at[c], w_sem.at[c])

    def kv_copy(i):
        src = k_hbm if i < n_chunk else v_hbm
        return pltpu.make_async_copy(src.at[pl.ds((i % n_chunk) * chunk_rows, chunk_rows)], kvbuf.at[i], kv_sem.at[i])

    def wo_copies(i):
        return [pltpu.make_async_copy(wo_hbm.at[:, pl.ds((i * wo_per_slot + r) * COLS, COLS)],
                                      wbuf.at[i, pl.ds(r * inner, inner)], w_sem.at[i]) for r in range(wo_per_slot)]

    loads = [[w_copy(c)] for c in range(n_w)] + [[kv_copy(i)] for i in range(2 * n_chunk)] + [wo_copies(i) for i in range(n_wo)]
    issued = [0]

    def issue(upto):
        while issued[0] < min(upto, len(loads)):
            for copy in loads[issued[0]]:
                copy.start()
            issued[0] += 1

    x_copy = pltpu.make_async_copy(x_hbm, xbuf, x_sem)
    x_copy.start()
    issue(window)

    pos = pos_ref[...]
    pos16 = jnp.broadcast_to(pos, (16, rows))

    def set_hit(t, carry):
        hit_ref[t] = jnp.where(pos16 == t, 1.0, 0.0).astype(BF16)
        return carry
    lax.fori_loop(0, t_len, set_hit, 0)

    lane = lax.broadcasted_iota(jnp.int32, (n_head, 128), 1)
    bucket = jnp.full((n_head, 128), 16, jnp.int32)
    for edge in BUCKET_EDGES:
        bucket = bucket + (lane >= edge).astype(jnp.int32)
    bucket = jnp.where(lane < 16, lane, bucket)
    rel = rel_ref[...]
    table = jnp.zeros((n_head, 128), F32)
    for b in range(rel.shape[1]):
        table = jnp.where(bucket == b, rel[:, b:b + 1], table)
    acc_ref[0:n_head, :] = table

    x_copy.wait()
    block = 16
    norm = norm_ref[0:1, :]

    def norm_rows(i, carry):
        at = pl.ds(pl.multiple_of(i * block, block), block)
        r = xbuf[at, :].astype(F32)
        inv = lax.rsqrt(jnp.mean(r * r, axis=-1, keepdims=True) + 1e-6)
        hbuf[at, :] = (r * inv * norm).astype(BF16)
        return carry
    lax.fori_loop(0, rows // block, norm_rows, 0)

    for c in range(n_w):
        w_copy(c).wait()
        issue(c + 1 + window)
        y = jnp.dot(hbuf[...], wbuf[c], preferred_element_type=F32).astype(BF16).astype(F32).T
        at = (c % per_mat) * COLS
        if c < per_mat:
            q_ref[at:at + COLS, :] = y
        else:
            kn_ref[c // per_mat - 1, at:at + COLS, :] = y.astype(BF16)

    def chunk_out(i):
        dst = newk_hbm if i < n_chunk else newv_hbm
        return pltpu.make_async_copy(kvbuf.at[i], dst.at[pl.ds((i % n_chunk) * chunk_rows, chunk_rows)], out_sem.at[i])

    for j in range(n_chunk):
        kv_copy(j).wait()
        issue(n_w + j + 1 + window)

        def k_head(h, carry):
            at = pl.multiple_of(h * d_head, d_head)
            q = q_ref[pl.ds(at, d_head), :]
            kn = kn_ref[0, pl.ds(at, d_head), :].reshape(sub, 16, rows)
            rows_out = []
            for tt in range(T_BLOCK):
                here = pl.ds(pl.multiple_of(tt * inner + at, d_head), d_head)
                old = kvbuf[j, here, :].reshape(sub, 16, rows)
                hit = hit_ref[j * T_BLOCK + tt] != 0
                new = jnp.where(hit[None], kn, old)
                kvbuf[j, here, :] = new.reshape(d_head, rows)
                prod = new.reshape(d_head, rows).astype(F32) * q
                rows_out.append(jnp.sum(prod, axis=0, keepdims=True))
            score_ref[h, j * T_BLOCK:(j + 1) * T_BLOCK, :] = jnp.concatenate(rows_out, axis=0)
            return carry
        lax.fori_loop(0, n_head, k_head, 0)
        chunk_out(j).start()

    t_iota = lax.broadcasted_iota(jnp.int32, (t_len, rows), 0)
    causal = t_iota <= pos
    back = jnp.maximum(pos - t_iota, 0)

    def soft_head(h, carry):
        line = jnp.broadcast_to(acc_ref[pl.ds(h, 1), :], (t_len, 128))
        s = score_ref[h] + jnp.take_along_axis(line, back, axis=1)
        s = jnp.where(causal, s, NEG_FILL)
        e = jnp.exp(s - jnp.max(s, axis=0, keepdims=True))
        p = e / jnp.sum(e, axis=0, keepdims=True)
        score_ref[h] = p.astype(BF16).astype(F32)
        return carry
    lax.fori_loop(0, n_head, soft_head, 0)

    acc_ref[...] = jnp.zeros_like(acc_ref)
    for j in range(n_chunk):
        kv_copy(n_chunk + j).wait()
        issue(n_w + n_chunk + j + 1 + window)

        def v_head(h, carry):
            at = pl.multiple_of(h * d_head, d_head)
            vn = kn_ref[1, pl.ds(at, d_head), :].reshape(sub, 16, rows)
            p = score_ref[h, j * T_BLOCK:(j + 1) * T_BLOCK, :]
            acc = acc_ref[pl.ds(at, d_head), :]
            for tt in range(T_BLOCK):
                here = pl.ds(pl.multiple_of(tt * inner + at, d_head), d_head)
                old = kvbuf[n_chunk + j, here, :].reshape(sub, 16, rows)
                hit = hit_ref[j * T_BLOCK + tt] != 0
                new = jnp.where(hit[None], vn, old)
                kvbuf[n_chunk + j, here, :] = new.reshape(d_head, rows)
                acc = acc + new.reshape(d_head, rows).astype(F32) * p[tt:tt + 1, :]
            acc_ref[pl.ds(at, d_head), :] = acc
            return carry
        lax.fori_loop(0, n_head, v_head, 0)
        chunk_out(n_chunk + j).start()

    issue(len(loads))
    hbuf[:, 0:inner] = acc_ref[...].T.astype(BF16)
    width = wo_per_slot * COLS
    part_copies = []
    for i in range(n_wo):
        for copy in wo_copies(i):
            copy.wait()
        for r in range(wo_per_slot):
            at = (i * wo_per_slot + r) * COLS
            y = jnp.dot(hbuf[:, 0:inner], wbuf[i, r * inner:(r + 1) * inner, :], preferred_element_type=F32)
            xbuf[:, at:at + COLS] = y.astype(BF16)
        copy = pltpu.make_async_copy(xbuf.at[:, pl.ds(i * width, width)], part_hbm.at[:, pl.ds(i * width, width)], part_sem.at[i])
        copy.start()
        part_copies.append(copy)
    for i in range(2 * n_chunk):
        chunk_out(i).wait()
    for copy in part_copies:
        copy.wait()


def self_attention(x_in, norms, tok_pos, rel_bias, w_q, w_k, w_v, w_o, self_k, self_v):
    rows, t_len, n_head, d_head = self_k.shape
    d_model = x_in.shape[1]
    inner = n_head * d_head
    flat = (t_len * inner, rows)
    k_flat = self_k.transpose(1, 2, 3, 0).reshape(flat)
    v_flat = self_v.transpose(1, 2, 3, 0).reshape(flat)
    n_w = 3 * (inner // COLS)
    n_chunk = t_len // T_BLOCK
    n_wo = w_o.shape[1] // COLS // (d_model // inner)

    def body(*refs):
        self_kernel(*refs, window=6)

    part, new_k, new_v = pl.pallas_call(
        body,
        out_shape=(jax.ShapeDtypeStruct((rows, w_o.shape[1]), BF16),
                   jax.ShapeDtypeStruct(flat, BF16), jax.ShapeDtypeStruct(flat, BF16)),
        in_specs=[ANY, VMEM, VMEM, VMEM] + [ANY] * 6,
        out_specs=(ANY, ANY, ANY),
        scratch_shapes=[
            pltpu.VMEM((rows, d_model), BF16),
            pltpu.VMEM((rows, d_model), BF16),
            pltpu.VMEM((n_w, d_model, COLS), BF16),
            pltpu.VMEM((2 * n_chunk, T_BLOCK * inner, rows), BF16),
            pltpu.VMEM((inner, rows), F32),
            pltpu.VMEM((2, inner, rows), BF16),
            pltpu.VMEM((t_len, 16, rows), BF16),
            pltpu.VMEM((n_head, t_len, rows), F32),
            pltpu.VMEM((inner, rows), F32),
            pltpu.SemaphoreType.DMA,
            pltpu.SemaphoreType.DMA((n_w,)),
            pltpu.SemaphoreType.DMA((2 * n_chunk,)),
            pltpu.SemaphoreType.DMA((2 * n_chunk,)),
            pltpu.SemaphoreType.DMA((n_wo,)),
        ],
        compiler_params=pltpu.CompilerParams(vmem_limit_bytes=66_900_000),
        cost_estimate=pl.CostEstimate(flops=4_400_000_000, bytes_accessed=104_000_000, transcendentals=131_072),
        name="self_part",
    )(x_in, norms, tok_pos.reshape(1, rows), rel_bias.T, w_q, w_k, w_v, w_o, k_flat, v_flat)

    def unflat(cache):
        return cache.reshape(t_len, n_head, d_head, rows).transpose(3, 0, 1, 2)
    return part, unflat(new_k), unflat(new_v)


def rms_norm(values, norm_scale):
    inv_rms = lax.rsqrt(jnp.mean(values * values, axis=-1, keepdims=True) + 1e-6)
    return (values * inv_rms * norm_scale.astype(jnp.float32)).astype(jnp.bfloat16)


def project(normed, weight):
    return jnp.dot(normed, weight, preferred_element_type=jnp.float32).astype(jnp.bfloat16)


def attend(queries, keys_all, values_all, extra):
    scores = jnp.einsum('bhk,bthk->bht', queries, keys_all, preferred_element_type=jnp.float32) + extra
    probs_bf = jax.nn.softmax(scores, axis=-1).astype(jnp.bfloat16)
    mixed_out = jnp.einsum('bht,bthk->bhk', probs_bf, values_all, preferred_element_type=jnp.float32)
    return mixed_out.astype(jnp.bfloat16)


def solution(mesh):
    def tp_sum(partial_out):
        return lax.psum(partial_out.astype(jnp.bfloat16), 'tp').astype(jnp.float32)

    def local_layer(x_in, tok_pos, self_k, self_v, cross_k, cross_v, enc_mask, rel_bias, w_q, w_k, w_v, w_o, cross_q, cross_o, w_gate, w_up, w_down, norm_self, norm_cross, norm_mlp):
        row_count, t_len, head_count, head_dim = self_k.shape
        head_shape = (row_count, head_count, head_dim)
        flat_dim = head_count * head_dim
        norms = jnp.stack([norm_self, norm_cross, norm_mlp]).astype(F32)
        part, new_self_k, new_self_v = self_attention(x_in, norms, tok_pos, rel_bias, w_q, w_k, w_v, w_o, self_k, self_v)
        residual = x_in.astype(jnp.float32) + tp_sum(part)
        normed = rms_norm(residual, norm_cross)
        cross_queries = project(normed, cross_q).reshape(head_shape)
        cross_extra = jnp.where(enc_mask[:, None, :] != 0, 0.0, NEG_FILL)
        mixed_cross = attend(cross_queries, cross_k, cross_v, cross_extra)
        residual = residual + tp_sum(jnp.dot(mixed_cross.reshape(row_count, flat_dim), cross_o, preferred_element_type=jnp.float32))
        normed = rms_norm(residual, norm_mlp)
        gate_pre = jnp.dot(normed, w_gate, preferred_element_type=jnp.float32)
        up_pre = jnp.dot(normed, w_up, preferred_element_type=jnp.float32)
        hidden = (jax.nn.gelu(gate_pre, approximate=True) * up_pre).astype(jnp.bfloat16)
        residual = residual + tp_sum(jnp.dot(hidden, w_down, preferred_element_type=jnp.float32))
        return residual.astype(jnp.bfloat16), new_self_k, new_self_v

    cache_spec = P('dp', None, 'tp', None)
    split_cols = P(None, 'tp')
    split_rows = P('tp', None)
    in_specs = (P('dp', None), P('dp'), cache_spec, cache_spec, cache_spec, cache_spec, P('dp', None), split_cols, split_cols, split_cols, split_cols, split_rows, split_cols, split_rows, split_cols, split_cols, split_rows, P(None), P(None), P(None))
    out_specs = (P('dp', None), cache_spec, cache_spec)
    return jax.shard_map(local_layer, mesh=mesh, in_specs=in_specs, out_specs=out_specs, check_vma=False)
```

```python
import functools
import math
import jax
import jax.numpy as jnp
from jax import lax
from jax.experimental import pallas as pl
from jax.experimental.pallas import tpu as pltpu
from jax.sharding import PartitionSpec as P

BUCKET_EDGES = tuple(int(math.ceil(16.0 * 8.0 ** (bucket_step / 16.0))) for bucket_step in range(1, 16))
NEG_FILL = -1e30
F32 = jnp.float32
BF16 = jnp.bfloat16
ANY = pl.BlockSpec(memory_space=pl.ANY)
VMEM = pl.BlockSpec(memory_space=pltpu.VMEM)
COLS = 256
T_BLOCK = 8


def self_kernel(x_hbm, norm_ref, pos_ref, rel_ref, wq_hbm, wk_hbm, wv_hbm, wo_hbm, k_hbm, v_hbm,
                part_hbm, newk_hbm, newv_hbm,
                xbuf, hbuf, wbuf, kvbuf, q_ref, kn_ref, hit_ref, score_ref, acc_ref,
                x_sem, w_sem, kv_sem, out_sem, part_sem, window):
    rows, d_model = xbuf.shape
    n_w = wbuf.shape[0]
    per_mat = n_w // 3
    n_chunk = kvbuf.shape[0] // 2
    n_head, t_len = score_ref.shape[0], score_ref.shape[1]
    inner = acc_ref.shape[0]
    d_head = inner // n_head
    chunk_rows = kvbuf.shape[1]
    sub = d_head // 16
    wo_per_slot = wbuf.shape[1] // inner
    n_wo = wo_hbm.shape[1] // COLS // wo_per_slot

    def w_copy(c):
        src = (wq_hbm, wk_hbm, wv_hbm)[c // per_mat]
        return pltpu.make_async_copy(src.at[:, pl.ds((c % per_mat) * COLS, COLS)], wbuf.at[c], w_sem.at[c])

    def kv_copy(i):
        src = k_hbm if i < n_chunk else v_hbm
        return pltpu.make_async_copy(src.at[pl.ds((i % n_chunk) * chunk_rows, chunk_rows)], kvbuf.at[i], kv_sem.at[i])

    def wo_copies(i):
        return [pltpu.make_async_copy(wo_hbm.at[:, pl.ds((i * wo_per_slot + r) * COLS, COLS)],
                                      wbuf.at[i, pl.ds(r * inner, inner)], w_sem.at[i]) for r in range(wo_per_slot)]

    loads = [[w_copy(c)] for c in range(n_w)] + [[kv_copy(i)] for i in range(2 * n_chunk)] + [wo_copies(i) for i in range(n_wo)]
    issued = [0]

    def issue(upto):
        while issued[0] < min(upto, len(loads)):
            for copy in loads[issued[0]]:
                copy.start()
            issued[0] += 1

    x_copy = pltpu.make_async_copy(x_hbm, xbuf, x_sem)
    x_copy.start()
    issue(window)

    pos = pos_ref[...]
    pos16 = jnp.broadcast_to(pos, (16, rows))

    def set_hit(t, carry):
        hit_ref[t] = jnp.where(pos16 == t, 1.0, 0.0).astype(BF16)
        return carry
    lax.fori_loop(0, t_len, set_hit, 0)

    lane = lax.broadcasted_iota(jnp.int32, (n_head, 128), 1)
    bucket = jnp.full((n_head, 128), 16, jnp.int32)
    for edge in BUCKET_EDGES:
        bucket = bucket + (lane >= edge).astype(jnp.int32)
    bucket = jnp.where(lane < 16, lane, bucket)
    rel = rel_ref[...]
    table = jnp.zeros((n_head, 128), F32)
    for b in range(rel.shape[1]):
        table = jnp.where(bucket == b, rel[:, b:b + 1], table)
    acc_ref[0:n_head, :] = table

    x_copy.wait()
    block = 16
    norm = norm_ref[0:1, :]

    def norm_rows(i, carry):
        at = pl.ds(pl.multiple_of(i * block, block), block)
        r = xbuf[at, :].astype(F32)
        inv = lax.rsqrt(jnp.mean(r * r, axis=-1, keepdims=True) + 1e-6)
        hbuf[at, :] = (r * inv * norm).astype(BF16)
        return carry
    lax.fori_loop(0, rows // block, norm_rows, 0)

    for c in range(n_w):
        w_copy(c).wait()
        issue(c + 1 + window)
        y = jnp.dot(hbuf[...], wbuf[c], preferred_element_type=F32).astype(BF16).astype(F32).T
        at = (c % per_mat) * COLS
        if c < per_mat:
            q_ref[at:at + COLS, :] = y
        else:
            kn_ref[c // per_mat - 1, at:at + COLS, :] = y.astype(BF16)

    def chunk_out(i):
        dst = newk_hbm if i < n_chunk else newv_hbm
        return pltpu.make_async_copy(kvbuf.at[i], dst.at[pl.ds((i % n_chunk) * chunk_rows, chunk_rows)], out_sem.at[i])

    for j in range(n_chunk):
        kv_copy(j).wait()
        issue(n_w + j + 1 + window)

        def k_head(h, carry):
            at = pl.multiple_of(h * d_head, d_head)
            q = q_ref[pl.ds(at, d_head), :]
            kn = kn_ref[0, pl.ds(at, d_head), :].reshape(sub, 16, rows)
            rows_out = []
            for tt in range(T_BLOCK):
                here = pl.ds(pl.multiple_of(tt * inner + at, d_head), d_head)
                old = kvbuf[j, here, :].reshape(sub, 16, rows)
                hit = hit_ref[j * T_BLOCK + tt] != 0
                new = jnp.where(hit[None], kn, old)
                kvbuf[j, here, :] = new.reshape(d_head, rows)
                prod = new.reshape(d_head, rows).astype(F32) * q
                rows_out.append(jnp.sum(prod, axis=0, keepdims=True))
            score_ref[h, j * T_BLOCK:(j + 1) * T_BLOCK, :] = jnp.concatenate(rows_out, axis=0)
            return carry
        lax.fori_loop(0, n_head, k_head, 0)
        chunk_out(j).start()

    t_iota = lax.broadcasted_iota(jnp.int32, (t_len, rows), 0)
    causal = t_iota <= pos
    back = jnp.maximum(pos - t_iota, 0)

    def soft_head(h, carry):
        line = jnp.broadcast_to(acc_ref[pl.ds(h, 1), :], (t_len, 128))
        s = score_ref[h] + jnp.take_along_axis(line, back, axis=1)
        s = jnp.where(causal, s, NEG_FILL)
        e = jnp.exp(s - jnp.max(s, axis=0, keepdims=True))
        p = e / jnp.sum(e, axis=0, keepdims=True)
        score_ref[h] = p.astype(BF16).astype(F32)
        return carry
    lax.fori_loop(0, n_head, soft_head, 0)

    acc_ref[...] = jnp.zeros_like(acc_ref)
    for j in range(n_chunk):
        kv_copy(n_chunk + j).wait()
        issue(n_w + n_chunk + j + 1 + window)

        def v_head(h, carry):
            at = pl.multiple_of(h * d_head, d_head)
            vn = kn_ref[1, pl.ds(at, d_head), :].reshape(sub, 16, rows)
            p = score_ref[h, j * T_BLOCK:(j + 1) * T_BLOCK, :]
            acc = acc_ref[pl.ds(at, d_head), :]
            for tt in range(T_BLOCK):
                here = pl.ds(pl.multiple_of(tt * inner + at, d_head), d_head)
                old = kvbuf[n_chunk + j, here, :].reshape(sub, 16, rows)
                hit = hit_ref[j * T_BLOCK + tt] != 0
                new = jnp.where(hit[None], vn, old)
                kvbuf[n_chunk + j, here, :] = new.reshape(d_head, rows)
                acc = acc + new.reshape(d_head, rows).astype(F32) * p[tt:tt + 1, :]
            acc_ref[pl.ds(at, d_head), :] = acc
            return carry
        lax.fori_loop(0, n_head, v_head, 0)
        chunk_out(n_chunk + j).start()

    issue(len(loads))
    hbuf[:, 0:inner] = acc_ref[...].T.astype(BF16)
    width = wo_per_slot * COLS
    part_copies = []
    for i in range(n_wo):
        for copy in wo_copies(i):
            copy.wait()
        for r in range(wo_per_slot):
            at = (i * wo_per_slot + r) * COLS
            y = jnp.dot(hbuf[:, 0:inner], wbuf[i, r * inner:(r + 1) * inner, :], preferred_element_type=F32)
            xbuf[:, at:at + COLS] = y.astype(BF16)
        copy = pltpu.make_async_copy(xbuf.at[:, pl.ds(i * width, width)], part_hbm.at[:, pl.ds(i * width, width)], part_sem.at[i])
        copy.start()
        part_copies.append(copy)
    for i in range(2 * n_chunk):
        chunk_out(i).wait()
    for copy in part_copies:
        copy.wait()


def self_attention(x_in, norms, tok_pos, rel_bias, w_q, w_k, w_v, w_o, self_k, self_v):
    rows, t_len, n_head, d_head = self_k.shape
    d_model = x_in.shape[1]
    inner = n_head * d_head
    flat = (t_len * inner, rows)
    k_flat = self_k.transpose(1, 2, 3, 0).reshape(flat)
    v_flat = self_v.transpose(1, 2, 3, 0).reshape(flat)
    n_w = 3 * (inner // COLS)
    n_chunk = t_len // T_BLOCK
    n_wo = w_o.shape[1] // COLS // (d_model // inner)

    def body(*refs):
        self_kernel(*refs, window=6)

    part, new_k, new_v = pl.pallas_call(
        body,
        out_shape=(jax.ShapeDtypeStruct((rows, w_o.shape[1]), BF16),
                   jax.ShapeDtypeStruct(flat, BF16), jax.ShapeDtypeStruct(flat, BF16)),
        in_specs=[ANY, VMEM, VMEM, VMEM] + [ANY] * 6,
        out_specs=(ANY, ANY, ANY),
        scratch_shapes=[
            pltpu.VMEM((rows, d_model), BF16),
            pltpu.VMEM((rows, d_model), BF16),
            pltpu.VMEM((n_w, d_model, COLS), BF16),
            pltpu.VMEM((2 * n_chunk, T_BLOCK * inner, rows), BF16),
            pltpu.VMEM((inner, rows), F32),
            pltpu.VMEM((2, inner, rows), BF16),
            pltpu.VMEM((t_len, 16, rows), BF16),
            pltpu.VMEM((n_head, t_len, rows), F32),
            pltpu.VMEM((inner, rows), F32),
            pltpu.SemaphoreType.DMA,
            pltpu.SemaphoreType.DMA((n_w,)),
            pltpu.SemaphoreType.DMA((2 * n_chunk,)),
            pltpu.SemaphoreType.DMA((2 * n_chunk,)),
            pltpu.SemaphoreType.DMA((n_wo,)),
        ],
        compiler_params=pltpu.CompilerParams(vmem_limit_bytes=66_900_000),
        cost_estimate=pl.CostEstimate(flops=4_400_000_000, bytes_accessed=104_000_000, transcendentals=131_072),
        name="self_part",
    )(x_in, norms, tok_pos.reshape(1, rows), rel_bias.T, w_q, w_k, w_v, w_o, k_flat, v_flat)

    def unflat(cache):
        return cache.reshape(t_len, n_head, d_head, rows).transpose(3, 0, 1, 2)
    return part, unflat(new_k), unflat(new_v)


SLOTS = 52
GROUP = 8
AR_CHUNKS = 4
LANES = 128


def cross_kernel(n_head, x_hbm, part_hbm, norm_ref, mask_ref, cq_hbm, ck_hbm, cv_hbm, co_hbm, wg_hbm, wu_hbm, wd_hbm,
                 out_hbm,
                 ring, pbuf, hbuf, res, xhalf, rx1, tx2, rx2, q_ref, mix_ref, mixbf, act,
                 ring_sem, load_sem, s1_send, s1_recv, s2_send, s2_recv, s3_send, s3_recv, out_sem):
    rows, d_model = hbuf.shape
    half = rows // 2
    depth = ring.shape[1]
    inner = q_ref.shape[1]
    d_ff = act.shape[1]
    width = d_model // AR_CHUNKS

    me = lax.axis_index("tp")
    core = lax.rem(me, 2)
    chip = me // 2
    partner = {"tp": chip * 2 + (1 - core)}
    across = {"tp": (1 - chip) * 2 + core}
    mine = pl.ds(pl.multiple_of(core * half, half), half)
    theirs = pl.ds(pl.multiple_of((1 - core) * half, half), half)
    MESH = pl.DeviceIdType.MESH

    n_q = cq_hbm.shape[1] // LANES
    per_step = GROUP * inner // depth
    n_step = rows // GROUP
    first_kv = n_q
    first_o = first_kv + 2 * per_step * n_step
    o_blocks = depth // inner
    n_o = co_hbm.shape[1] // LANES // o_blocks
    first_gu = first_o + n_o
    n_gu = d_ff // LANES
    first_d = first_gu + 2 * n_gu
    n_d = d_model // LANES
    total = first_d + n_d

    def slot_of(j):
        return j % SLOTS if isinstance(j, int) else lax.rem(j, SLOTS)

    def start(src, j, used=None):
        dst = ring.at[slot_of(j)] if used is None else ring.at[slot_of(j), used]
        pltpu.make_async_copy(src, dst, ring_sem.at[slot_of(j)]).start()

    def cols(ref, i):
        at = i * LANES
        return ref.at[:, pl.ds(at if isinstance(at, int) else pl.multiple_of(at, LANES), LANES)]

    def issue_q(j):
        start(cols(cq_hbm, j), j)

    def issue_kv(j):
        n = j - first_kv
        step, piece = n // (2 * per_step), n % (2 * per_step)
        if isinstance(j, int):
            src = ck_hbm if piece < per_step else cv_hbm
            start(src.at[pl.ds((step * per_step + piece % per_step) * depth, depth)], j)

    def issue_step(step, j0):
        for piece in range(2 * per_step):
            src = ck_hbm if piece < per_step else cv_hbm
            at = (step * per_step + piece % per_step) * depth
            start(src.at[pl.ds(pl.multiple_of(at, depth), depth)], j0 + piece)

    def issue_o(j):
        n = j - first_o
        for r in range(o_blocks):
            start(cols(co_hbm, n * o_blocks + r), j, pl.ds(r * inner, inner))

    def issue_gu(pair, j0):
        start(cols(wg_hbm, pair), j0)
        start(cols(wu_hbm, pair), j0 + 1)

    def issue_d(j):
        start(cols(wd_hbm, j - first_d), j, pl.ds(0, d_ff))

    def issue(j):
        if j >= total:
            return
        if j < first_kv:
            issue_q(j)
        elif j < first_o:
            issue_kv(j)
        elif j < first_gu:
            issue_o(j)
        elif j < first_d:
            n = j - first_gu
            start(cols(wu_hbm if n % 2 else wg_hbm, n // 2), j)
        else:
            issue_d(j)

    def landed(j, used=None):
        dst = ring.at[slot_of(j)] if used is None else ring.at[slot_of(j), pl.ds(0, used)]
        src = ck_hbm.at[pl.ds(0, depth if used is None else used)]
        pltpu.make_async_copy(src, dst, ring_sem.at[slot_of(j)]).wait()

    def part_load(j):
        at = pl.ds(j * width, width)
        return pltpu.make_async_copy(part_hbm.at[:, at], pbuf.at[:, at], load_sem.at[j])
    x_load = pltpu.make_async_copy(x_hbm.at[mine], xhalf, load_sem.at[AR_CHUNKS])
    for j in range(AR_CHUNKS):
        part_load(j).start()
    x_load.start()

    barrier = pltpu.get_barrier_semaphore()
    for other in (partner, across):
        pl.semaphore_signal(barrier, inc=1, device_id=other, device_id_type=MESH)
    pl.semaphore_wait(barrier, 2)

    def to_partner(a, j):
        at = pl.ds(j * width, width)
        return pltpu.make_async_remote_copy(
            src_ref=pbuf.at[theirs, at], dst_ref=rx1.at[a % 2, :, at], send_sem=s1_send.at[a % 2, j],
            recv_sem=s1_recv.at[a % 2, j], device_id=partner, device_id_type=MESH)

    def to_across(a, j):
        at = pl.ds(j * width, width)
        return pltpu.make_async_remote_copy(
            src_ref=tx2.at[a % 2, :, at], dst_ref=rx2.at[a % 2, :, at], send_sem=s2_send.at[a % 2, j],
            recv_sem=s2_recv.at[a % 2, j], device_id=across, device_id_type=MESH)

    def blocks(fn, n=half // 16):
        def body(i, carry):
            fn(pl.multiple_of(i * 16, 16))
            return carry
        lax.fori_loop(0, n, body, 0)

    def chip_sum(a, j):
        at = pl.ds(j * width, width)
        to_partner(a, j).wait_recv()

        def add(r):
            own = pbuf[pl.ds(pl.multiple_of(core * half + r, 16), 16), at].astype(F32)
            tx2[a % 2, pl.ds(r, 16), at] = (own + rx1[a % 2, pl.ds(r, 16), at].astype(F32)).astype(BF16)
        blocks(add)
        to_across(a, j).start()

    def full_sum(a, j):
        at = pl.ds(j * width, width)
        to_across(a, j).wait_recv()

        def add(r):
            both = tx2[a % 2, pl.ds(r, 16), at].astype(F32) + rx2[a % 2, pl.ds(r, 16), at].astype(F32)
            res[pl.ds(r, 16), at] = res[pl.ds(r, 16), at] + both
        blocks(add)

    def sent(a):
        for j in range(AR_CHUNKS):
            to_partner(a, j).wait_send()
            to_across(a, j).wait_send()

    def rows_back(a, i):
        at = pl.ds(pl.multiple_of(core * half + i * 16, 16), 16)
        return pltpu.make_async_remote_copy(
            src_ref=hbuf.at[at], dst_ref=hbuf.at[at], send_sem=s3_send.at[a % 2, i],
            recv_sem=s3_recv.at[a % 2, i], device_id=partner, device_id_type=MESH)

    def normalise(a):
        norm = norm_ref[a + 1:a + 2, :]
        for i in range(half // 16):
            r = res[i * 16:(i + 1) * 16, :]
            inv = lax.rsqrt(jnp.mean(r * r, axis=-1, keepdims=True) + 1e-6)
            hbuf[pl.ds(pl.multiple_of(core * half + i * 16, 16), 16), :] = (r * inv * norm).astype(BF16)
            rows_back(a, i).start()
        for i in range(half // 16):
            rows_back(a, i).wait()

    for j in range(AR_CHUNKS):
        part_load(j).wait()
        to_partner(0, j).start()
    for j in range(SLOTS):
        issue(j)
    x_load.wait()
    blocks(lambda r: res.__setitem__((pl.ds(r, 16), slice(None)), xhalf[pl.ds(r, 16), :].astype(F32)))
    for j in range(AR_CHUNKS):
        chip_sum(0, j)
    for j in range(AR_CHUNKS):
        full_sum(0, j)
    normalise(0)

    def pair(j0, used=None):
        a, b = ring.at[slot_of(j0)], ring.at[slot_of(j0 + 1)]
        if used is None:
            return jnp.concatenate([a[...], b[...]], axis=1)
        return jnp.concatenate([a[0:used, :], b[0:used, :]], axis=1)

    for i in range(n_q // 2):
        landed(2 * i)
        landed(2 * i + 1)
        y = jnp.dot(hbuf[...], pair(2 * i), preferred_element_type=F32)
        q_ref[:, 2 * i * LANES:(2 * i + 2) * LANES] = y.astype(BF16).astype(F32)
        issue(2 * i + SLOTS)
        issue(2 * i + 1 + SLOTS)

    own_head = (lax.broadcasted_iota(jnp.int32, (n_head, inner), 1) // (inner // n_head)
                == lax.broadcasted_iota(jnp.int32, (n_head, inner), 0))
    in_slot = GROUP // per_step

    def attend_step(g, carry):
        j0 = first_kv + 2 * per_step * g
        at = pl.ds(pl.multiple_of(g * GROUP, GROUP), GROUP)
        q8 = q_ref[at, :]
        m8 = mask_ref[at, :]

        def spread(r):
            return jnp.where(own_head, jnp.broadcast_to(q8[r:r + 1, :], (n_head, inner)), 0.0).astype(BF16)
        landed(j0)
        landed(j0 + 1)
        scores = [None] * GROUP
        for r in range(in_slot):
            here = slice(r * inner, (r + 1) * inner)
            keys = jnp.concatenate([ring.at[slot_of(j0)][here, :], ring.at[slot_of(j0 + 1)][here, :]], axis=1)
            s = jnp.dot(jnp.concatenate([spread(r), spread(r + in_slot)], axis=0), keys, preferred_element_type=F32)
            scores[r] = jnp.where(m8[r:r + 1, :] != 0, s[0:n_head, 0:LANES], NEG_FILL)
            scores[r + in_slot] = jnp.where(m8[r + in_slot:r + in_slot + 1, :] != 0, s[n_head:, LANES:], NEG_FILL)
        s = jnp.concatenate(scores, axis=0)
        e = jnp.exp(s - jnp.max(s, axis=1, keepdims=True))
        p = (e / jnp.sum(e, axis=1, keepdims=True)).astype(BF16)
        landed(j0 + 2)
        landed(j0 + 3)
        none = jnp.zeros((n_head, LANES), BF16)
        mixed = [None] * GROUP
        for r in range(in_slot):
            here = slice(r * inner, (r + 1) * inner)
            values = jnp.concatenate([ring.at[slot_of(j0 + 2)][here, :], ring.at[slot_of(j0 + 3)][here, :]], axis=1)
            pa = p[r * n_head:(r + 1) * n_head, :]
            pb = p[(r + in_slot) * n_head:(r + in_slot + 1) * n_head, :]
            lhs = jnp.concatenate([jnp.concatenate([pa, none], axis=1), jnp.concatenate([none, pb], axis=1)], axis=0)
            y = lax.dot_general(lhs, values, (((1,), (1,)), ((), ())), preferred_element_type=F32)
            mixed[r] = jnp.sum(jnp.where(own_head, y[0:n_head], 0.0), axis=0, keepdims=True)
            mixed[r + in_slot] = jnp.sum(jnp.where(own_head, y[n_head:], 0.0), axis=0, keepdims=True)
        mix_ref[at, :] = jnp.concatenate(mixed, axis=0)

        n0 = j0 + SLOTS
        last = (first_o - SLOTS - first_kv) // (2 * per_step)
        last_o = (first_gu - SLOTS - first_kv) // (2 * per_step)
        last_gu = (first_d - SLOTS - first_kv) // (2 * per_step)

        @pl.when(g < last)
        def _():
            issue_step(g + SLOTS_STEPS, n0)

        @pl.when((g >= last) & (g < last_o))
        def _():
            for piece in range(2 * per_step):
                issue_o(n0 + piece)

        @pl.when((g >= last_o) & (g < last_gu))
        def _():
            for piece in range(per_step):
                issue_gu((g - last_o) * per_step + piece, n0 + 2 * piece)

        @pl.when(g >= last_gu)
        def _():
            for piece in range(2 * per_step):
                issue_d(n0 + piece)
        return carry
    SLOTS_STEPS = SLOTS // (2 * per_step)
    lax.fori_loop(0, n_step, attend_step, 0)

    sent(0)
    mixbf[...] = mix_ref[...].astype(BF16)
    o_cols = o_blocks * LANES
    per_chunk = width // o_cols
    for n in range(n_o):
        j = first_o + n
        landed(j)
        w = jnp.concatenate([ring.at[slot_of(j)][r * inner:(r + 1) * inner, :] for r in range(o_blocks)], axis=1)
        y = jnp.dot(mixbf[...], w, preferred_element_type=F32)
        pbuf[:, n * o_cols:(n + 1) * o_cols] = y.astype(BF16)
        issue(j + SLOTS)
        if n % per_chunk == per_chunk - 1:
            to_partner(1, n // per_chunk).start()
            if n // per_chunk > 0:
                chip_sum(1, n // per_chunk - 1)
    chip_sum(1, AR_CHUNKS - 1)
    for j in range(AR_CHUNKS):
        full_sum(1, j)
    normalise(1)

    root = math.sqrt(2.0 / math.pi)

    def gate_up(i, carry):
        j0 = first_gu + 2 * i
        landed(j0)
        landed(j0 + 1)
        y = jnp.dot(hbuf[...], pair(j0), preferred_element_type=F32)
        u = y[:, 0:LANES]
        gelu = 0.5 * u * (1.0 + jnp.tanh(root * (u + 0.044715 * (u * u * u))))
        act[:, pl.ds(pl.multiple_of(i * LANES, LANES), LANES)] = (gelu * y[:, LANES:]).astype(BF16)

        @pl.when(j0 + SLOTS < total)
        def _():
            issue_d(j0 + SLOTS)
            issue_d(j0 + 1 + SLOTS)
        return carry
    lax.fori_loop(0, n_gu, gate_up, 0)
    sent(1)

    per_piece = width // (2 * LANES)

    def out_back(j):
        at = pl.ds(j * width, width)
        return pltpu.make_async_remote_copy(
            src_ref=hbuf.at[mine, at], dst_ref=hbuf.at[mine, at], send_sem=s3_send.at[0, j],
            recv_sem=s3_recv.at[0, j], device_id=partner, device_id_type=MESH)

    for c in range(AR_CHUNKS):
        def down(i, carry):
            j0 = first_d + 2 * (c * per_piece + i)
            landed(j0, d_ff)
            landed(j0 + 1, d_ff)
            y = jnp.dot(act[...], pair(j0, d_ff), preferred_element_type=F32)
            at = pl.multiple_of((c * per_piece + i) * 2 * LANES, 2 * LANES)
            pbuf[:, pl.ds(at, 2 * LANES)] = y.astype(BF16)
            return carry
        lax.fori_loop(0, per_piece, down, 0)
        to_partner(2, c).start()
        if c > 0:
            chip_sum(2, c - 1)
    chip_sum(2, AR_CHUNKS - 1)

    def out_copy(j):
        at = pl.ds(j * width, width)
        return pltpu.make_async_copy(hbuf.at[:, at], out_hbm.at[:, at], out_sem.at[j])

    for j in range(AR_CHUNKS):
        at = pl.ds(j * width, width)
        to_across(2, j).wait_recv()

        def add(r):
            both = tx2[0, pl.ds(r, 16), at].astype(F32) + rx2[0, pl.ds(r, 16), at].astype(F32)
            hbuf[pl.ds(pl.multiple_of(core * half + r, 16), 16), at] = (res[pl.ds(r, 16), at] + both).astype(BF16)
        blocks(add)
        out_back(j).start()
    for j in range(AR_CHUNKS):
        out_back(j).wait()
        out_copy(j).start()
    sent(2)
    for j in range(AR_CHUNKS):
        out_copy(j).wait()


def rest_of_layer(x_in, part, norms, enc_mask, cross_k, cross_v, cross_q, cross_o, w_gate, w_up, w_down):
    rows, d_model = x_in.shape
    _, src_len, n_head, d_head = cross_k.shape
    inner = n_head * d_head
    d_ff = w_gate.shape[1]
    half = rows // 2
    flat = (rows * inner, src_len)
    k_flat = cross_k.transpose(0, 2, 3, 1).reshape(flat)
    v_flat = cross_v.transpose(0, 2, 3, 1).reshape(flat)
    return pl.pallas_call(
        functools.partial(cross_kernel, n_head),
        out_shape=jax.ShapeDtypeStruct((rows, d_model), BF16),
        in_specs=[ANY, ANY, VMEM, VMEM] + [ANY] * 7,
        out_specs=ANY,
        scratch_shapes=[
            pltpu.VMEM((SLOTS, d_model, LANES), BF16),
            pltpu.VMEM((rows, d_model), BF16),
            pltpu.VMEM((rows, d_model), BF16),
            pltpu.VMEM((half, d_model), F32),
            pltpu.VMEM((half, d_model), BF16),
            pltpu.VMEM((2, half, d_model), BF16),
            pltpu.VMEM((2, half, d_model), BF16),
            pltpu.VMEM((2, half, d_model), BF16),
            pltpu.VMEM((rows, inner), F32),
            pltpu.VMEM((rows, inner), F32),
            pltpu.VMEM((rows, inner), BF16),
            pltpu.VMEM((rows, d_ff), BF16),
            pltpu.SemaphoreType.DMA((SLOTS,)),
            pltpu.SemaphoreType.DMA((AR_CHUNKS + 1,)),
            pltpu.SemaphoreType.DMA((2, AR_CHUNKS)),
            pltpu.SemaphoreType.DMA((2, AR_CHUNKS)),
            pltpu.SemaphoreType.DMA((2, AR_CHUNKS)),
            pltpu.SemaphoreType.DMA((2, AR_CHUNKS)),
            pltpu.SemaphoreType.DMA((2, AR_CHUNKS)),
            pltpu.SemaphoreType.DMA((2, AR_CHUNKS)),
            pltpu.SemaphoreType.DMA((AR_CHUNKS,)),
        ],
        compiler_params=pltpu.CompilerParams(vmem_limit_bytes=67_000_000, collective_id=0, has_side_effects=True),
        name="rest_part",
    )(x_in, part, norms, enc_mask, cross_q, k_flat, v_flat, cross_o, w_gate, w_up, w_down)


def solution(mesh):
    def local_layer(x_in, tok_pos, self_k, self_v, cross_k, cross_v, enc_mask, rel_bias, w_q, w_k, w_v, w_o, cross_q, cross_o, w_gate, w_up, w_down, norm_self, norm_cross, norm_mlp):
        norms = jnp.stack([norm_self, norm_cross, norm_mlp]).astype(F32)
        part, new_self_k, new_self_v = self_attention(x_in, norms, tok_pos, rel_bias, w_q, w_k, w_v, w_o, self_k, self_v)
        x_out = rest_of_layer(x_in, part, norms, enc_mask, cross_k, cross_v, cross_q, cross_o, w_gate, w_up, w_down)
        return x_out, new_self_k, new_self_v

    cache_spec = P('dp', None, 'tp', None)
    split_cols = P(None, 'tp')
    split_rows = P('tp', None)
    in_specs = (P('dp', None), P('dp'), cache_spec, cache_spec, cache_spec, cache_spec, P('dp', None), split_cols, split_cols, split_cols, split_cols, split_rows, split_cols, split_rows, split_cols, split_cols, split_rows, P(None), P(None), P(None))
    out_specs = (P('dp', None), cache_spec, cache_spec)
    return jax.shard_map(local_layer, mesh=mesh, in_specs=in_specs, out_specs=out_specs, check_vma=False)
```

```python
import functools
import math
import jax
import jax.numpy as jnp
from jax import lax
from jax.experimental import pallas as pl
from jax.experimental.pallas import tpu as pltpu
from jax.sharding import PartitionSpec as P

BUCKET_EDGES = tuple(int(math.ceil(16.0 * 8.0 ** (bucket_step / 16.0))) for bucket_step in range(1, 16))
NEG_FILL = -1e30
F32 = jnp.float32
BF16 = jnp.bfloat16
ANY = pl.BlockSpec(memory_space=pl.ANY)
VMEM = pl.BlockSpec(memory_space=pltpu.VMEM)
COLS = 256
T_BLOCK = 8


def lay_row(dst, at, norm):
    values = norm[...].astype(F32)
    for i in range(values.shape[0]):
        dst[at:at + 1, i * 128:(i + 1) * 128] = values[i:i + 1, :]


def self_kernel(x_hbm, norm_hbm, pos_hbm, rel_hbm, wq_hbm, wk_hbm, wv_hbm, wo_hbm, k_hbm, v_hbm,
                part_hbm, newk_hbm, newv_hbm,
                xbuf, hbuf, wbuf, kvbuf, q_ref, kn_ref, hit_ref, score_ref, acc_ref,
                norm_ref, nrow, pos_ref, rel_ref,
                x_sem, small_sem, w_sem, kv_sem, out_sem, part_sem, window):
    rows, d_model = xbuf.shape
    n_w = wbuf.shape[0]
    per_mat = n_w // 3
    n_chunk = kvbuf.shape[0] // 2
    n_head, t_len = score_ref.shape[0], score_ref.shape[1]
    inner = acc_ref.shape[0]
    d_head = inner // n_head
    chunk_rows = kvbuf.shape[1]
    sub = d_head // 16
    wo_per_slot = wbuf.shape[1] // inner
    n_wo = wo_hbm.shape[1] // COLS // wo_per_slot

    def w_copy(c):
        src = (wq_hbm, wk_hbm, wv_hbm)[c // per_mat]
        return pltpu.make_async_copy(src.at[:, pl.ds((c % per_mat) * COLS, COLS)], wbuf.at[c], w_sem.at[c])

    def kv_copy(i):
        src = k_hbm if i < n_chunk else v_hbm
        return pltpu.make_async_copy(src.at[pl.ds((i % n_chunk) * chunk_rows, chunk_rows)], kvbuf.at[i], kv_sem.at[i])

    def wo_copies(i):
        return [pltpu.make_async_copy(wo_hbm.at[:, pl.ds((i * wo_per_slot + r) * COLS, COLS)],
                                      wbuf.at[i, pl.ds(r * inner, inner)], w_sem.at[i]) for r in range(wo_per_slot)]

    loads = [[w_copy(c)] for c in range(n_w)] + [[kv_copy(i)] for i in range(2 * n_chunk)] + [wo_copies(i) for i in range(n_wo)]
    issued = [0]

    def issue(upto):
        while issued[0] < min(upto, len(loads)):
            for copy in loads[issued[0]]:
                copy.start()
            issued[0] += 1

    x_copy = pltpu.make_async_copy(x_hbm, xbuf, x_sem)
    x_copy.start()
    small = [pltpu.make_async_copy(src, dst, small_sem.at[i]) for i, (src, dst) in enumerate(
        ((pos_hbm, pos_ref), (rel_hbm, rel_ref), (norm_hbm, norm_ref)))]
    for copy in small:
        copy.start()
    issue(window)
    for copy in small:
        copy.wait()

    lay_row(nrow, 0, norm_ref)
    pos = pos_ref[...]
    pos16 = jnp.broadcast_to(pos, (16, rows))

    def set_hit(t, carry):
        hit_ref[t] = jnp.where(pos16 == t, 1.0, 0.0).astype(BF16)
        return carry
    lax.fori_loop(0, t_len, set_hit, 0)

    lane = lax.broadcasted_iota(jnp.int32, (n_head, 128), 1)
    bucket = jnp.full((n_head, 128), 16, jnp.int32)
    for edge in BUCKET_EDGES:
        bucket = bucket + (lane >= edge).astype(jnp.int32)
    bucket = jnp.where(lane < 16, lane, bucket)
    rel = rel_ref[...]
    table = jnp.zeros((n_head, 128), F32)
    for b in range(rel.shape[1]):
        table = jnp.where(bucket == b, rel[:, b:b + 1], table)
    acc_ref[0:n_head, :] = table

    x_copy.wait()
    block = 16
    norm = nrow[0:1, :]

    def norm_rows(i, carry):
        at = pl.ds(pl.multiple_of(i * block, block), block)
        r = xbuf[at, :].astype(F32)
        inv = lax.rsqrt(jnp.mean(r * r, axis=-1, keepdims=True) + 1e-6)
        hbuf[at, :] = (r * inv * norm).astype(BF16)
        return carry
    lax.fori_loop(0, rows // block, norm_rows, 0)

    for c in range(n_w):
        w_copy(c).wait()
        issue(c + 1 + window)
        y = jnp.dot(hbuf[...], wbuf[c], preferred_element_type=F32).astype(BF16).astype(F32).T
        at = (c % per_mat) * COLS
        if c < per_mat:
            q_ref[at:at + COLS, :] = y
        else:
            kn_ref[c // per_mat - 1, at:at + COLS, :] = y.astype(BF16)

    def chunk_out(i):
        dst = newk_hbm if i < n_chunk else newv_hbm
        return pltpu.make_async_copy(kvbuf.at[i], dst.at[pl.ds((i % n_chunk) * chunk_rows, chunk_rows)], out_sem.at[i])

    for j in range(n_chunk):
        kv_copy(j).wait()
        issue(n_w + j + 1 + window)

        def k_head(h, carry):
            at = pl.multiple_of(h * d_head, d_head)
            q = q_ref[pl.ds(at, d_head), :]
            kn = kn_ref[0, pl.ds(at, d_head), :].reshape(sub, 16, rows)
            rows_out = []
            for tt in range(T_BLOCK):
                here = pl.ds(pl.multiple_of(tt * inner + at, d_head), d_head)
                old = kvbuf[j, here, :].reshape(sub, 16, rows)
                hit = hit_ref[j * T_BLOCK + tt] != 0
                new = jnp.where(hit[None], kn, old)
                kvbuf[j, here, :] = new.reshape(d_head, rows)
                prod = new.reshape(d_head, rows).astype(F32) * q
                rows_out.append(jnp.sum(prod, axis=0, keepdims=True))
            score_ref[h, j * T_BLOCK:(j + 1) * T_BLOCK, :] = jnp.concatenate(rows_out, axis=0)
            return carry
        lax.fori_loop(0, n_head, k_head, 0)
        chunk_out(j).start()

    t_iota = lax.broadcasted_iota(jnp.int32, (t_len, rows), 0)
    causal = t_iota <= pos
    back = jnp.maximum(pos - t_iota, 0)

    def soft_head(h, carry):
        line = jnp.broadcast_to(acc_ref[pl.ds(h, 1), :], (t_len, 128))
        s = score_ref[h] + jnp.take_along_axis(line, back, axis=1)
        s = jnp.where(causal, s, NEG_FILL)
        e = jnp.exp(s - jnp.max(s, axis=0, keepdims=True))
        p = e / jnp.sum(e, axis=0, keepdims=True)
        score_ref[h] = p.astype(BF16).astype(F32)
        return carry
    lax.fori_loop(0, n_head, soft_head, 0)

    acc_ref[...] = jnp.zeros_like(acc_ref)
    for j in range(n_chunk):
        kv_copy(n_chunk + j).wait()
        issue(n_w + n_chunk + j + 1 + window)

        def v_head(h, carry):
            at = pl.multiple_of(h * d_head, d_head)
            vn = kn_ref[1, pl.ds(at, d_head), :].reshape(sub, 16, rows)
            p = score_ref[h, j * T_BLOCK:(j + 1) * T_BLOCK, :]
            acc = acc_ref[pl.ds(at, d_head), :]
            for tt in range(T_BLOCK):
                here = pl.ds(pl.multiple_of(tt * inner + at, d_head), d_head)
                old = kvbuf[n_chunk + j, here, :].reshape(sub, 16, rows)
                hit = hit_ref[j * T_BLOCK + tt] != 0
                new = jnp.where(hit[None], vn, old)
                kvbuf[n_chunk + j, here, :] = new.reshape(d_head, rows)
                acc = acc + new.reshape(d_head, rows).astype(F32) * p[tt:tt + 1, :]
            acc_ref[pl.ds(at, d_head), :] = acc
            return carry
        lax.fori_loop(0, n_head, v_head, 0)
        chunk_out(n_chunk + j).start()

    issue(len(loads))
    hbuf[:, 0:inner] = acc_ref[...].T.astype(BF16)
    width = wo_per_slot * COLS
    part_copies = []
    for i in range(n_wo):
        for copy in wo_copies(i):
            copy.wait()
        for r in range(wo_per_slot):
            at = (i * wo_per_slot + r) * COLS
            y = jnp.dot(hbuf[:, 0:inner], wbuf[i, r * inner:(r + 1) * inner, :], preferred_element_type=F32)
            xbuf[:, at:at + COLS] = y.astype(BF16)
        copy = pltpu.make_async_copy(xbuf.at[:, pl.ds(i * width, width)], part_hbm.at[:, pl.ds(i * width, width)], part_sem.at[i])
        copy.start()
        part_copies.append(copy)
    for i in range(2 * n_chunk):
        chunk_out(i).wait()
    for copy in part_copies:
        copy.wait()


def self_attention(x_in, norm_self, tok_pos, rel_bias, w_q, w_k, w_v, w_o, self_k, self_v):
    rows, t_len, n_head, d_head = self_k.shape
    d_model = x_in.shape[1]
    inner = n_head * d_head
    flat = (t_len * inner, rows)
    k_flat = self_k.transpose(1, 2, 3, 0).reshape(flat)
    v_flat = self_v.transpose(1, 2, 3, 0).reshape(flat)
    n_w = 3 * (inner // COLS)
    n_chunk = t_len // T_BLOCK
    n_wo = w_o.shape[1] // COLS // (d_model // inner)

    def body(*refs):
        self_kernel(*refs, window=12)

    part, new_k, new_v = pl.pallas_call(
        body,
        out_shape=(jax.ShapeDtypeStruct((rows, w_o.shape[1]), BF16),
                   jax.ShapeDtypeStruct(flat, BF16), jax.ShapeDtypeStruct(flat, BF16)),
        in_specs=[ANY] * 10,
        out_specs=(ANY, ANY, ANY),
        scratch_shapes=[
            pltpu.VMEM((rows, d_model), BF16),
            pltpu.VMEM((rows, d_model), BF16),
            pltpu.VMEM((n_w, d_model, COLS), BF16),
            pltpu.VMEM((2 * n_chunk, T_BLOCK * inner, rows), BF16),
            pltpu.VMEM((inner, rows), F32),
            pltpu.VMEM((2, inner, rows), BF16),
            pltpu.VMEM((t_len, 16, rows), BF16),
            pltpu.VMEM((n_head, t_len, rows), F32),
            pltpu.VMEM((inner, rows), F32),
            pltpu.VMEM((d_model // 128, 128), BF16),
            pltpu.VMEM((1, d_model), F32),
            pltpu.VMEM((1, rows), jnp.int32),
            pltpu.VMEM(rel_bias.shape[::-1], F32),
            pltpu.SemaphoreType.DMA,
            pltpu.SemaphoreType.DMA((3,)),
            pltpu.SemaphoreType.DMA((n_w,)),
            pltpu.SemaphoreType.DMA((2 * n_chunk,)),
            pltpu.SemaphoreType.DMA((2 * n_chunk,)),
            pltpu.SemaphoreType.DMA((n_wo,)),
        ],
        compiler_params=pltpu.CompilerParams(vmem_limit_bytes=66_900_000),
        cost_estimate=pl.CostEstimate(flops=4_400_000_000, bytes_accessed=104_000_000, transcendentals=131_072),
        name="self_part",
    )(x_in, norm_self.reshape(d_model // 128, 128), tok_pos.reshape(1, rows), rel_bias.T, w_q, w_k, w_v, w_o, k_flat, v_flat)

    def unflat(cache):
        return cache.reshape(t_len, n_head, d_head, rows).transpose(3, 0, 1, 2)
    return part, unflat(new_k), unflat(new_v)


SLOTS = 52
FIXED = 8
RING = SLOTS - 2 * FIXED
GROUP = 8
AR_CHUNKS = 4
LANES = 128


def cross_kernel(n_head, x_hbm, part_hbm, ncross_hbm, nmlp_hbm, mask_hbm, cq_hbm, ck_hbm, cv_hbm, co_hbm, wg_hbm, wu_hbm, wd_hbm,
                 out_hbm,
                 ring, pbuf, hbuf, res, xhalf, rx1, tx2, rx2, q_ref, mix_ref, act, norm_in, nrow, mask_ref,
                 ring_sem, load_sem, small_sem, s1_send, s1_recv, s2_send, s2_recv, s3_send, s3_recv, out_sem):
    rows, d_model = hbuf.shape
    half = rows // 2
    part = half // 2
    depth = ring.shape[1]
    inner = q_ref.shape[1]
    d_ff = act.shape[1]
    width = d_model // AR_CHUNKS
    MESH = pl.DeviceIdType.MESH

    me = lax.axis_index("tp")
    core = lax.rem(me, 2)
    chip = me // 2
    partner = {"tp": chip * 2 + (1 - core)}
    across = {"tp": (1 - chip) * 2 + core}

    def mine(at, n):
        return pl.ds(pl.multiple_of(core * half + at, 16), n)

    def theirs(at, n):
        return pl.ds(pl.multiple_of((1 - core) * half + at, 16), n)

    def piece(j):
        return pl.ds(j * width, width)

    per_step = GROUP * inner // depth
    n_step = rows // GROUP
    n_kv = 2 * per_step * n_step
    n_gu = d_ff // LANES
    n_d = d_model // LANES
    o_blocks = depth // inner
    fixed_d = 2 * FIXED

    def copy_in(src, slot, used=None):
        dst = ring.at[slot] if used is None else ring.at[slot, used]
        pltpu.make_async_copy(src, dst, ring_sem.at[slot]).start()

    def landed(slot, used=depth):
        pltpu.make_async_copy(ck_hbm.at[pl.ds(0, used)], ring.at[slot, pl.ds(0, used)], ring_sem.at[slot]).wait()

    def cols(ref, i):
        return ref.at[:, pl.ds(i * LANES if isinstance(i, int) else pl.multiple_of(i * LANES, LANES), LANES)]

    def ring_slot(n):
        return 2 * FIXED + n % RING

    def group_of(step):
        per_half, u = n_step // 2, step % (n_step // 2)
        return (step // per_half) * (part // GROUP) + u + (u // (part // GROUP)) * (part // GROUP)

    def issue_step(step):
        for k in range(2 * per_step):
            src = ck_hbm if k < per_step else cv_hbm
            at = (group_of(step) * per_step + k % per_step) * depth
            at = at if isinstance(at, int) else pl.multiple_of(at, depth)
            copy_in(src.at[pl.ds(at, depth)], ring_slot(step * 2 * per_step + k))

    def issue_gu(i):
        copy_in(cols(wg_hbm, i), ring_slot(n_kv + 2 * i))
        copy_in(cols(wu_hbm, i), ring_slot(n_kv + 2 * i + 1))

    def d_slot(i):
        if isinstance(i, int) and i < fixed_d:
            return i
        return ring_slot(n_kv + 2 * n_gu + i - fixed_d)

    def issue_d(i):
        copy_in(cols(wd_hbm, i), d_slot(i), pl.ds(0, d_ff))

    def to_partner(a, h, j, at, n):
        return pltpu.make_async_remote_copy(
            src_ref=pbuf.at[theirs(at, n), piece(j)], dst_ref=rx1.at[a % 2, pl.ds(at, n), piece(j)],
            send_sem=s1_send.at[a % 2, h, j], recv_sem=s1_recv.at[a % 2, h, j], device_id=partner, device_id_type=MESH)

    def to_across(a, h, j, at, n):
        return pltpu.make_async_remote_copy(
            src_ref=tx2.at[a % 2, pl.ds(at, n), piece(j)], dst_ref=rx2.at[a % 2, pl.ds(at, n), piece(j)],
            send_sem=s2_send.at[a % 2, h, j], recv_sem=s2_recv.at[a % 2, h, j], device_id=across, device_id_type=MESH)

    def blocks(at, n, fn):
        def body(i, carry):
            fn(pl.multiple_of(at + i * 16, 16))
            return carry
        lax.fori_loop(0, n // 16, body, 0)

    def chip_sum(a, h, j, at, n):
        to_partner(a, h, j, at, n).wait_recv()

        def add(r):
            own = pbuf[mine(r, 16), piece(j)].astype(F32)
            tx2[a % 2, pl.ds(r, 16), piece(j)] = (own + rx1[a % 2, pl.ds(r, 16), piece(j)].astype(F32)).astype(BF16)
        blocks(at, n, add)
        to_across(a, h, j, at, n).start()

    def full_sum(a, h, j, at, n):
        to_across(a, h, j, at, n).wait_recv()

        def add(r):
            both = tx2[a % 2, pl.ds(r, 16), piece(j)].astype(F32) + rx2[a % 2, pl.ds(r, 16), piece(j)].astype(F32)
            res[pl.ds(r, 16), piece(j)] = res[pl.ds(r, 16), piece(j)] + both
        blocks(at, n, add)

    def sent(a, h, at, n):
        for j in range(AR_CHUNKS):
            to_partner(a, h, j, at, n).wait_send()
            to_across(a, h, j, at, n).wait_send()

    def rows_back(a, h, i):
        at = mine(h * part + i * 16, 16)
        return pltpu.make_async_remote_copy(
            src_ref=hbuf.at[at], dst_ref=hbuf.at[at], send_sem=s3_send.at[a % 2, h, i],
            recv_sem=s3_recv.at[a % 2, h, i], device_id=partner, device_id_type=MESH)

    def normalise(a, h):
        norm = nrow[a:a + 1, :]
        for i in range(part // 16):
            r = res[h * part + i * 16:h * part + (i + 1) * 16, :]
            inv = lax.rsqrt(jnp.mean(r * r, axis=-1, keepdims=True) + 1e-6)
            hbuf[mine(h * part + i * 16, 16), :] = (r * inv * norm).astype(BF16)
            rows_back(a, h, i).start()

    def all_rows(a, h):
        for i in range(part // 16):
            rows_back(a, h, i).wait()

    pieces = range(AR_CHUNKS)
    halves = range(2)
    first = [pltpu.make_async_copy(part_hbm.at[:, piece(j)], pbuf.at[:, piece(j)], load_sem.at[j]) for j in pieces]
    for copy in first:
        copy.start()
    small = [pltpu.make_async_copy(src, dst, small_sem.at[i]) for i, (src, dst) in enumerate(
        ((x_hbm.at[mine(0, half)], xhalf), (ncross_hbm, norm_in.at[0]), (nmlp_hbm, norm_in.at[1]), (mask_hbm, mask_ref)))]
    for copy in small:
        copy.start()
    barrier = pltpu.get_barrier_semaphore()
    for other in (partner, across):
        pl.semaphore_signal(barrier, inc=1, device_id=other, device_id_type=MESH)
    pl.semaphore_wait(barrier, 2)

    for j in pieces:
        first[j].wait()
        to_partner(0, 0, j, 0, part).start()
    for j in pieces:
        to_partner(0, 1, j, part, part).start()
    for i in range(FIXED):
        copy_in(cols(cq_hbm, i), i)
    for step in range(RING // (2 * per_step)):
        issue_step(step)
    for i in range(FIXED):
        for r in range(o_blocks):
            copy_in(cols(co_hbm, i * o_blocks + r), FIXED + i, pl.ds(r * inner, inner))
    for h in halves:
        for j in pieces:
            chip_sum(0, h, j, h * part, part)
    for copy in small:
        copy.wait()
    lay_row(nrow, 0, norm_in.at[0])
    lay_row(nrow, 1, norm_in.at[1])
    blocks(0, half, lambda r: res.__setitem__((pl.ds(r, 16), slice(None)), xhalf[pl.ds(r, 16), :].astype(F32)))

    def beside(a, b, used=depth):
        return jnp.concatenate([ring[a, 0:used, :], ring[b, 0:used, :]], axis=1)

    def both_cores(ref, h):
        return jnp.concatenate([ref[h * part:(h + 1) * part, :], ref[half + h * part:half + (h + 1) * part, :]], axis=0)

    def project_q(h):
        lhs = both_cores(hbuf, h)
        for i in range(FIXED // 2):
            if h == 0:
                landed(2 * i)
                landed(2 * i + 1)
            y = jnp.dot(lhs, beside(2 * i, 2 * i + 1), preferred_element_type=F32).astype(BF16).astype(F32)
            here = slice(2 * i * LANES, (2 * i + 2) * LANES)
            q_ref[h * part:(h + 1) * part, here] = y[0:part]
            q_ref[half + h * part:half + (h + 1) * part, here] = y[part:]

    own_head = (lax.broadcasted_iota(jnp.int32, (n_head, inner), 1) // (inner // n_head)
                == lax.broadcasted_iota(jnp.int32, (n_head, inner), 0))
    in_slot = GROUP // per_step

    def attend_step(step, carry):
        at = pl.ds(pl.multiple_of(group_of(step) * GROUP, GROUP), GROUP)
        ka, kb, va, vb = [ring_slot(step * 2 * per_step + k) for k in range(4)]
        q8 = q_ref[at, :]
        m8 = mask_ref[at, :]

        def spread(r):
            return jnp.where(own_head, jnp.broadcast_to(q8[r:r + 1, :], (n_head, inner)), 0.0).astype(BF16)

        def rows_of(a, b, r):
            here = pl.ds(r * inner, inner)
            return jnp.concatenate([ring[a, here, :], ring[b, here, :]], axis=1)
        landed(ka)
        landed(kb)
        scores = [None] * GROUP
        for r in range(in_slot):
            s = jnp.dot(jnp.concatenate([spread(r), spread(r + in_slot)], axis=0), rows_of(ka, kb, r), preferred_element_type=F32)
            scores[r] = jnp.where(m8[r:r + 1, :] != 0, s[0:n_head, 0:LANES], NEG_FILL)
            scores[r + in_slot] = jnp.where(m8[r + in_slot:r + in_slot + 1, :] != 0, s[n_head:, LANES:], NEG_FILL)
        s = jnp.concatenate(scores, axis=0)
        e = jnp.exp(s - jnp.max(s, axis=1, keepdims=True))
        p = (e / jnp.sum(e, axis=1, keepdims=True)).astype(BF16)
        landed(va)
        landed(vb)
        none = jnp.zeros((n_head, LANES), BF16)
        mixed = [None] * GROUP
        for r in range(in_slot):
            pa = p[r * n_head:(r + 1) * n_head, :]
            pb = p[(r + in_slot) * n_head:(r + in_slot + 1) * n_head, :]
            lhs = jnp.concatenate([jnp.concatenate([pa, none], axis=1), jnp.concatenate([none, pb], axis=1)], axis=0)
            y = lax.dot_general(lhs, rows_of(va, vb, r), (((1,), (1,)), ((), ())), preferred_element_type=F32)
            mixed[r] = jnp.sum(jnp.where(own_head, y[0:n_head], 0.0), axis=0, keepdims=True)
            mixed[r + in_slot] = jnp.sum(jnp.where(own_head, y[n_head:], 0.0), axis=0, keepdims=True)
        mix_ref[at, :] = jnp.concatenate(mixed, axis=0)

        ahead = RING // (2 * per_step)

        @pl.when(step + ahead < n_step)
        def _():
            issue_step(step + ahead)

        @pl.when(step + ahead >= n_step)
        def _():
            for k in range(per_step):
                issue_gu((step + ahead - n_step) * per_step + k)
        return carry

    o_cols = o_blocks * LANES
    per_piece_o = width // o_cols

    def project_o(h, after):
        lhs = both_cores(mix_ref, h).astype(BF16)
        for n in range(FIXED):
            if h == 0:
                landed(FIXED + n)
            w = jnp.concatenate([ring[FIXED + n, r * inner:(r + 1) * inner, :] for r in range(o_blocks)], axis=1)
            y = jnp.dot(lhs, w, preferred_element_type=F32).astype(BF16)
            here = slice(n * o_cols, (n + 1) * o_cols)
            pbuf[h * part:(h + 1) * part, here] = y[0:part]
            pbuf[half + h * part:half + (h + 1) * part, here] = y[part:]
            if n % per_piece_o == per_piece_o - 1:
                j = n // per_piece_o
                to_partner(1, h, j, h * part, part).start()
                if after and j > 0:
                    chip_sum(1, h, j - 1, h * part, part)
        if after:
            chip_sum(1, h, AR_CHUNKS - 1, h * part, part)

    for j in pieces:
        full_sum(0, 0, j, 0, part)
    normalise(0, 0)
    all_rows(0, 0)
    project_q(0)
    lax.fori_loop(0, n_step // 2, attend_step, 0)
    sent(0, 0, 0, part)
    project_o(0, False)
    for j in pieces:
        full_sum(0, 1, j, part, part)
    normalise(0, 1)
    for j in pieces:
        chip_sum(1, 0, j, 0, part)
    all_rows(0, 1)
    project_q(1)
    lax.fori_loop(n_step // 2, n_step, attend_step, 0)
    sent(0, 1, part, part)
    project_o(1, True)
    for i in range(fixed_d):
        issue_d(i)
    for j in pieces:
        full_sum(1, 0, j, 0, part)
    normalise(1, 0)
    for j in pieces:
        full_sum(1, 1, j, part, part)
    normalise(1, 1)
    for h in halves:
        all_rows(1, h)
        sent(1, h, h * part, part)

    root = math.sqrt(2.0 / math.pi)
    gu_ahead = (n_kv + 2 * n_gu - (n_kv + RING)) // 2

    def gate_up(i, carry):
        a, b = ring_slot(n_kv + 2 * i), ring_slot(n_kv + 2 * i + 1)
        landed(a)
        landed(b)
        y = jnp.dot(hbuf[...], beside(a, b), preferred_element_type=F32)
        u = y[:, 0:LANES]
        gelu = 0.5 * u * (1.0 + jnp.tanh(root * (u + 0.044715 * (u * u * u))))
        act[:, pl.ds(pl.multiple_of(i * LANES, LANES), LANES)] = (gelu * y[:, LANES:]).astype(BF16)

        @pl.when(i < gu_ahead)
        def _():
            issue_gu(i + RING // 2)

        @pl.when((i >= gu_ahead) & (i < gu_ahead + (n_d - fixed_d) // 2))
        def _():
            issue_d(fixed_d + 2 * (i - gu_ahead))
            issue_d(fixed_d + 2 * (i - gu_ahead) + 1)
        return carry
    lax.fori_loop(0, n_gu, gate_up, 0)

    per_piece = width // (2 * LANES)

    def out_back(j):
        return pltpu.make_async_remote_copy(
            src_ref=hbuf.at[mine(0, half), piece(j)], dst_ref=hbuf.at[mine(0, half), piece(j)], send_sem=s3_send.at[0, 0, j],
            recv_sem=s3_recv.at[0, 0, j], device_id=partner, device_id_type=MESH)

    for c in pieces:
        def down(i, carry):
            n = c * per_piece + i
            if (c + 1) * per_piece * 2 <= fixed_d:
                a, b = 2 * n, 2 * n + 1
            else:
                a = ring_slot(n_kv + 2 * n_gu + 2 * n - fixed_d)
                b = ring_slot(n_kv + 2 * n_gu + 2 * n + 1 - fixed_d)
            landed(a, d_ff)
            landed(b, d_ff)
            y = jnp.dot(act[...], beside(a, b, d_ff), preferred_element_type=F32)
            pbuf[:, pl.ds(pl.multiple_of(n * 2 * LANES, 2 * LANES), 2 * LANES)] = y.astype(BF16)
            return carry
        lax.fori_loop(0, per_piece, down, 0)
        to_partner(2, 0, c, 0, half).start()
        if c > 0:
            chip_sum(2, 0, c - 1, 0, half)
    chip_sum(2, 0, AR_CHUNKS - 1, 0, half)

    def out_copy(j):
        return pltpu.make_async_copy(hbuf.at[:, piece(j)], out_hbm.at[:, piece(j)], out_sem.at[j])

    for j in pieces:
        to_across(2, 0, j, 0, half).wait_recv()

        def add(r):
            both = tx2[0, pl.ds(r, 16), piece(j)].astype(F32) + rx2[0, pl.ds(r, 16), piece(j)].astype(F32)
            hbuf[mine(r, 16), piece(j)] = (res[pl.ds(r, 16), piece(j)] + both).astype(BF16)
        blocks(0, half, add)
        out_back(j).start()
        if j > 0:
            out_back(j - 1).wait()
            out_copy(j - 1).start()
    out_back(AR_CHUNKS - 1).wait()
    out_copy(AR_CHUNKS - 1).start()
    sent(2, 0, 0, half)
    for j in pieces:
        out_copy(j).wait()


def rest_of_layer(x_in, part, norm_cross, norm_mlp, enc_mask, cross_k, cross_v, cross_q, cross_o, w_gate, w_up, w_down):
    rows, d_model = x_in.shape
    _, src_len, n_head, d_head = cross_k.shape
    inner = n_head * d_head
    d_ff = w_gate.shape[1]
    half = rows // 2
    flat = (rows * inner, src_len)
    k_flat = cross_k.transpose(0, 2, 3, 1).reshape(flat)
    v_flat = cross_v.transpose(0, 2, 3, 1).reshape(flat)
    square = (d_model // 128, 128)
    return pl.pallas_call(
        functools.partial(cross_kernel, n_head),
        out_shape=jax.ShapeDtypeStruct((rows, d_model), BF16),
        in_specs=[ANY] * 12,
        out_specs=ANY,
        scratch_shapes=[
            pltpu.VMEM((SLOTS, d_model, LANES), BF16),
            pltpu.VMEM((rows, d_model), BF16),
            pltpu.VMEM((rows, d_model), BF16),
            pltpu.VMEM((half, d_model), F32),
            pltpu.VMEM((half, d_model), BF16),
            pltpu.VMEM((2, half, d_model), BF16),
            pltpu.VMEM((2, half, d_model), BF16),
            pltpu.VMEM((2, half, d_model), BF16),
            pltpu.VMEM((rows, inner), F32),
            pltpu.VMEM((rows, inner), F32),
            pltpu.VMEM((rows, d_ff), BF16),
            pltpu.VMEM((2,) + square, BF16),
            pltpu.VMEM((2, d_model), F32),
            pltpu.VMEM((rows, src_len), jnp.int32),
            pltpu.SemaphoreType.DMA((SLOTS,)),
            pltpu.SemaphoreType.DMA((AR_CHUNKS,)),
            pltpu.SemaphoreType.DMA((4,)),
            pltpu.SemaphoreType.DMA((2, 2, AR_CHUNKS)),
            pltpu.SemaphoreType.DMA((2, 2, AR_CHUNKS)),
            pltpu.SemaphoreType.DMA((2, 2, AR_CHUNKS)),
            pltpu.SemaphoreType.DMA((2, 2, AR_CHUNKS)),
            pltpu.SemaphoreType.DMA((2, 2, AR_CHUNKS)),
            pltpu.SemaphoreType.DMA((2, 2, AR_CHUNKS)),
            pltpu.SemaphoreType.DMA((AR_CHUNKS,)),
        ],
        compiler_params=pltpu.CompilerParams(vmem_limit_bytes=67_000_000, collective_id=0, has_side_effects=True),
        name="rest_part",
    )(x_in, part, norm_cross.reshape(square), norm_mlp.reshape(square), enc_mask, cross_q, k_flat, v_flat, cross_o, w_gate, w_up, w_down)


def solution(mesh):
    def local_layer(x_in, tok_pos, self_k, self_v, cross_k, cross_v, enc_mask, rel_bias, w_q, w_k, w_v, w_o, cross_q, cross_o, w_gate, w_up, w_down, norm_self, norm_cross, norm_mlp):
        part, new_self_k, new_self_v = self_attention(x_in, norm_self, tok_pos, rel_bias, w_q, w_k, w_v, w_o, self_k, self_v)
        x_out = rest_of_layer(x_in, part, norm_cross, norm_mlp, enc_mask, cross_k, cross_v, cross_q, cross_o, w_gate, w_up, w_down)
        return x_out, new_self_k, new_self_v

    cache_spec = P('dp', None, 'tp', None)
    split_cols = P(None, 'tp')
    split_rows = P('tp', None)
    in_specs = (P('dp', None), P('dp'), cache_spec, cache_spec, cache_spec, cache_spec, P('dp', None), split_cols, split_cols, split_cols, split_cols, split_rows, split_cols, split_rows, split_cols, split_cols, split_rows, P(None), P(None), P(None))
    out_specs = (P('dp', None), cache_spec, cache_spec)
    return jax.shard_map(local_layer, mesh=mesh, in_specs=in_specs, out_specs=out_specs, check_vma=False)
```

```python
import functools
import math
import jax
import jax.numpy as jnp
from jax import lax
from jax.experimental import pallas as pl
from jax.experimental.pallas import tpu as pltpu
from jax.sharding import PartitionSpec as P

BUCKET_EDGES = tuple(int(math.ceil(16.0 * 8.0 ** (bucket_step / 16.0))) for bucket_step in range(1, 16))
NEG_FILL = -1e30
F32 = jnp.float32
BF16 = jnp.bfloat16
ANY = pl.BlockSpec(memory_space=pl.ANY)
VMEM = pl.BlockSpec(memory_space=pltpu.VMEM)
COLS = 256
T_BLOCK = 8


def lay_row(dst, at, norm):
    values = norm[...].astype(F32)
    for i in range(values.shape[0]):
        dst[at:at + 1, i * 128:(i + 1) * 128] = values[i:i + 1, :]


def self_kernel(x_hbm, norm_hbm, pos_hbm, rel_hbm, wq_hbm, wk_hbm, wv_hbm, wo_hbm, k_hbm, v_hbm,
                part_hbm, newk_hbm, newv_hbm,
                xbuf, hbuf, wbuf, kvbuf, sum_ref, q_ref, kn_ref, hit_ref, score_ref, acc_ref,
                norm_ref, nrow, pos_ref, rel_ref,
                x_sem, small_sem, w_sem, kv_sem, out_sem, part_sem, window):
    rows, d_model = xbuf.shape
    n_w = wbuf.shape[0]
    per_mat = n_w // 3
    n_chunk = kvbuf.shape[0] // 2
    n_head, t_len = score_ref.shape[0], score_ref.shape[1]
    inner = acc_ref.shape[0]
    d_head = inner // n_head
    chunk_rows = kvbuf.shape[1]
    sub = d_head // 16
    k_rows = wbuf.shape[1]
    n_wo = wo_hbm.shape[1] // inner

    def w_copy(c):
        src = (wq_hbm, wk_hbm, wv_hbm)[c // per_mat]
        return pltpu.make_async_copy(src.at[pl.ds((c % per_mat) * k_rows, k_rows)], wbuf.at[c], w_sem.at[c])

    def kv_copy(i):
        src = k_hbm if i < n_chunk else v_hbm
        return pltpu.make_async_copy(src.at[pl.ds((i % n_chunk) * chunk_rows, chunk_rows)], kvbuf.at[i], kv_sem.at[i])

    def wo_copies(i):
        return [pltpu.make_async_copy(wo_hbm.at[:, pl.ds(i * inner, inner)], wbuf.at[i], w_sem.at[i])]

    loads = [[w_copy(c)] for c in range(n_w)] + [[kv_copy(i)] for i in range(2 * n_chunk)] + [wo_copies(i) for i in range(n_wo)]
    issued = [0]

    def issue(upto):
        while issued[0] < min(upto, len(loads)):
            for copy in loads[issued[0]]:
                copy.start()
            issued[0] += 1

    x_copy = pltpu.make_async_copy(x_hbm, xbuf, x_sem)
    x_copy.start()
    small = [pltpu.make_async_copy(src, dst, small_sem.at[i]) for i, (src, dst) in enumerate(
        ((pos_hbm, pos_ref), (rel_hbm, rel_ref), (norm_hbm, norm_ref)))]
    for copy in small:
        copy.start()
    issue(window)
    for copy in small:
        copy.wait()

    lay_row(nrow, 0, norm_ref)
    pos = pos_ref[...]
    pos16 = jnp.broadcast_to(pos, (16, rows))

    def set_hit(t, carry):
        hit_ref[t] = jnp.where(pos16 == t, 1.0, 0.0).astype(BF16)
        return carry
    lax.fori_loop(0, t_len, set_hit, 0)

    lane = lax.broadcasted_iota(jnp.int32, (n_head, 128), 1)
    bucket = jnp.full((n_head, 128), 16, jnp.int32)
    for edge in BUCKET_EDGES:
        bucket = bucket + (lane >= edge).astype(jnp.int32)
    bucket = jnp.where(lane < 16, lane, bucket)
    rel = rel_ref[...]
    table = jnp.zeros((n_head, 128), F32)
    for b in range(rel.shape[1]):
        table = jnp.where(bucket == b, rel[:, b:b + 1], table)
    acc_ref[0:n_head, :] = table

    x_copy.wait()
    block = 16
    norm = nrow[0:1, :]

    def norm_rows(i, carry):
        at = pl.ds(pl.multiple_of(i * block, block), block)
        r = xbuf[at, :].astype(F32)
        inv = lax.rsqrt(jnp.mean(r * r, axis=-1, keepdims=True) + 1e-6)
        hbuf[at, :] = (r * inv * norm).astype(BF16)
        return carry
    lax.fori_loop(0, rows // block, norm_rows, 0)

    for c in range(n_w):
        w_copy(c).wait()
        issue(c + 1 + window)
        k = c % per_mat
        for n in range(inner // COLS):
            here = slice(n * COLS, (n + 1) * COLS)
            y = jnp.dot(hbuf[:, k * k_rows:(k + 1) * k_rows], wbuf[c, :, here], preferred_element_type=F32)
            if k > 0:
                y = y + sum_ref[:, here]
            if k < per_mat - 1:
                sum_ref[:, here] = y
                continue
            y = y.astype(BF16).astype(F32).T
            if c < per_mat:
                q_ref[here, :] = y
            else:
                kn_ref[c // per_mat - 1, here, :] = y.astype(BF16)

    def chunk_out(i):
        dst = newk_hbm if i < n_chunk else newv_hbm
        return pltpu.make_async_copy(kvbuf.at[i], dst.at[pl.ds((i % n_chunk) * chunk_rows, chunk_rows)], out_sem.at[i])

    for j in range(n_chunk):
        kv_copy(j).wait()
        issue(n_w + j + 1 + window)

        def k_head(h, carry):
            at = pl.multiple_of(h * d_head, d_head)
            q = q_ref[pl.ds(at, d_head), :]
            kn = kn_ref[0, pl.ds(at, d_head), :].reshape(sub, 16, rows)
            rows_out = []
            for tt in range(T_BLOCK):
                here = pl.ds(pl.multiple_of(tt * inner + at, d_head), d_head)
                old = kvbuf[j, here, :].reshape(sub, 16, rows)
                hit = hit_ref[j * T_BLOCK + tt] != 0
                new = jnp.where(hit[None], kn, old)
                kvbuf[j, here, :] = new.reshape(d_head, rows)
                prod = new.reshape(d_head, rows).astype(F32) * q
                rows_out.append(jnp.sum(prod, axis=0, keepdims=True))
            score_ref[h, j * T_BLOCK:(j + 1) * T_BLOCK, :] = jnp.concatenate(rows_out, axis=0)
            return carry
        lax.fori_loop(0, n_head, k_head, 0)
        chunk_out(j).start(priority=1)

    t_iota = lax.broadcasted_iota(jnp.int32, (t_len, rows), 0)
    causal = t_iota <= pos
    back = jnp.maximum(pos - t_iota, 0)

    def soft_head(h, carry):
        line = jnp.broadcast_to(acc_ref[pl.ds(h, 1), :], (t_len, 128))
        s = score_ref[h] + jnp.take_along_axis(line, back, axis=1)
        s = jnp.where(causal, s, NEG_FILL)
        e = jnp.exp(s - jnp.max(s, axis=0, keepdims=True))
        p = e / jnp.sum(e, axis=0, keepdims=True)
        score_ref[h] = p.astype(BF16).astype(F32)
        return carry
    lax.fori_loop(0, n_head, soft_head, 0)

    acc_ref[...] = jnp.zeros_like(acc_ref)
    for j in range(n_chunk):
        kv_copy(n_chunk + j).wait()
        issue(n_w + n_chunk + j + 1 + window)

        def v_head(h, carry):
            at = pl.multiple_of(h * d_head, d_head)
            vn = kn_ref[1, pl.ds(at, d_head), :].reshape(sub, 16, rows)
            p = score_ref[h, j * T_BLOCK:(j + 1) * T_BLOCK, :]
            acc = acc_ref[pl.ds(at, d_head), :]
            for tt in range(T_BLOCK):
                here = pl.ds(pl.multiple_of(tt * inner + at, d_head), d_head)
                old = kvbuf[n_chunk + j, here, :].reshape(sub, 16, rows)
                hit = hit_ref[j * T_BLOCK + tt] != 0
                new = jnp.where(hit[None], vn, old)
                kvbuf[n_chunk + j, here, :] = new.reshape(d_head, rows)
                acc = acc + new.reshape(d_head, rows).astype(F32) * p[tt:tt + 1, :]
            acc_ref[pl.ds(at, d_head), :] = acc
            return carry
        lax.fori_loop(0, n_head, v_head, 0)
        chunk_out(n_chunk + j).start(priority=1)

    issue(len(loads))
    hbuf[:, 0:inner] = acc_ref[...].T.astype(BF16)
    part_copies = []
    for i in range(n_wo):
        for copy in wo_copies(i):
            copy.wait()
        for r in range(inner // COLS):
            at = i * inner + r * COLS
            y = jnp.dot(hbuf[:, 0:inner], wbuf[i, :, r * COLS:(r + 1) * COLS], preferred_element_type=F32)
            xbuf[:, at:at + COLS] = y.astype(BF16)
        here = pl.ds(i * inner, inner)
        copy = pltpu.make_async_copy(xbuf.at[:, here], part_hbm.at[:, here], part_sem.at[i])
        copy.start()
        part_copies.append(copy)
    for i in range(2 * n_chunk):
        chunk_out(i).wait()
    for copy in part_copies:
        copy.wait()


def self_attention(x_in, norm_self, tok_pos, rel_bias, w_q, w_k, w_v, w_o, self_k, self_v):
    rows, t_len, n_head, d_head = self_k.shape
    d_model = x_in.shape[1]
    inner = n_head * d_head
    flat = (t_len * inner, rows)
    k_flat = self_k.transpose(1, 2, 3, 0).reshape(flat)
    v_flat = self_v.transpose(1, 2, 3, 0).reshape(flat)
    n_w = 3 * (d_model // inner)
    n_chunk = t_len // T_BLOCK
    n_wo = w_o.shape[1] // inner

    def body(*refs):
        self_kernel(*refs, window=8)

    part, new_k, new_v = pl.pallas_call(
        body,
        out_shape=(jax.ShapeDtypeStruct((rows, w_o.shape[1]), BF16),
                   jax.ShapeDtypeStruct(flat, BF16), jax.ShapeDtypeStruct(flat, BF16)),
        in_specs=[ANY] * 10,
        out_specs=(ANY, ANY, ANY),
        scratch_shapes=[
            pltpu.VMEM((rows, d_model), BF16),
            pltpu.VMEM((rows, d_model), BF16),
            pltpu.VMEM((n_w, inner, inner), BF16),
            pltpu.VMEM((2 * n_chunk, T_BLOCK * inner, rows), BF16),
            pltpu.VMEM((rows, inner), F32),
            pltpu.VMEM((inner, rows), F32),
            pltpu.VMEM((2, inner, rows), BF16),
            pltpu.VMEM((t_len, 16, rows), BF16),
            pltpu.VMEM((n_head, t_len, rows), F32),
            pltpu.VMEM((inner, rows), F32),
            pltpu.VMEM((d_model // 128, 128), BF16),
            pltpu.VMEM((1, d_model), F32),
            pltpu.VMEM((1, rows), jnp.int32),
            pltpu.VMEM(rel_bias.shape[::-1], F32),
            pltpu.SemaphoreType.DMA,
            pltpu.SemaphoreType.DMA((3,)),
            pltpu.SemaphoreType.DMA((n_w,)),
            pltpu.SemaphoreType.DMA((2 * n_chunk,)),
            pltpu.SemaphoreType.DMA((2 * n_chunk,)),
            pltpu.SemaphoreType.DMA((n_wo,)),
        ],
        compiler_params=pltpu.CompilerParams(vmem_limit_bytes=66_900_000),
        cost_estimate=pl.CostEstimate(flops=4_400_000_000, bytes_accessed=104_000_000, transcendentals=131_072),
        name="self_part",
    )(x_in, norm_self.reshape(d_model // 128, 128), tok_pos.reshape(1, rows), rel_bias.T, w_q, w_k, w_v, w_o, k_flat, v_flat)

    def unflat(cache):
        return cache.reshape(t_len, n_head, d_head, rows).transpose(3, 0, 1, 2)
    return part, unflat(new_k), unflat(new_v)


SLOTS = 52
FIXED = 8
RING = SLOTS - 2 * FIXED
GROUP = 8
AR_CHUNKS = 4
LANES = 128


def cross_kernel(n_head, x_hbm, part_hbm, ncross_hbm, nmlp_hbm, mask_hbm, cq_hbm, ck_hbm, cv_hbm, co_hbm, wg_hbm, wu_hbm, wd_hbm,
                 out_hbm,
                 ring, pbuf, hbuf, res, xhalf, rx1, tx2, rx2, q_ref, mix_ref, act, norm_in, nrow, mask_ref,
                 ring_sem, load_sem, small_sem, s1_send, s1_recv, s2_send, s2_recv, s3_send, s3_recv, out_sem):
    rows, d_model = hbuf.shape
    half = rows // 2
    part = half // 2
    depth = ring.shape[1]
    inner = q_ref.shape[1]
    d_ff = act.shape[1]
    width = d_model // AR_CHUNKS
    MESH = pl.DeviceIdType.MESH

    me = lax.axis_index("tp")
    core = lax.rem(me, 2)
    chip = me // 2
    partner = {"tp": chip * 2 + (1 - core)}
    across = {"tp": (1 - chip) * 2 + core}

    def mine(at, n):
        return pl.ds(pl.multiple_of(core * half + at, 16), n)

    def theirs(at, n):
        return pl.ds(pl.multiple_of((1 - core) * half + at, 16), n)

    def piece(j):
        return pl.ds(j * width, width)

    per_step = GROUP * inner // depth
    n_step = rows // GROUP
    n_kv = 2 * per_step * n_step
    n_gu = d_ff // LANES
    n_d = d_model // LANES
    o_blocks = depth // inner
    fixed_d = 2 * FIXED

    def copy_in(src, slot, used=None):
        dst = ring.at[slot] if used is None else ring.at[slot, used]
        pltpu.make_async_copy(src, dst, ring_sem.at[slot]).start()

    def landed(slot, used=depth):
        pltpu.make_async_copy(ck_hbm.at[pl.ds(0, used)], ring.at[slot, pl.ds(0, used)], ring_sem.at[slot]).wait()

    def cols(ref, i):
        return ref.at[:, pl.ds(i * LANES if isinstance(i, int) else pl.multiple_of(i * LANES, LANES), LANES)]

    def ring_slot(n):
        return 2 * FIXED + n % RING

    def group_of(step):
        per_half, u = n_step // 2, step % (n_step // 2)
        return (step // per_half) * (part // GROUP) + u + (u // (part // GROUP)) * (part // GROUP)

    def issue_step(step):
        for k in range(2 * per_step):
            src = ck_hbm if k < per_step else cv_hbm
            at = (group_of(step) * per_step + k % per_step) * depth
            at = at if isinstance(at, int) else pl.multiple_of(at, depth)
            copy_in(src.at[pl.ds(at, depth)], ring_slot(step * 2 * per_step + k))

    def issue_gu(i):
        copy_in(cols(wg_hbm, i), ring_slot(n_kv + 2 * i))
        copy_in(cols(wu_hbm, i), ring_slot(n_kv + 2 * i + 1))

    def d_slot(i):
        if isinstance(i, int) and i < fixed_d:
            return i
        return ring_slot(n_kv + 2 * n_gu + i - fixed_d)

    def issue_d(i):
        copy_in(cols(wd_hbm, i), d_slot(i), pl.ds(0, d_ff))

    def to_partner(a, h, j, at, n):
        return pltpu.make_async_remote_copy(
            src_ref=pbuf.at[theirs(at, n), piece(j)], dst_ref=rx1.at[a % 2, pl.ds(at, n), piece(j)],
            send_sem=s1_send.at[a % 2, h, j], recv_sem=s1_recv.at[a % 2, h, j], device_id=partner, device_id_type=MESH)

    def to_across(a, h, j, at, n):
        return pltpu.make_async_remote_copy(
            src_ref=tx2.at[a % 2, pl.ds(at, n), piece(j)], dst_ref=rx2.at[a % 2, pl.ds(at, n), piece(j)],
            send_sem=s2_send.at[a % 2, h, j], recv_sem=s2_recv.at[a % 2, h, j], device_id=across, device_id_type=MESH)

    def blocks(at, n, fn):
        def body(i, carry):
            fn(pl.multiple_of(at + i * 16, 16))
            return carry
        lax.fori_loop(0, n // 16, body, 0)

    def chip_sum(a, h, j, at, n):
        to_partner(a, h, j, at, n).wait_recv()

        def add(r):
            own = pbuf[mine(r, 16), piece(j)].astype(F32)
            tx2[a % 2, pl.ds(r, 16), piece(j)] = (own + rx1[a % 2, pl.ds(r, 16), piece(j)].astype(F32)).astype(BF16)
        blocks(at, n, add)
        to_across(a, h, j, at, n).start()

    def full_sum(a, h, j, at, n):
        to_across(a, h, j, at, n).wait_recv()

        def add(r):
            both = tx2[a % 2, pl.ds(r, 16), piece(j)].astype(F32) + rx2[a % 2, pl.ds(r, 16), piece(j)].astype(F32)
            res[pl.ds(r, 16), piece(j)] = res[pl.ds(r, 16), piece(j)] + both
        blocks(at, n, add)

    def sent(a, h, at, n):
        for j in range(AR_CHUNKS):
            to_partner(a, h, j, at, n).wait_send()
            to_across(a, h, j, at, n).wait_send()

    def rows_back(a, h, i):
        at = mine(h * part + i * 16, 16)
        return pltpu.make_async_remote_copy(
            src_ref=hbuf.at[at], dst_ref=hbuf.at[at], send_sem=s3_send.at[a % 2, h, i],
            recv_sem=s3_recv.at[a % 2, h, i], device_id=partner, device_id_type=MESH)

    def normalise(a, h):
        norm = nrow[a:a + 1, :]
        for i in range(part // 16):
            r = res[h * part + i * 16:h * part + (i + 1) * 16, :]
            inv = lax.rsqrt(jnp.mean(r * r, axis=-1, keepdims=True) + 1e-6)
            hbuf[mine(h * part + i * 16, 16), :] = (r * inv * norm).astype(BF16)
            rows_back(a, h, i).start()

    def all_rows(a, h):
        for i in range(part // 16):
            rows_back(a, h, i).wait()

    pieces = range(AR_CHUNKS)
    halves = range(2)
    first = [pltpu.make_async_copy(part_hbm.at[:, piece(j)], pbuf.at[:, piece(j)], load_sem.at[j]) for j in pieces]
    for copy in first:
        copy.start()
    small = [pltpu.make_async_copy(src, dst, small_sem.at[i]) for i, (src, dst) in enumerate(
        ((x_hbm.at[mine(0, half)], xhalf), (ncross_hbm, norm_in.at[0]), (nmlp_hbm, norm_in.at[1]), (mask_hbm, mask_ref)))]
    for copy in small:
        copy.start()
    barrier = pltpu.get_barrier_semaphore()
    for other in (partner, across):
        pl.semaphore_signal(barrier, inc=1, device_id=other, device_id_type=MESH)
    pl.semaphore_wait(barrier, 2)

    for j in pieces:
        first[j].wait()
        to_partner(0, 0, j, 0, part).start()
    for j in pieces:
        to_partner(0, 1, j, part, part).start()
    for i in range(FIXED):
        copy_in(cols(cq_hbm, i), i)
    for step in range(RING // (2 * per_step)):
        issue_step(step)
    for i in range(FIXED):
        for r in range(o_blocks):
            copy_in(cols(co_hbm, i * o_blocks + r), FIXED + i, pl.ds(r * inner, inner))
    for h in halves:
        for j in pieces:
            chip_sum(0, h, j, h * part, part)
    for copy in small:
        copy.wait()
    lay_row(nrow, 0, norm_in.at[0])
    lay_row(nrow, 1, norm_in.at[1])
    blocks(0, half, lambda r: res.__setitem__((pl.ds(r, 16), slice(None)), xhalf[pl.ds(r, 16), :].astype(F32)))

    def beside(a, b, used=depth):
        return jnp.concatenate([ring[a, 0:used, :], ring[b, 0:used, :]], axis=1)

    def both_cores(ref, h):
        return jnp.concatenate([ref[h * part:(h + 1) * part, :], ref[half + h * part:half + (h + 1) * part, :]], axis=0)

    def project_q(h):
        lhs = both_cores(hbuf, h)
        for i in range(FIXED // 2):
            if h == 0:
                landed(2 * i)
                landed(2 * i + 1)
            y = jnp.dot(lhs, beside(2 * i, 2 * i + 1), preferred_element_type=F32).astype(BF16).astype(F32)
            here = slice(2 * i * LANES, (2 * i + 2) * LANES)
            q_ref[h * part:(h + 1) * part, here] = y[0:part]
            q_ref[half + h * part:half + (h + 1) * part, here] = y[part:]

    own_head = (lax.broadcasted_iota(jnp.int32, (n_head, inner), 1) // (inner // n_head)
                == lax.broadcasted_iota(jnp.int32, (n_head, inner), 0))
    in_slot = GROUP // per_step

    def attend_step(step, carry):
        at = pl.ds(pl.multiple_of(group_of(step) * GROUP, GROUP), GROUP)
        ka, kb, va, vb = [ring_slot(step * 2 * per_step + k) for k in range(4)]
        q8 = q_ref[at, :]
        m8 = mask_ref[at, :]

        def spread(r):
            return jnp.where(own_head, jnp.broadcast_to(q8[r:r + 1, :], (n_head, inner)), 0.0).astype(BF16)

        def rows_of(a, b, r):
            here = pl.ds(r * inner, inner)
            return jnp.concatenate([ring[a, here, :], ring[b, here, :]], axis=1)
        landed(ka)
        landed(kb)
        scores = [None] * GROUP
        for r in range(in_slot):
            s = jnp.dot(jnp.concatenate([spread(r), spread(r + in_slot)], axis=0), rows_of(ka, kb, r), preferred_element_type=F32)
            scores[r] = jnp.where(m8[r:r + 1, :] != 0, s[0:n_head, 0:LANES], NEG_FILL)
            scores[r + in_slot] = jnp.where(m8[r + in_slot:r + in_slot + 1, :] != 0, s[n_head:, LANES:], NEG_FILL)
        s = jnp.concatenate(scores, axis=0)
        e = jnp.exp(s - jnp.max(s, axis=1, keepdims=True))
        p = (e / jnp.sum(e, axis=1, keepdims=True)).astype(BF16)
        landed(va)
        landed(vb)
        none = jnp.zeros((n_head, LANES), BF16)
        mixed = [None] * GROUP
        for r in range(in_slot):
            pa = p[r * n_head:(r + 1) * n_head, :]
            pb = p[(r + in_slot) * n_head:(r + in_slot + 1) * n_head, :]
            lhs = jnp.concatenate([jnp.concatenate([pa, none], axis=1), jnp.concatenate([none, pb], axis=1)], axis=0)
            y = lax.dot_general(lhs, rows_of(va, vb, r), (((1,), (1,)), ((), ())), preferred_element_type=F32)
            mixed[r] = jnp.sum(jnp.where(own_head, y[0:n_head], 0.0), axis=0, keepdims=True)
            mixed[r + in_slot] = jnp.sum(jnp.where(own_head, y[n_head:], 0.0), axis=0, keepdims=True)
        mix_ref[at, :] = jnp.concatenate(mixed, axis=0)

        ahead = RING // (2 * per_step)

        @pl.when(step + ahead < n_step)
        def _():
            issue_step(step + ahead)

        @pl.when(step + ahead >= n_step)
        def _():
            for k in range(per_step):
                issue_gu((step + ahead - n_step) * per_step + k)
        return carry

    o_cols = o_blocks * LANES
    per_piece_o = width // o_cols

    def project_o(h, after):
        lhs = both_cores(mix_ref, h).astype(BF16)
        for n in range(FIXED):
            if h == 0:
                landed(FIXED + n)
            w = jnp.concatenate([ring[FIXED + n, r * inner:(r + 1) * inner, :] for r in range(o_blocks)], axis=1)
            y = jnp.dot(lhs, w, preferred_element_type=F32).astype(BF16)
            here = slice(n * o_cols, (n + 1) * o_cols)
            pbuf[h * part:(h + 1) * part, here] = y[0:part]
            pbuf[half + h * part:half + (h + 1) * part, here] = y[part:]
            if n % per_piece_o == per_piece_o - 1:
                j = n // per_piece_o
                to_partner(1, h, j, h * part, part).start()
                if after and j > 0:
                    chip_sum(1, h, j - 1, h * part, part)
        if after:
            chip_sum(1, h, AR_CHUNKS - 1, h * part, part)

    for j in pieces:
        full_sum(0, 0, j, 0, part)
    normalise(0, 0)
    all_rows(0, 0)
    project_q(0)
    lax.fori_loop(0, n_step // 2, attend_step, 0)
    sent(0, 0, 0, part)
    project_o(0, False)
    for j in pieces:
        full_sum(0, 1, j, part, part)
    normalise(0, 1)
    for j in pieces:
        chip_sum(1, 0, j, 0, part)
    all_rows(0, 1)
    project_q(1)
    lax.fori_loop(n_step // 2, n_step, attend_step, 0)
    sent(0, 1, part, part)
    project_o(1, True)
    for i in range(fixed_d):
        issue_d(i)
    for j in pieces:
        full_sum(1, 0, j, 0, part)
    normalise(1, 0)
    for j in pieces:
        full_sum(1, 1, j, part, part)
    normalise(1, 1)
    for h in halves:
        all_rows(1, h)
        sent(1, h, h * part, part)

    root = math.sqrt(2.0 / math.pi)
    gu_ahead = (n_kv + 2 * n_gu - (n_kv + RING)) // 2

    def gate_up(i, carry):
        a, b = ring_slot(n_kv + 2 * i), ring_slot(n_kv + 2 * i + 1)
        landed(a)
        landed(b)
        y = jnp.dot(hbuf[...], beside(a, b), preferred_element_type=F32)
        u = y[:, 0:LANES]
        gelu = 0.5 * u * (1.0 + jnp.tanh(root * (u + 0.044715 * (u * u * u))))
        act[:, pl.ds(pl.multiple_of(i * LANES, LANES), LANES)] = (gelu * y[:, LANES:]).astype(BF16)

        @pl.when(i < gu_ahead)
        def _():
            issue_gu(i + RING // 2)

        @pl.when((i >= gu_ahead) & (i < gu_ahead + (n_d - fixed_d) // 2))
        def _():
            issue_d(fixed_d + 2 * (i - gu_ahead))
            issue_d(fixed_d + 2 * (i - gu_ahead) + 1)
        return carry
    lax.fori_loop(0, n_gu, gate_up, 0)

    per_piece = width // (2 * LANES)

    def out_back(j):
        return pltpu.make_async_remote_copy(
            src_ref=hbuf.at[mine(0, half), piece(j)], dst_ref=hbuf.at[mine(0, half), piece(j)], send_sem=s3_send.at[0, 0, j],
            recv_sem=s3_recv.at[0, 0, j], device_id=partner, device_id_type=MESH)

    for c in pieces:
        def down(i, carry):
            n = c * per_piece + i
            if (c + 1) * per_piece * 2 <= fixed_d:
                a, b = 2 * n, 2 * n + 1
            else:
                a = ring_slot(n_kv + 2 * n_gu + 2 * n - fixed_d)
                b = ring_slot(n_kv + 2 * n_gu + 2 * n + 1 - fixed_d)
            landed(a, d_ff)
            landed(b, d_ff)
            y = jnp.dot(act[...], beside(a, b, d_ff), preferred_element_type=F32)
            pbuf[:, pl.ds(pl.multiple_of(n * 2 * LANES, 2 * LANES), 2 * LANES)] = y.astype(BF16)
            return carry
        lax.fori_loop(0, per_piece, down, 0)
        to_partner(2, 0, c, 0, half).start()
        if c > 0:
            chip_sum(2, 0, c - 1, 0, half)
    chip_sum(2, 0, AR_CHUNKS - 1, 0, half)

    def out_copy(j):
        return pltpu.make_async_copy(hbuf.at[:, piece(j)], out_hbm.at[:, piece(j)], out_sem.at[j])

    for j in pieces:
        to_across(2, 0, j, 0, half).wait_recv()

        def add(r):
            both = tx2[0, pl.ds(r, 16), piece(j)].astype(F32) + rx2[0, pl.ds(r, 16), piece(j)].astype(F32)
            hbuf[mine(r, 16), piece(j)] = (res[pl.ds(r, 16), piece(j)] + both).astype(BF16)
        blocks(0, half, add)
        out_back(j).start()
        if j > 0:
            out_back(j - 1).wait()
            out_copy(j - 1).start()
    out_back(AR_CHUNKS - 1).wait()
    out_copy(AR_CHUNKS - 1).start()
    sent(2, 0, 0, half)
    for j in pieces:
        out_copy(j).wait()


def rest_of_layer(x_in, part, norm_cross, norm_mlp, enc_mask, cross_k, cross_v, cross_q, cross_o, w_gate, w_up, w_down):
    rows, d_model = x_in.shape
    _, src_len, n_head, d_head = cross_k.shape
    inner = n_head * d_head
    d_ff = w_gate.shape[1]
    half = rows // 2
    flat = (rows * inner, src_len)
    k_flat = cross_k.transpose(0, 2, 3, 1).reshape(flat)
    v_flat = cross_v.transpose(0, 2, 3, 1).reshape(flat)
    square = (d_model // 128, 128)
    return pl.pallas_call(
        functools.partial(cross_kernel, n_head),
        out_shape=jax.ShapeDtypeStruct((rows, d_model), BF16),
        in_specs=[ANY] * 12,
        out_specs=ANY,
        scratch_shapes=[
            pltpu.VMEM((SLOTS, d_model, LANES), BF16),
            pltpu.VMEM((rows, d_model), BF16),
            pltpu.VMEM((rows, d_model), BF16),
            pltpu.VMEM((half, d_model), F32),
            pltpu.VMEM((half, d_model), BF16),
            pltpu.VMEM((2, half, d_model), BF16),
            pltpu.VMEM((2, half, d_model), BF16),
            pltpu.VMEM((2, half, d_model), BF16),
            pltpu.VMEM((rows, inner), F32),
            pltpu.VMEM((rows, inner), F32),
            pltpu.VMEM((rows, d_ff), BF16),
            pltpu.VMEM((2,) + square, BF16),
            pltpu.VMEM((2, d_model), F32),
            pltpu.VMEM((rows, src_len), jnp.int32),
            pltpu.SemaphoreType.DMA((SLOTS,)),
            pltpu.SemaphoreType.DMA((AR_CHUNKS,)),
            pltpu.SemaphoreType.DMA((4,)),
            pltpu.SemaphoreType.DMA((2, 2, AR_CHUNKS)),
            pltpu.SemaphoreType.DMA((2, 2, AR_CHUNKS)),
            pltpu.SemaphoreType.DMA((2, 2, AR_CHUNKS)),
            pltpu.SemaphoreType.DMA((2, 2, AR_CHUNKS)),
            pltpu.SemaphoreType.DMA((2, 2, AR_CHUNKS)),
            pltpu.SemaphoreType.DMA((2, 2, AR_CHUNKS)),
            pltpu.SemaphoreType.DMA((AR_CHUNKS,)),
        ],
        compiler_params=pltpu.CompilerParams(vmem_limit_bytes=67_000_000, collective_id=0, has_side_effects=True),
        name="rest_part",
    )(x_in, part, norm_cross.reshape(square), norm_mlp.reshape(square), enc_mask, cross_q, k_flat, v_flat, cross_o, w_gate, w_up, w_down)


def solution(mesh):
    def local_layer(x_in, tok_pos, self_k, self_v, cross_k, cross_v, enc_mask, rel_bias, w_q, w_k, w_v, w_o, cross_q, cross_o, w_gate, w_up, w_down, norm_self, norm_cross, norm_mlp):
        part, new_self_k, new_self_v = self_attention(x_in, norm_self, tok_pos, rel_bias, w_q, w_k, w_v, w_o, self_k, self_v)
        x_out = rest_of_layer(x_in, part, norm_cross, norm_mlp, enc_mask, cross_k, cross_v, cross_q, cross_o, w_gate, w_up, w_down)
        return x_out, new_self_k, new_self_v

    cache_spec = P('dp', None, 'tp', None)
    split_cols = P(None, 'tp')
    split_rows = P('tp', None)
    in_specs = (P('dp', None), P('dp'), cache_spec, cache_spec, cache_spec, cache_spec, P('dp', None), split_cols, split_cols, split_cols, split_cols, split_rows, split_cols, split_rows, split_cols, split_cols, split_rows, P(None), P(None), P(None))
    out_specs = (P('dp', None), cache_spec, cache_spec)
    return jax.shard_map(local_layer, mesh=mesh, in_specs=in_specs, out_specs=out_specs, check_vma=False)
```

```python
import functools
import math
import jax
import jax.numpy as jnp
from jax import lax
from jax.experimental import pallas as pl
from jax.experimental.pallas import tpu as pltpu
from jax.sharding import PartitionSpec as P

BUCKET_EDGES = tuple(int(math.ceil(16.0 * 8.0 ** (bucket_step / 16.0))) for bucket_step in range(1, 16))
NEG_FILL = -1e30
F32 = jnp.float32
BF16 = jnp.bfloat16
ANY = pl.BlockSpec(memory_space=pl.ANY)
VMEM = pl.BlockSpec(memory_space=pltpu.VMEM)
COLS = 256
T_BLOCK = 8


def lay_row(dst, at, norm):
    values = norm[...].astype(F32)
    for i in range(values.shape[0]):
        dst[at:at + 1, i * 128:(i + 1) * 128] = values[i:i + 1, :]


def self_kernel(x_hbm, norm_hbm, pos_hbm, rel_hbm, wq_hbm, wk_hbm, wv_hbm, wo_hbm, k_hbm, v_hbm,
                part_hbm, newk_hbm, newv_hbm,
                xbuf, hbuf, wbuf, kvbuf, sum_ref, q_ref, kn_ref, hit_ref, score_ref, acc_ref,
                norm_ref, nrow, pos_ref, rel_ref,
                x_sem, small_sem, w_sem, kv_sem, out_sem, part_sem, window):
    rows, d_model = xbuf.shape
    n_w = wbuf.shape[0]
    per_mat = n_w // 3
    n_chunk = kvbuf.shape[0] // 2
    n_head, t_len = score_ref.shape[0], score_ref.shape[1]
    inner = acc_ref.shape[0]
    d_head = inner // n_head
    chunk_rows = kvbuf.shape[1]
    sub = d_head // 16
    k_rows = wbuf.shape[1]
    n_wo = wo_hbm.shape[1] // inner

    def w_copy(c):
        src = (wq_hbm, wk_hbm, wv_hbm)[c // per_mat]
        return pltpu.make_async_copy(src.at[pl.ds((c % per_mat) * k_rows, k_rows)], wbuf.at[c], w_sem.at[c])

    def kv_copy(i):
        src = k_hbm if i < n_chunk else v_hbm
        return pltpu.make_async_copy(src.at[pl.ds((i % n_chunk) * chunk_rows, chunk_rows)], kvbuf.at[i], kv_sem.at[i])

    def wo_copies(i):
        return [pltpu.make_async_copy(wo_hbm.at[:, pl.ds(i * inner, inner)], wbuf.at[i], w_sem.at[i])]

    loads = [[w_copy(c)] for c in range(n_w)] + [[kv_copy(i)] for i in range(2 * n_chunk)] + [wo_copies(i) for i in range(n_wo)]
    issued = [0]

    def issue(upto):
        while issued[0] < min(upto, len(loads)):
            for copy in loads[issued[0]]:
                copy.start()
            issued[0] += 1

    x_copy = pltpu.make_async_copy(x_hbm, xbuf, x_sem)
    x_copy.start()
    small = [pltpu.make_async_copy(src, dst, small_sem.at[i]) for i, (src, dst) in enumerate(
        ((pos_hbm, pos_ref), (rel_hbm, rel_ref), (norm_hbm, norm_ref)))]
    for copy in small:
        copy.start()
    issue(window)
    for copy in small:
        copy.wait()

    lay_row(nrow, 0, norm_ref)
    pos = pos_ref[...]
    pos16 = jnp.broadcast_to(pos, (16, rows))

    def set_hit(t, carry):
        hit_ref[t] = jnp.where(pos16 == t, 1.0, 0.0).astype(BF16)
        return carry
    lax.fori_loop(0, t_len, set_hit, 0)

    lane = lax.broadcasted_iota(jnp.int32, (n_head, 128), 1)
    bucket = jnp.full((n_head, 128), 16, jnp.int32)
    for edge in BUCKET_EDGES:
        bucket = bucket + (lane >= edge).astype(jnp.int32)
    bucket = jnp.where(lane < 16, lane, bucket)
    rel = rel_ref[...]
    table = jnp.zeros((n_head, 128), F32)
    for b in range(rel.shape[1]):
        table = jnp.where(bucket == b, rel[:, b:b + 1], table)
    acc_ref[0:n_head, :] = table

    x_copy.wait()
    block = 16
    norm = nrow[0:1, :]

    def norm_rows(i, carry):
        at = pl.ds(pl.multiple_of(i * block, block), block)
        r = xbuf[at, :].astype(F32)
        inv = lax.rsqrt(jnp.mean(r * r, axis=-1, keepdims=True) + 1e-6)
        hbuf[at, :] = (r * inv * norm).astype(BF16)
        return carry
    lax.fori_loop(0, rows // block, norm_rows, 0)

    for c in range(n_w):
        w_copy(c).wait()
        issue(c + 1 + window)
        k = c % per_mat
        for n in range(inner // COLS):
            here = slice(n * COLS, (n + 1) * COLS)
            y = jnp.dot(hbuf[:, k * k_rows:(k + 1) * k_rows], wbuf[c, :, here], preferred_element_type=F32)
            if k > 0:
                y = y + sum_ref[:, here]
            if k < per_mat - 1:
                sum_ref[:, here] = y
                continue
            y = y.astype(BF16).astype(F32).T
            if c < per_mat:
                q_ref[here, :] = y
            else:
                kn_ref[c // per_mat - 1, here, :] = y.astype(BF16)

    def chunk_out(i):
        dst = newk_hbm if i < n_chunk else newv_hbm
        return pltpu.make_async_copy(kvbuf.at[i], dst.at[pl.ds((i % n_chunk) * chunk_rows, chunk_rows)], out_sem.at[i])

    for j in range(n_chunk):
        kv_copy(j).wait()
        issue(n_w + j + 1 + window)

        def k_head(h, carry):
            at = pl.multiple_of(h * d_head, d_head)
            q = q_ref[pl.ds(at, d_head), :]
            kn = kn_ref[0, pl.ds(at, d_head), :].reshape(sub, 16, rows)
            rows_out = []
            for tt in range(T_BLOCK):
                here = pl.ds(pl.multiple_of(tt * inner + at, d_head), d_head)
                old = kvbuf[j, here, :].reshape(sub, 16, rows)
                hit = hit_ref[j * T_BLOCK + tt] != 0
                new = jnp.where(hit[None], kn, old)
                kvbuf[j, here, :] = new.reshape(d_head, rows)
                prod = new.reshape(d_head, rows).astype(F32) * q
                rows_out.append(jnp.sum(prod, axis=0, keepdims=True))
            score_ref[h, j * T_BLOCK:(j + 1) * T_BLOCK, :] = jnp.concatenate(rows_out, axis=0)
            return carry
        lax.fori_loop(0, n_head, k_head, 0)
        chunk_out(j).start(priority=1)

    t_iota = lax.broadcasted_iota(jnp.int32, (t_len, rows), 0)
    causal = t_iota <= pos
    back = jnp.maximum(pos - t_iota, 0)

    def soft_head(h, carry):
        line = jnp.broadcast_to(acc_ref[pl.ds(h, 1), :], (t_len, 128))
        s = score_ref[h] + jnp.take_along_axis(line, back, axis=1)
        s = jnp.where(causal, s, NEG_FILL)
        e = jnp.exp(s - jnp.max(s, axis=0, keepdims=True))
        p = e / jnp.sum(e, axis=0, keepdims=True)
        score_ref[h] = p.astype(BF16).astype(F32)
        return carry
    lax.fori_loop(0, n_head, soft_head, 0)

    acc_ref[...] = jnp.zeros_like(acc_ref)
    for j in range(n_chunk):
        kv_copy(n_chunk + j).wait()
        issue(n_w + n_chunk + j + 1 + window)

        def v_head(h, carry):
            at = pl.multiple_of(h * d_head, d_head)
            vn = kn_ref[1, pl.ds(at, d_head), :].reshape(sub, 16, rows)
            p = score_ref[h, j * T_BLOCK:(j + 1) * T_BLOCK, :]
            acc = acc_ref[pl.ds(at, d_head), :]
            for tt in range(T_BLOCK):
                here = pl.ds(pl.multiple_of(tt * inner + at, d_head), d_head)
                old = kvbuf[n_chunk + j, here, :].reshape(sub, 16, rows)
                hit = hit_ref[j * T_BLOCK + tt] != 0
                new = jnp.where(hit[None], vn, old)
                kvbuf[n_chunk + j, here, :] = new.reshape(d_head, rows)
                acc = acc + new.reshape(d_head, rows).astype(F32) * p[tt:tt + 1, :]
            acc_ref[pl.ds(at, d_head), :] = acc
            return carry
        lax.fori_loop(0, n_head, v_head, 0)
        chunk_out(n_chunk + j).start(priority=1)

    issue(len(loads))
    hbuf[:, 0:inner] = acc_ref[...].T.astype(BF16)
    part_copies = []
    for i in range(n_wo):
        for copy in wo_copies(i):
            copy.wait()
        for r in range(inner // COLS):
            at = i * inner + r * COLS
            y = jnp.dot(hbuf[:, 0:inner], wbuf[i, :, r * COLS:(r + 1) * COLS], preferred_element_type=F32)
            xbuf[:, at:at + COLS] = y.astype(BF16)
        here = pl.ds(i * inner, inner)
        copy = pltpu.make_async_copy(xbuf.at[:, here], part_hbm.at[:, here], part_sem.at[i])
        copy.start()
        part_copies.append(copy)
    for i in range(2 * n_chunk):
        chunk_out(i).wait()
    for copy in part_copies:
        copy.wait()


def self_attention(x_in, norm_self, tok_pos, rel_bias, w_q, w_k, w_v, w_o, self_k, self_v):
    rows, t_len, n_head, d_head = self_k.shape
    d_model = x_in.shape[1]
    inner = n_head * d_head
    flat = (t_len * inner, rows)
    k_flat = self_k.transpose(1, 2, 3, 0).reshape(flat)
    v_flat = self_v.transpose(1, 2, 3, 0).reshape(flat)
    n_w = 3 * (d_model // inner)
    n_chunk = t_len // T_BLOCK
    n_wo = w_o.shape[1] // inner

    def body(*refs):
        self_kernel(*refs, window=8)

    part, new_k, new_v = pl.pallas_call(
        body,
        out_shape=(jax.ShapeDtypeStruct((rows, w_o.shape[1]), BF16),
                   jax.ShapeDtypeStruct(flat, BF16), jax.ShapeDtypeStruct(flat, BF16)),
        in_specs=[ANY] * 10,
        out_specs=(ANY, ANY, ANY),
        scratch_shapes=[
            pltpu.VMEM((rows, d_model), BF16),
            pltpu.VMEM((rows, d_model), BF16),
            pltpu.VMEM((n_w, inner, inner), BF16),
            pltpu.VMEM((2 * n_chunk, T_BLOCK * inner, rows), BF16),
            pltpu.VMEM((rows, inner), F32),
            pltpu.VMEM((inner, rows), F32),
            pltpu.VMEM((2, inner, rows), BF16),
            pltpu.VMEM((t_len, 16, rows), BF16),
            pltpu.VMEM((n_head, t_len, rows), F32),
            pltpu.VMEM((inner, rows), F32),
            pltpu.VMEM((d_model // 128, 128), BF16),
            pltpu.VMEM((1, d_model), F32),
            pltpu.VMEM((1, rows), jnp.int32),
            pltpu.VMEM(rel_bias.shape[::-1], F32),
            pltpu.SemaphoreType.DMA,
            pltpu.SemaphoreType.DMA((3,)),
            pltpu.SemaphoreType.DMA((n_w,)),
            pltpu.SemaphoreType.DMA((2 * n_chunk,)),
            pltpu.SemaphoreType.DMA((2 * n_chunk,)),
            pltpu.SemaphoreType.DMA((n_wo,)),
        ],
        compiler_params=pltpu.CompilerParams(vmem_limit_bytes=66_900_000),
        cost_estimate=pl.CostEstimate(flops=4_400_000_000, bytes_accessed=104_000_000, transcendentals=131_072),
        name="self_part",
    )(x_in, norm_self.reshape(d_model // 128, 128), tok_pos.reshape(1, rows), rel_bias.T, w_q, w_k, w_v, w_o, k_flat, v_flat)

    def unflat(cache):
        return cache.reshape(t_len, n_head, d_head, rows).transpose(3, 0, 1, 2)
    return part, unflat(new_k), unflat(new_v)


RING = 20
WIDE = 1024
GROUP = 8
AR_CHUNKS = 4
LANES = 128


def cross_kernel(n_head, x_hbm, part_hbm, ncross_hbm, nmlp_hbm, mask_hbm, cq_hbm, ck_hbm, cv_hbm, co_hbm, wg_hbm, wu_hbm, wd_hbm,
                 out_hbm,
                 ring, pw, gw, pbuf, hbuf, res, xhalf, rx1, tx2, rx2, q_ref, mix_ref, act, norm_in, nrow, mask_ref,
                 ring_sem, p_sem, g_sem, load_sem, small_sem, s1_send, s1_recv, s2_send, s2_recv, s3_send, s3_recv, out_sem):
    rows, d_model = hbuf.shape
    half = rows // 2
    part = half // 2
    depth = ring.shape[1]
    inner = q_ref.shape[1]
    d_ff = act.shape[1]
    width = d_model // AR_CHUNKS
    MESH = pl.DeviceIdType.MESH

    me = lax.axis_index("tp")
    core = lax.rem(me, 2)
    chip = me // 2
    partner = {"tp": chip * 2 + (1 - core)}
    across = {"tp": (1 - chip) * 2 + core}

    def mine(at, n):
        return pl.ds(pl.multiple_of(core * half + at, 16), n)

    def theirs(at, n):
        return pl.ds(pl.multiple_of((1 - core) * half + at, 16), n)

    def piece(j):
        return pl.ds(j * width, width)

    per_step = GROUP * inner // depth
    n_step = rows // GROUP
    ahead = RING // (2 * per_step)
    n_sq = pw.shape[0] // 2
    g_rows, g_cols = gw.shape[1:]
    g_cut = d_model // g_rows
    n_pair = gw.shape[0] // (2 * g_cut)

    def copy_in(src, slot, used=None):
        dst = ring.at[slot] if used is None else ring.at[slot, used]
        pltpu.make_async_copy(src, dst, ring_sem.at[slot]).start()

    def landed(slot, used=depth):
        pltpu.make_async_copy(ck_hbm.at[pl.ds(0, used)], ring.at[slot, pl.ds(0, used)], ring_sem.at[slot]).wait()

    def ring_slot(n):
        return n % RING

    def group_of(step):
        per_half, u = n_step // 2, step % (n_step // 2)
        return (step // per_half) * (part // GROUP) + u + (u // (part // GROUP)) * (part // GROUP)

    def issue_step(step):
        for k in range(2 * per_step):
            src = ck_hbm if k < per_step else cv_hbm
            at = (group_of(step) * per_step + k % per_step) * depth
            at = at if isinstance(at, int) else pl.multiple_of(at, depth)
            copy_in(src.at[pl.ds(at, depth)], ring_slot(step * 2 * per_step + k))

    def q_copy(k):
        return pltpu.make_async_copy(cq_hbm.at[pl.ds(k * WIDE, WIDE)], pw.at[k], p_sem.at[k])

    def o_copy(i):
        return pltpu.make_async_copy(co_hbm.at[:, pl.ds(i * WIDE, WIDE)], pw.at[n_sq + i], p_sem.at[n_sq + i])

    def gu_square(i):
        src = wg_hbm if i < n_sq else wu_hbm
        return pltpu.make_async_copy(src.at[pl.ds((i % n_sq) * WIDE, WIDE), pl.ds(0, WIDE)], pw.at[i], p_sem.at[i])

    def gu_tall(pair, i):
        src = wg_hbm if i < g_cut else wu_hbm
        slot = (pair % n_pair) * 2 * g_cut + i
        return pltpu.make_async_copy(src.at[pl.ds((i % g_cut) * g_rows, g_rows), pl.ds(WIDE + pair * g_cols, g_cols)],
                                     gw.at[slot], g_sem.at[slot])

    d_cut = -(-d_ff // WIDE)
    d_narrow = 2 * WIDE // LANES

    def d_square(c, i):
        slot = (c - 2) * d_cut + i
        n = min(WIDE, d_ff - i * WIDE)
        return pltpu.make_async_copy(wd_hbm.at[pl.ds(i * WIDE, n), pl.ds(c * WIDE, WIDE)],
                                     pw.at[slot, pl.ds(0, n)], p_sem.at[slot])

    def issue_d(i):
        copy_in(wd_hbm.at[:, pl.ds(i * LANES, LANES)], i, pl.ds(0, d_ff))

    def to_partner(a, h, j, at, n):
        return pltpu.make_async_remote_copy(
            src_ref=pbuf.at[theirs(at, n), piece(j)], dst_ref=rx1.at[a % 2, pl.ds(at, n), piece(j)],
            send_sem=s1_send.at[a % 2, h, j], recv_sem=s1_recv.at[a % 2, h, j], device_id=partner, device_id_type=MESH)

    def to_across(a, h, j, at, n):
        return pltpu.make_async_remote_copy(
            src_ref=tx2.at[a % 2, pl.ds(at, n), piece(j)], dst_ref=rx2.at[a % 2, pl.ds(at, n), piece(j)],
            send_sem=s2_send.at[a % 2, h, j], recv_sem=s2_recv.at[a % 2, h, j], device_id=across, device_id_type=MESH)

    def blocks(at, n, fn):
        def body(i, carry):
            fn(pl.multiple_of(at + i * 16, 16))
            return carry
        lax.fori_loop(0, n // 16, body, 0)

    def chip_sum(a, h, j, at, n):
        to_partner(a, h, j, at, n).wait_recv()

        def add(r):
            own = pbuf[mine(r, 16), piece(j)].astype(F32)
            tx2[a % 2, pl.ds(r, 16), piece(j)] = (own + rx1[a % 2, pl.ds(r, 16), piece(j)].astype(F32)).astype(BF16)
        blocks(at, n, add)
        to_across(a, h, j, at, n).start()

    def full_sum(a, h, j, at, n):
        to_across(a, h, j, at, n).wait_recv()

        def add(r):
            both = tx2[a % 2, pl.ds(r, 16), piece(j)].astype(F32) + rx2[a % 2, pl.ds(r, 16), piece(j)].astype(F32)
            res[pl.ds(r, 16), piece(j)] = res[pl.ds(r, 16), piece(j)] + both
        blocks(at, n, add)

    def sent(a, h, at, n):
        for j in range(AR_CHUNKS):
            to_partner(a, h, j, at, n).wait_send()
            to_across(a, h, j, at, n).wait_send()

    def rows_back(a, h, i):
        at = mine(h * part + i * 16, 16)
        return pltpu.make_async_remote_copy(
            src_ref=hbuf.at[at], dst_ref=hbuf.at[at], send_sem=s3_send.at[a % 2, h, i],
            recv_sem=s3_recv.at[a % 2, h, i], device_id=partner, device_id_type=MESH)

    def normalise(a, h):
        norm = nrow[a:a + 1, :]
        for i in range(part // 16):
            r = res[h * part + i * 16:h * part + (i + 1) * 16, :]
            inv = lax.rsqrt(jnp.mean(r * r, axis=-1, keepdims=True) + 1e-6)
            hbuf[mine(h * part + i * 16, 16), :] = (r * inv * norm).astype(BF16)
            rows_back(a, h, i).start()

    def all_rows(a, h):
        for i in range(part // 16):
            rows_back(a, h, i).wait()

    pieces = range(AR_CHUNKS)
    halves = range(2)
    first = [pltpu.make_async_copy(part_hbm.at[:, piece(j)], pbuf.at[:, piece(j)], load_sem.at[j]) for j in pieces]
    for copy in first:
        copy.start()
    small = [pltpu.make_async_copy(src, dst, small_sem.at[i]) for i, (src, dst) in enumerate(
        ((x_hbm.at[mine(0, half)], xhalf), (ncross_hbm, norm_in.at[0]), (nmlp_hbm, norm_in.at[1]), (mask_hbm, mask_ref)))]
    for copy in small:
        copy.start()
    barrier = pltpu.get_barrier_semaphore()
    for other in (partner, across):
        pl.semaphore_signal(barrier, inc=1, device_id=other, device_id_type=MESH)
    pl.semaphore_wait(barrier, 2)

    for j in pieces:
        first[j].wait()
        to_partner(0, 0, j, 0, part).start()
    for j in pieces:
        to_partner(0, 1, j, part, part).start()
    for k in range(n_sq):
        q_copy(k).start()
    for step in range(ahead):
        issue_step(step)
    for i in range(n_sq):
        o_copy(i).start()
    for i in range(2 * g_cut):
        gu_tall(0, i).start()
    for h in halves:
        for j in pieces:
            chip_sum(0, h, j, h * part, part)
    for copy in small:
        copy.wait()
    lay_row(nrow, 0, norm_in.at[0])
    lay_row(nrow, 1, norm_in.at[1])
    blocks(0, half, lambda r: res.__setitem__((pl.ds(r, 16), slice(None)), xhalf[pl.ds(r, 16), :].astype(F32)))

    def beside(a, b, used=depth):
        return jnp.concatenate([ring[a, 0:used, :], ring[b, 0:used, :]], axis=1)

    def both_cores(ref, h, at=slice(None)):
        return jnp.concatenate([ref[h * part:(h + 1) * part, at], ref[half + h * part:half + (h + 1) * part, at]], axis=0)

    def project_q(h):
        if h == 0:
            for k in range(n_sq):
                q_copy(k).wait()

        def block(n, carry):
            here = pl.ds(pl.multiple_of(n * COLS, COLS), COLS)
            y = None
            for k in range(n_sq):
                z = jnp.dot(both_cores(hbuf, h, slice(k * WIDE, (k + 1) * WIDE)), pw[k, :, here], preferred_element_type=F32)
                y = z if y is None else y + z
            y = y.astype(BF16).astype(F32)
            q_ref[h * part:(h + 1) * part, here] = y[0:part]
            q_ref[half + h * part:half + (h + 1) * part, here] = y[part:]
            return carry
        lax.fori_loop(0, inner // COLS, block, 0)

    own_head = (lax.broadcasted_iota(jnp.int32, (n_head, inner), 1) // (inner // n_head)
                == lax.broadcasted_iota(jnp.int32, (n_head, inner), 0))
    in_slot = GROUP // per_step

    def attend_step(step, carry):
        at = pl.ds(pl.multiple_of(group_of(step) * GROUP, GROUP), GROUP)
        ka, kb, va, vb = [ring_slot(step * 2 * per_step + k) for k in range(4)]
        q8 = q_ref[at, :]
        m8 = mask_ref[at, :]

        def spread(r):
            return jnp.where(own_head, jnp.broadcast_to(q8[r:r + 1, :], (n_head, inner)), 0.0).astype(BF16)

        def rows_of(a, b, r):
            here = pl.ds(r * inner, inner)
            return jnp.concatenate([ring[a, here, :], ring[b, here, :]], axis=1)
        landed(ka)
        landed(kb)
        scores = [None] * GROUP
        for r in range(in_slot):
            s = jnp.dot(jnp.concatenate([spread(r), spread(r + in_slot)], axis=0), rows_of(ka, kb, r), preferred_element_type=F32)
            scores[r] = jnp.where(m8[r:r + 1, :] != 0, s[0:n_head, 0:LANES], NEG_FILL)
            scores[r + in_slot] = jnp.where(m8[r + in_slot:r + in_slot + 1, :] != 0, s[n_head:, LANES:], NEG_FILL)
        s = jnp.concatenate(scores, axis=0)
        e = jnp.exp(s - jnp.max(s, axis=1, keepdims=True))
        p = (e / jnp.sum(e, axis=1, keepdims=True)).astype(BF16)
        landed(va)
        landed(vb)
        none = jnp.zeros((n_head, LANES), BF16)
        mixed = [None] * GROUP
        for r in range(in_slot):
            pa = p[r * n_head:(r + 1) * n_head, :]
            pb = p[(r + in_slot) * n_head:(r + in_slot + 1) * n_head, :]
            lhs = jnp.concatenate([jnp.concatenate([pa, none], axis=1), jnp.concatenate([none, pb], axis=1)], axis=0)
            y = lax.dot_general(lhs, rows_of(va, vb, r), (((1,), (1,)), ((), ())), preferred_element_type=F32)
            mixed[r] = jnp.sum(jnp.where(own_head, y[0:n_head], 0.0), axis=0, keepdims=True)
            mixed[r + in_slot] = jnp.sum(jnp.where(own_head, y[n_head:], 0.0), axis=0, keepdims=True)
        mix_ref[at, :] = jnp.concatenate(mixed, axis=0)

        @pl.when(step + ahead < n_step)
        def _():
            issue_step(step + ahead)
        return carry

    def project_o(h, after):
        lhs = both_cores(mix_ref, h).astype(BF16)
        for j in pieces:
            if h == 0:
                o_copy(j).wait()
            for n in range(WIDE // COLS):
                y = jnp.dot(lhs, pw[n_sq + j, :, n * COLS:(n + 1) * COLS], preferred_element_type=F32).astype(BF16)
                here = slice(j * WIDE + n * COLS, j * WIDE + (n + 1) * COLS)
                pbuf[h * part:(h + 1) * part, here] = y[0:part]
                pbuf[half + h * part:half + (h + 1) * part, here] = y[part:]
            to_partner(1, h, j, h * part, part).start()
            if after and j > 0:
                chip_sum(1, h, j - 1, h * part, part)
        if after:
            chip_sum(1, h, AR_CHUNKS - 1, h * part, part)

    for j in pieces:
        full_sum(0, 0, j, 0, part)
    normalise(0, 0)
    all_rows(0, 0)
    project_q(0)
    lax.fori_loop(0, n_step // 2, attend_step, 0)
    for pair in range(1, n_pair):
        for i in range(2 * g_cut):
            gu_tall(pair, i).start()
    sent(0, 0, 0, part)
    project_o(0, False)
    for j in pieces:
        full_sum(0, 1, j, part, part)
    normalise(0, 1)
    for j in pieces:
        chip_sum(1, 0, j, 0, part)
    all_rows(0, 1)
    project_q(1)
    for i in range(n_sq):
        gu_square(i).start()
    lax.fori_loop(n_step // 2, n_step, attend_step, 0)
    sent(0, 1, part, part)
    project_o(1, True)
    for i in range(n_sq):
        gu_square(n_sq + i).start()
    for i in range(d_narrow):
        issue_d(i)
    for j in pieces:
        full_sum(1, 0, j, 0, part)
    normalise(1, 0)
    for j in pieces:
        full_sum(1, 1, j, part, part)
    normalise(1, 1)
    for h in halves:
        all_rows(1, h)
        sent(1, h, h * part, part)

    root = math.sqrt(2.0 / math.pi)
    def mlp_block(at, gate, up):
        u, v = None, None
        for k in range(len(gate)):
            n = d_model // len(gate)
            lhs = hbuf[:, k * n:(k + 1) * n]
            y = jnp.dot(lhs, gate[k], preferred_element_type=F32)
            z = jnp.dot(lhs, up[k], preferred_element_type=F32)
            u, v = (y, z) if u is None else (u + y, v + z)
        gelu = 0.5 * u * (1.0 + jnp.tanh(root * (u + 0.044715 * (u * u * u))))
        act[:, pl.ds(at, COLS)] = (gelu * v).astype(BF16)

    def mlp_tall(pair):
        for i in range(2 * g_cut):
            gu_tall(pair, i).wait()
        base = (pair % n_pair) * 2 * g_cut

        def block(n, carry):
            here = pl.ds(pl.multiple_of(n * COLS, COLS), COLS)
            mlp_block(pl.multiple_of(WIDE + pair * g_cols + n * COLS, COLS), [gw[base + i, :, here] for i in range(g_cut)],
                      [gw[base + g_cut + i, :, here] for i in range(g_cut)])
            return carry
        lax.fori_loop(0, g_cols // COLS, block, 0)

    def mlp_square():
        for i in range(2 * n_sq):
            gu_square(i).wait()

        def block(n, carry):
            here = pl.ds(pl.multiple_of(n * COLS, COLS), COLS)
            mlp_block(pl.multiple_of(n * COLS, COLS), [pw[i, :, here] for i in range(n_sq)],
                      [pw[n_sq + i, :, here] for i in range(n_sq)])
            return carry
        lax.fori_loop(0, WIDE // COLS, block, 0)

    n_tall = (d_ff - WIDE) // g_cols
    for pair in range(n_pair):
        mlp_tall(pair)
        if pair + n_pair < n_tall:
            for i in range(2 * g_cut):
                gu_tall(pair + n_pair, i).start()
    mlp_square()
    for c in (2, 3):
        for i in range(d_cut):
            d_square(c, i).start()
    for pair in range(n_pair, n_tall):
        mlp_tall(pair)

    per_piece = width // COLS

    def out_back(j):
        return pltpu.make_async_remote_copy(
            src_ref=hbuf.at[mine(0, half), piece(j)], dst_ref=hbuf.at[mine(0, half), piece(j)], send_sem=s3_send.at[0, 0, j],
            recv_sem=s3_recv.at[0, 0, j], device_id=partner, device_id_type=MESH)

    for c in pieces:
        if c >= 2:
            for i in range(d_cut):
                d_square(c, i).wait()

        def down(i, carry):
            n = c * per_piece + i
            if c < 2:
                landed(2 * n, d_ff)
                landed(2 * n + 1, d_ff)
                y = jnp.dot(act[...], beside(2 * n, 2 * n + 1, d_ff), preferred_element_type=F32)
            else:
                y = None
                for k in range(d_cut):
                    at, rest = k * WIDE, min(WIDE, d_ff - k * WIDE)
                    w = pw[(c - 2) * d_cut + k, 0:rest, pl.ds(pl.multiple_of(i * COLS, COLS), COLS)]
                    z = jnp.dot(act[:, at:at + rest], w, preferred_element_type=F32)
                    y = z if y is None else y + z
            pbuf[:, pl.ds(pl.multiple_of(n * COLS, COLS), COLS)] = y.astype(BF16)
            return carry
        lax.fori_loop(0, per_piece, down, 0)
        to_partner(2, 0, c, 0, half).start()
        if c > 0:
            chip_sum(2, 0, c - 1, 0, half)
    chip_sum(2, 0, AR_CHUNKS - 1, 0, half)

    def out_copy(j):
        return pltpu.make_async_copy(hbuf.at[:, piece(j)], out_hbm.at[:, piece(j)], out_sem.at[j])

    for j in pieces:
        to_across(2, 0, j, 0, half).wait_recv()

        def add(r):
            both = tx2[0, pl.ds(r, 16), piece(j)].astype(F32) + rx2[0, pl.ds(r, 16), piece(j)].astype(F32)
            hbuf[mine(r, 16), piece(j)] = (res[pl.ds(r, 16), piece(j)] + both).astype(BF16)
        blocks(0, half, add)
        out_back(j).start()
        if j > 0:
            out_back(j - 1).wait()
            out_copy(j - 1).start()
    out_back(AR_CHUNKS - 1).wait()
    out_copy(AR_CHUNKS - 1).start()
    sent(2, 0, 0, half)
    for j in pieces:
        out_copy(j).wait()


def rest_of_layer(x_in, part, norm_cross, norm_mlp, enc_mask, cross_k, cross_v, cross_q, cross_o, w_gate, w_up, w_down):
    rows, d_model = x_in.shape
    _, src_len, n_head, d_head = cross_k.shape
    inner = n_head * d_head
    d_ff = w_gate.shape[1]
    half = rows // 2
    flat = (rows * inner, src_len)
    k_flat = cross_k.transpose(0, 2, 3, 1).reshape(flat)
    v_flat = cross_v.transpose(0, 2, 3, 1).reshape(flat)
    square = (d_model // 128, 128)
    return pl.pallas_call(
        functools.partial(cross_kernel, n_head),
        out_shape=jax.ShapeDtypeStruct((rows, d_model), BF16),
        in_specs=[ANY] * 12,
        out_specs=ANY,
        scratch_shapes=[
            pltpu.VMEM((RING, d_model, LANES), BF16),
            pltpu.VMEM((8, WIDE, WIDE), BF16),
            pltpu.VMEM((8, d_model // 2, 512), BF16),
            pltpu.VMEM((rows, d_model), BF16),
            pltpu.VMEM((rows, d_model), BF16),
            pltpu.VMEM((half, d_model), F32),
            pltpu.VMEM((half, d_model), BF16),
            pltpu.VMEM((2, half, d_model), BF16),
            pltpu.VMEM((2, half, d_model), BF16),
            pltpu.VMEM((2, half, d_model), BF16),
            pltpu.VMEM((rows, inner), F32),
            pltpu.VMEM((rows, inner), F32),
            pltpu.VMEM((rows, d_ff), BF16),
            pltpu.VMEM((2,) + square, BF16),
            pltpu.VMEM((2, d_model), F32),
            pltpu.VMEM((rows, src_len), jnp.int32),
            pltpu.SemaphoreType.DMA((RING,)),
            pltpu.SemaphoreType.DMA((8,)),
            pltpu.SemaphoreType.DMA((8,)),
            pltpu.SemaphoreType.DMA((AR_CHUNKS,)),
            pltpu.SemaphoreType.DMA((4,)),
            pltpu.SemaphoreType.DMA((2, 2, AR_CHUNKS)),
            pltpu.SemaphoreType.DMA((2, 2, AR_CHUNKS)),
            pltpu.SemaphoreType.DMA((2, 2, AR_CHUNKS)),
            pltpu.SemaphoreType.DMA((2, 2, AR_CHUNKS)),
            pltpu.SemaphoreType.DMA((2, 2, AR_CHUNKS)),
            pltpu.SemaphoreType.DMA((2, 2, AR_CHUNKS)),
            pltpu.SemaphoreType.DMA((AR_CHUNKS,)),
        ],
        compiler_params=pltpu.CompilerParams(vmem_limit_bytes=67_000_000, collective_id=0, has_side_effects=True),
        name="rest_part",
    )(x_in, part, norm_cross.reshape(square), norm_mlp.reshape(square), enc_mask, cross_q, k_flat, v_flat, cross_o, w_gate, w_up, w_down)


def solution(mesh):
    def local_layer(x_in, tok_pos, self_k, self_v, cross_k, cross_v, enc_mask, rel_bias, w_q, w_k, w_v, w_o, cross_q, cross_o, w_gate, w_up, w_down, norm_self, norm_cross, norm_mlp):
        part, new_self_k, new_self_v = self_attention(x_in, norm_self, tok_pos, rel_bias, w_q, w_k, w_v, w_o, self_k, self_v)
        x_out = rest_of_layer(x_in, part, norm_cross, norm_mlp, enc_mask, cross_k, cross_v, cross_q, cross_o, w_gate, w_up, w_down)
        return x_out, new_self_k, new_self_v

    cache_spec = P('dp', None, 'tp', None)
    split_cols = P(None, 'tp')
    split_rows = P('tp', None)
    in_specs = (P('dp', None), P('dp'), cache_spec, cache_spec, cache_spec, cache_spec, P('dp', None), split_cols, split_cols, split_cols, split_cols, split_rows, split_cols, split_rows, split_cols, split_cols, split_rows, P(None), P(None), P(None))
    out_specs = (P('dp', None), cache_spec, cache_spec)
    return jax.shard_map(local_layer, mesh=mesh, in_specs=in_specs, out_specs=out_specs, check_vma=False)
```

```python
import functools
import math
import jax
import jax.numpy as jnp
from jax import lax
from jax.experimental import pallas as pl
from jax.experimental.pallas import tpu as pltpu
from jax.sharding import PartitionSpec as P

BUCKET_EDGES = tuple(int(math.ceil(16.0 * 8.0 ** (bucket_step / 16.0))) for bucket_step in range(1, 16))
NEG_FILL = -1e30
F32 = jnp.float32
BF16 = jnp.bfloat16
ANY = pl.BlockSpec(memory_space=pl.ANY)
VMEM = pl.BlockSpec(memory_space=pltpu.VMEM)
COLS = 256
T_BLOCK = 8


def lay_row(dst, at, norm):
    values = norm[...].astype(F32)
    for i in range(values.shape[0]):
        dst[at:at + 1, i * 128:(i + 1) * 128] = values[i:i + 1, :]


def self_kernel(x_hbm, norm_hbm, pos_hbm, rel_hbm, wq_hbm, wk_hbm, wv_hbm, wo_hbm, k_hbm, v_hbm,
                part_hbm, newk_hbm, newv_hbm,
                xbuf, hbuf, wbuf, kvbuf, sum_ref, q_ref, kn_ref, hit_ref, score_ref, acc_ref,
                norm_ref, nrow, pos_ref, rel_ref,
                x_sem, small_sem, w_sem, kv_sem, out_sem, part_sem, window):
    rows, d_model = xbuf.shape
    n_w = wbuf.shape[0]
    per_mat = n_w // 3
    n_chunk = kvbuf.shape[0] // 2
    n_head, t_len = score_ref.shape[0], score_ref.shape[1]
    inner = acc_ref.shape[0]
    d_head = inner // n_head
    chunk_rows = kvbuf.shape[1]
    sub = d_head // 16
    k_rows = wbuf.shape[1]
    n_wo = wo_hbm.shape[1] // inner

    def w_copy(c):
        src = (wq_hbm, wk_hbm, wv_hbm)[c // per_mat]
        return pltpu.make_async_copy(src.at[pl.ds((c % per_mat) * k_rows, k_rows)], wbuf.at[c], w_sem.at[c])

    def kv_copy(i):
        src = k_hbm if i < n_chunk else v_hbm
        return pltpu.make_async_copy(src.at[pl.ds((i % n_chunk) * chunk_rows, chunk_rows)], kvbuf.at[i], kv_sem.at[i])

    def wo_copies(i):
        return [pltpu.make_async_copy(wo_hbm.at[:, pl.ds(i * inner, inner)], wbuf.at[i], w_sem.at[i])]

    loads = [[w_copy(c)] for c in range(n_w)] + [[kv_copy(i)] for i in range(2 * n_chunk)] + [wo_copies(i) for i in range(n_wo)]
    issued = [0]

    def issue(upto):
        while issued[0] < min(upto, len(loads)):
            for copy in loads[issued[0]]:
                copy.start()
            issued[0] += 1

    x_copy = pltpu.make_async_copy(x_hbm, xbuf, x_sem)
    x_copy.start()
    small = [pltpu.make_async_copy(src, dst, small_sem.at[i]) for i, (src, dst) in enumerate(
        ((pos_hbm, pos_ref), (rel_hbm, rel_ref), (norm_hbm, norm_ref)))]
    for copy in small:
        copy.start()
    issue(window)
    for copy in small:
        copy.wait()

    lay_row(nrow, 0, norm_ref)
    pos = pos_ref[...]
    pos16 = jnp.broadcast_to(pos, (16, rows))

    def set_hit(t, carry):
        hit_ref[t] = jnp.where(pos16 == t, 1.0, 0.0).astype(BF16)
        return carry
    lax.fori_loop(0, t_len, set_hit, 0)

    lane = lax.broadcasted_iota(jnp.int32, (n_head, 128), 1)
    bucket = jnp.full((n_head, 128), 16, jnp.int32)
    for edge in BUCKET_EDGES:
        bucket = bucket + (lane >= edge).astype(jnp.int32)
    bucket = jnp.where(lane < 16, lane, bucket)
    rel = rel_ref[...]
    table = jnp.zeros((n_head, 128), F32)
    for b in range(rel.shape[1]):
        table = jnp.where(bucket == b, rel[:, b:b + 1], table)
    acc_ref[0:n_head, :] = table

    x_copy.wait()
    block = 16
    norm = nrow[0:1, :]

    def norm_rows(i, carry):
        at = pl.ds(pl.multiple_of(i * block, block), block)
        r = xbuf[at, :].astype(F32)
        inv = lax.rsqrt(jnp.mean(r * r, axis=-1, keepdims=True) + 1e-6)
        hbuf[at, :] = (r * inv * norm).astype(BF16)
        return carry
    lax.fori_loop(0, rows // block, norm_rows, 0)

    for c in range(n_w):
        w_copy(c).wait()
        issue(c + 1 + window)
        k = c % per_mat
        for n in range(inner // COLS):
            here = slice(n * COLS, (n + 1) * COLS)
            y = jnp.dot(hbuf[:, k * k_rows:(k + 1) * k_rows], wbuf[c, :, here], preferred_element_type=F32)
            if k > 0:
                y = y + sum_ref[:, here]
            if k < per_mat - 1:
                sum_ref[:, here] = y
                continue
            y = y.astype(BF16).astype(F32).T
            if c < per_mat:
                q_ref[here, :] = y
            else:
                kn_ref[c // per_mat - 1, here, :] = y.astype(BF16)

    def chunk_out(i):
        dst = newk_hbm if i < n_chunk else newv_hbm
        return pltpu.make_async_copy(kvbuf.at[i], dst.at[pl.ds((i % n_chunk) * chunk_rows, chunk_rows)], out_sem.at[i])

    for j in range(n_chunk):
        kv_copy(j).wait()
        issue(n_w + j + 1 + window)

        def k_head(h, carry):
            at = pl.multiple_of(h * d_head, d_head)
            q = q_ref[pl.ds(at, d_head), :]
            kn = kn_ref[0, pl.ds(at, d_head), :].reshape(sub, 16, rows)
            rows_out = []
            for tt in range(T_BLOCK):
                here = pl.ds(pl.multiple_of(tt * inner + at, d_head), d_head)
                old = kvbuf[j, here, :].reshape(sub, 16, rows)
                hit = hit_ref[j * T_BLOCK + tt] != 0
                new = jnp.where(hit[None], kn, old)
                kvbuf[j, here, :] = new.reshape(d_head, rows)
                prod = new.reshape(d_head, rows).astype(F32) * q
                rows_out.append(jnp.sum(prod, axis=0, keepdims=True))
            score_ref[h, j * T_BLOCK:(j + 1) * T_BLOCK, :] = jnp.concatenate(rows_out, axis=0)
            return carry
        lax.fori_loop(0, n_head, k_head, 0)
        chunk_out(j).start(priority=1)

    t_iota = lax.broadcasted_iota(jnp.int32, (t_len, rows), 0)
    causal = t_iota <= pos
    back = jnp.maximum(pos - t_iota, 0)

    def soft_head(h, carry):
        line = jnp.broadcast_to(acc_ref[pl.ds(h, 1), :], (t_len, 128))
        s = score_ref[h] + jnp.take_along_axis(line, back, axis=1)
        s = jnp.where(causal, s, NEG_FILL)
        e = jnp.exp(s - jnp.max(s, axis=0, keepdims=True))
        p = e / jnp.sum(e, axis=0, keepdims=True)
        score_ref[h] = p.astype(BF16).astype(F32)
        return carry
    lax.fori_loop(0, n_head, soft_head, 0)

    acc_ref[...] = jnp.zeros_like(acc_ref)
    for j in range(n_chunk):
        kv_copy(n_chunk + j).wait()
        issue(n_w + n_chunk + j + 1 + window)

        def v_head(h, carry):
            at = pl.multiple_of(h * d_head, d_head)
            vn = kn_ref[1, pl.ds(at, d_head), :].reshape(sub, 16, rows)
            p = score_ref[h, j * T_BLOCK:(j + 1) * T_BLOCK, :]
            acc = acc_ref[pl.ds(at, d_head), :]
            for tt in range(T_BLOCK):
                here = pl.ds(pl.multiple_of(tt * inner + at, d_head), d_head)
                old = kvbuf[n_chunk + j, here, :].reshape(sub, 16, rows)
                hit = hit_ref[j * T_BLOCK + tt] != 0
                new = jnp.where(hit[None], vn, old)
                kvbuf[n_chunk + j, here, :] = new.reshape(d_head, rows)
                acc = acc + new.reshape(d_head, rows).astype(F32) * p[tt:tt + 1, :]
            acc_ref[pl.ds(at, d_head), :] = acc
            return carry
        lax.fori_loop(0, n_head, v_head, 0)
        chunk_out(n_chunk + j).start(priority=1)

    issue(len(loads))
    hbuf[:, 0:inner] = acc_ref[...].T.astype(BF16)
    part_copies = []
    for i in range(n_wo):
        for copy in wo_copies(i):
            copy.wait()
        for r in range(inner // COLS):
            at = i * inner + r * COLS
            y = jnp.dot(hbuf[:, 0:inner], wbuf[i, :, r * COLS:(r + 1) * COLS], preferred_element_type=F32)
            xbuf[:, at:at + COLS] = y.astype(BF16)
        here = pl.ds(i * inner, inner)
        copy = pltpu.make_async_copy(xbuf.at[:, here], part_hbm.at[:, here], part_sem.at[i])
        copy.start()
        part_copies.append(copy)
    for i in range(2 * n_chunk):
        chunk_out(i).wait()
    for copy in part_copies:
        copy.wait()


def self_attention(x_in, norm_self, tok_pos, rel_bias, w_q, w_k, w_v, w_o, self_k, self_v):
    rows, t_len, n_head, d_head = self_k.shape
    d_model = x_in.shape[1]
    inner = n_head * d_head
    flat = (t_len * inner, rows)
    k_flat = self_k.transpose(1, 2, 3, 0).reshape(flat)
    v_flat = self_v.transpose(1, 2, 3, 0).reshape(flat)
    n_w = 3 * (d_model // inner)
    n_chunk = t_len // T_BLOCK
    n_wo = w_o.shape[1] // inner

    def body(*refs):
        self_kernel(*refs, window=14)

    part, new_k, new_v = pl.pallas_call(
        body,
        out_shape=(jax.ShapeDtypeStruct((rows, w_o.shape[1]), BF16),
                   jax.ShapeDtypeStruct(flat, BF16), jax.ShapeDtypeStruct(flat, BF16)),
        in_specs=[ANY] * 10,
        out_specs=(ANY, ANY, ANY),
        scratch_shapes=[
            pltpu.VMEM((rows, d_model), BF16),
            pltpu.VMEM((rows, d_model), BF16),
            pltpu.VMEM((n_w, inner, inner), BF16),
            pltpu.VMEM((2 * n_chunk, T_BLOCK * inner, rows), BF16),
            pltpu.VMEM((rows, inner), F32),
            pltpu.VMEM((inner, rows), F32),
            pltpu.VMEM((2, inner, rows), BF16),
            pltpu.VMEM((t_len, 16, rows), BF16),
            pltpu.VMEM((n_head, t_len, rows), F32),
            pltpu.VMEM((inner, rows), F32),
            pltpu.VMEM((d_model // 128, 128), BF16),
            pltpu.VMEM((1, d_model), F32),
            pltpu.VMEM((1, rows), jnp.int32),
            pltpu.VMEM(rel_bias.shape[::-1], F32),
            pltpu.SemaphoreType.DMA,
            pltpu.SemaphoreType.DMA((3,)),
            pltpu.SemaphoreType.DMA((n_w,)),
            pltpu.SemaphoreType.DMA((2 * n_chunk,)),
            pltpu.SemaphoreType.DMA((2 * n_chunk,)),
            pltpu.SemaphoreType.DMA((n_wo,)),
        ],
        compiler_params=pltpu.CompilerParams(vmem_limit_bytes=66_900_000),
        cost_estimate=pl.CostEstimate(flops=4_400_000_000, bytes_accessed=104_000_000, transcendentals=131_072),
        name="self_part",
    )(x_in, norm_self.reshape(d_model // 128, 128), tok_pos.reshape(1, rows), rel_bias.T, w_q, w_k, w_v, w_o, k_flat, v_flat)

    def unflat(cache):
        return cache.reshape(t_len, n_head, d_head, rows).transpose(3, 0, 1, 2)
    return part, unflat(new_k), unflat(new_v)


RING = 20
WIDE = 1024
GROUP = 8
AR_CHUNKS = 4
LANES = 128


def cross_kernel(n_head, x_hbm, part_hbm, ncross_hbm, nmlp_hbm, mask_hbm, cq_hbm, ck_hbm, cv_hbm, co_hbm, wg_hbm, wu_hbm, wd_hbm,
                 out_hbm,
                 ring, pw, gw, pbuf, hbuf, res, xhalf, rx1, tx2, rx2, q_ref, mix_ref, act, norm_in, nrow, mask_ref,
                 ring_sem, p_sem, g_sem, load_sem, small_sem, s1_send, s1_recv, s2_send, s2_recv, s3_send, s3_recv, out_sem):
    rows, d_model = hbuf.shape
    half = rows // 2
    part = half // 2
    depth = ring.shape[1]
    inner = q_ref.shape[1]
    d_ff = act.shape[1]
    width = d_model // AR_CHUNKS
    MESH = pl.DeviceIdType.MESH

    me = lax.axis_index("tp")
    core = lax.rem(me, 2)
    chip = me // 2
    partner = {"tp": chip * 2 + (1 - core)}
    across = {"tp": (1 - chip) * 2 + core}

    def mine(at, n):
        return pl.ds(pl.multiple_of(core * half + at, 16), n)

    def theirs(at, n):
        return pl.ds(pl.multiple_of((1 - core) * half + at, 16), n)

    def piece(j):
        return pl.ds(j * width, width)

    per_step = GROUP * inner // depth
    n_step = rows // GROUP
    ahead = RING // (2 * per_step)
    n_sq = pw.shape[0] // 2
    g_rows, g_cols = gw.shape[1:]
    g_cut = d_model // g_rows
    n_pair = gw.shape[0] // (2 * g_cut)

    def copy_in(src, slot, used=None):
        dst = ring.at[slot] if used is None else ring.at[slot, used]
        pltpu.make_async_copy(src, dst, ring_sem.at[slot]).start()

    def landed(slot, used=depth):
        pltpu.make_async_copy(ck_hbm.at[pl.ds(0, used)], ring.at[slot, pl.ds(0, used)], ring_sem.at[slot]).wait()

    def ring_slot(n):
        return n % RING

    def group_of(step):
        per_half, u = n_step // 2, step % (n_step // 2)
        return (step // per_half) * (part // GROUP) + u + (u // (part // GROUP)) * (part // GROUP)

    def issue_step(step):
        for k in range(2 * per_step):
            src = ck_hbm if k < per_step else cv_hbm
            at = (group_of(step) * per_step + k % per_step) * depth
            at = at if isinstance(at, int) else pl.multiple_of(at, depth)
            copy_in(src.at[pl.ds(at, depth)], ring_slot(step * 2 * per_step + k))

    def q_copy(k):
        return pltpu.make_async_copy(cq_hbm.at[pl.ds(k * WIDE, WIDE)], pw.at[k], p_sem.at[k])

    def o_copy(i):
        return pltpu.make_async_copy(co_hbm.at[:, pl.ds(i * WIDE, WIDE)], pw.at[n_sq + i], p_sem.at[n_sq + i])

    def gu_square(i):
        src = wg_hbm if i < n_sq else wu_hbm
        return pltpu.make_async_copy(src.at[pl.ds((i % n_sq) * WIDE, WIDE), pl.ds(0, WIDE)], pw.at[i], p_sem.at[i])

    def gu_tall(pair, i):
        src = wg_hbm if i < g_cut else wu_hbm
        slot = (pair % n_pair) * 2 * g_cut + i
        return pltpu.make_async_copy(src.at[pl.ds((i % g_cut) * g_rows, g_rows), pl.ds(WIDE + pair * g_cols, g_cols)],
                                     gw.at[slot], g_sem.at[slot])

    d_cut = -(-d_ff // WIDE)
    d_narrow = 2 * WIDE // LANES

    def d_square(c, i):
        slot = (c - 2) * d_cut + i
        n = min(WIDE, d_ff - i * WIDE)
        return pltpu.make_async_copy(wd_hbm.at[pl.ds(i * WIDE, n), pl.ds(c * WIDE, WIDE)],
                                     pw.at[slot, pl.ds(0, n)], p_sem.at[slot])

    def issue_d(i):
        copy_in(wd_hbm.at[:, pl.ds(i * LANES, LANES)], i, pl.ds(0, d_ff))

    def to_partner(a, h, j, at, n):
        return pltpu.make_async_remote_copy(
            src_ref=pbuf.at[theirs(at, n), piece(j)], dst_ref=rx1.at[a % 2, pl.ds(at, n), piece(j)],
            send_sem=s1_send.at[a % 2, h, j], recv_sem=s1_recv.at[a % 2, h, j], device_id=partner, device_id_type=MESH)

    def to_across(a, h, j, at, n):
        return pltpu.make_async_remote_copy(
            src_ref=tx2.at[a % 2, pl.ds(at, n), piece(j)], dst_ref=rx2.at[a % 2, pl.ds(at, n), piece(j)],
            send_sem=s2_send.at[a % 2, h, j], recv_sem=s2_recv.at[a % 2, h, j], device_id=across, device_id_type=MESH)

    def blocks(at, n, fn):
        def body(i, carry):
            fn(pl.multiple_of(at + i * 16, 16))
            return carry
        lax.fori_loop(0, n // 16, body, 0)

    def chip_sum(a, h, j, at, n):
        to_partner(a, h, j, at, n).wait_recv()

        def add(r):
            own = pbuf[mine(r, 16), piece(j)].astype(F32)
            tx2[a % 2, pl.ds(r, 16), piece(j)] = (own + rx1[a % 2, pl.ds(r, 16), piece(j)].astype(F32)).astype(BF16)
        blocks(at, n, add)
        to_across(a, h, j, at, n).start()

    def full_sum(a, h, j, at, n):
        to_across(a, h, j, at, n).wait_recv()

        def add(r):
            both = tx2[a % 2, pl.ds(r, 16), piece(j)].astype(F32) + rx2[a % 2, pl.ds(r, 16), piece(j)].astype(F32)
            res[pl.ds(r, 16), piece(j)] = res[pl.ds(r, 16), piece(j)] + both
        blocks(at, n, add)

    def sent(a, h, at, n):
        for j in range(AR_CHUNKS):
            to_partner(a, h, j, at, n).wait_send()
            to_across(a, h, j, at, n).wait_send()

    def rows_back(a, h, i):
        at = mine(h * part + i * 16, 16)
        return pltpu.make_async_remote_copy(
            src_ref=hbuf.at[at], dst_ref=hbuf.at[at], send_sem=s3_send.at[a % 2, h, i],
            recv_sem=s3_recv.at[a % 2, h, i], device_id=partner, device_id_type=MESH)

    def normalise(a, h):
        norm = nrow[a:a + 1, :]
        for i in range(part // 16):
            r = res[h * part + i * 16:h * part + (i + 1) * 16, :]
            inv = lax.rsqrt(jnp.mean(r * r, axis=-1, keepdims=True) + 1e-6)
            hbuf[mine(h * part + i * 16, 16), :] = (r * inv * norm).astype(BF16)
            rows_back(a, h, i).start()

    def all_rows(a, h):
        for i in range(part // 16):
            rows_back(a, h, i).wait()

    pieces = range(AR_CHUNKS)
    halves = range(2)
    first = [pltpu.make_async_copy(part_hbm.at[:, piece(j)], pbuf.at[:, piece(j)], load_sem.at[j]) for j in pieces]
    for copy in first:
        copy.start()
    small = [pltpu.make_async_copy(src, dst, small_sem.at[i]) for i, (src, dst) in enumerate(
        ((x_hbm.at[mine(0, half)], xhalf), (ncross_hbm, norm_in.at[0]), (nmlp_hbm, norm_in.at[1]), (mask_hbm, mask_ref)))]
    for copy in small:
        copy.start()
    barrier = pltpu.get_barrier_semaphore()
    for other in (partner, across):
        pl.semaphore_signal(barrier, inc=1, device_id=other, device_id_type=MESH)
    pl.semaphore_wait(barrier, 2)

    for j in pieces:
        first[j].wait()
        to_partner(0, 0, j, 0, part).start()
    for j in pieces:
        to_partner(0, 1, j, part, part).start()
    for k in range(n_sq):
        q_copy(k).start()
    for step in range(ahead):
        issue_step(step)
    for i in range(n_sq):
        o_copy(i).start()
    for i in range(2 * g_cut):
        gu_tall(0, i).start()
    for h in halves:
        for j in pieces:
            chip_sum(0, h, j, h * part, part)
    for copy in small:
        copy.wait()
    lay_row(nrow, 0, norm_in.at[0])
    lay_row(nrow, 1, norm_in.at[1])
    blocks(0, half, lambda r: res.__setitem__((pl.ds(r, 16), slice(None)), xhalf[pl.ds(r, 16), :].astype(F32)))

    def beside(a, b, used=depth):
        return jnp.concatenate([ring[a, 0:used, :], ring[b, 0:used, :]], axis=1)

    def both_cores(ref, h, at=slice(None)):
        return jnp.concatenate([ref[h * part:(h + 1) * part, at], ref[half + h * part:half + (h + 1) * part, at]], axis=0)

    def project_q(h):
        if h == 0:
            for k in range(n_sq):
                q_copy(k).wait()

        def block(n, carry):
            here = pl.ds(pl.multiple_of(n * COLS, COLS), COLS)
            y = None
            for k in range(n_sq):
                z = jnp.dot(both_cores(hbuf, h, slice(k * WIDE, (k + 1) * WIDE)), pw[k, :, here], preferred_element_type=F32)
                y = z if y is None else y + z
            y = y.astype(BF16).astype(F32)
            q_ref[h * part:(h + 1) * part, here] = y[0:part]
            q_ref[half + h * part:half + (h + 1) * part, here] = y[part:]
            return carry
        lax.fori_loop(0, inner // COLS, block, 0)

    own_head = (lax.broadcasted_iota(jnp.int32, (n_head, inner), 1) // (inner // n_head)
                == lax.broadcasted_iota(jnp.int32, (n_head, inner), 0))
    in_slot = GROUP // per_step

    def attend_step(step, carry):
        at = pl.ds(pl.multiple_of(group_of(step) * GROUP, GROUP), GROUP)
        ka, kb, va, vb = [ring_slot(step * 2 * per_step + k) for k in range(4)]
        q8 = q_ref[at, :]
        m8 = mask_ref[at, :]

        def spread(r):
            return jnp.where(own_head, jnp.broadcast_to(q8[r:r + 1, :], (n_head, inner)), 0.0).astype(BF16)

        def rows_of(a, b, r):
            here = pl.ds(r * inner, inner)
            return jnp.concatenate([ring[a, here, :], ring[b, here, :]], axis=1)
        landed(ka)
        landed(kb)
        scores = [None] * GROUP
        for r in range(in_slot):
            s = jnp.dot(jnp.concatenate([spread(r), spread(r + in_slot)], axis=0), rows_of(ka, kb, r), preferred_element_type=F32)
            scores[r] = jnp.where(m8[r:r + 1, :] != 0, s[0:n_head, 0:LANES], NEG_FILL)
            scores[r + in_slot] = jnp.where(m8[r + in_slot:r + in_slot + 1, :] != 0, s[n_head:, LANES:], NEG_FILL)
        s = jnp.concatenate(scores, axis=0)
        e = jnp.exp(s - jnp.max(s, axis=1, keepdims=True))
        p = (e / jnp.sum(e, axis=1, keepdims=True)).astype(BF16)
        landed(va)
        landed(vb)
        none = jnp.zeros((n_head, LANES), BF16)
        mixed = [None] * GROUP
        for r in range(in_slot):
            pa = p[r * n_head:(r + 1) * n_head, :]
            pb = p[(r + in_slot) * n_head:(r + in_slot + 1) * n_head, :]
            lhs = jnp.concatenate([jnp.concatenate([pa, none], axis=1), jnp.concatenate([none, pb], axis=1)], axis=0)
            y = lax.dot_general(lhs, rows_of(va, vb, r), (((1,), (1,)), ((), ())), preferred_element_type=F32)
            mixed[r] = jnp.sum(jnp.where(own_head, y[0:n_head], 0.0), axis=0, keepdims=True)
            mixed[r + in_slot] = jnp.sum(jnp.where(own_head, y[n_head:], 0.0), axis=0, keepdims=True)
        mix_ref[at, :] = jnp.concatenate(mixed, axis=0)

        @pl.when(step + ahead < n_step)
        def _():
            issue_step(step + ahead)
        return carry

    def project_o(h, after):
        lhs = both_cores(mix_ref, h).astype(BF16)
        for j in pieces:
            if h == 0:
                o_copy(j).wait()
            for n in range(WIDE // COLS):
                y = jnp.dot(lhs, pw[n_sq + j, :, n * COLS:(n + 1) * COLS], preferred_element_type=F32).astype(BF16)
                here = slice(j * WIDE + n * COLS, j * WIDE + (n + 1) * COLS)
                pbuf[h * part:(h + 1) * part, here] = y[0:part]
                pbuf[half + h * part:half + (h + 1) * part, here] = y[part:]
            to_partner(1, h, j, h * part, part).start()
            if after and j > 0:
                chip_sum(1, h, j - 1, h * part, part)
        if after:
            chip_sum(1, h, AR_CHUNKS - 1, h * part, part)

    for j in pieces:
        full_sum(0, 0, j, 0, part)
    normalise(0, 0)
    all_rows(0, 0)
    project_q(0)
    lax.fori_loop(0, n_step // 2, attend_step, 0)
    sent(0, 0, 0, part)
    project_o(0, False)
    for j in pieces:
        full_sum(0, 1, j, part, part)
    normalise(0, 1)
    for j in pieces:
        chip_sum(1, 0, j, 0, part)
    all_rows(0, 1)
    project_q(1)
    lax.fori_loop(n_step // 2, n_step, attend_step, 0)
    for pair in range(1, n_pair):
        for i in range(2 * g_cut):
            gu_tall(pair, i).start()
    for i in range(n_sq):
        gu_square(i).start()
    sent(0, 1, part, part)
    project_o(1, True)
    for i in range(n_sq):
        gu_square(n_sq + i).start()
    for i in range(d_narrow):
        issue_d(i)
    for j in pieces:
        full_sum(1, 0, j, 0, part)
    normalise(1, 0)
    for j in pieces:
        full_sum(1, 1, j, part, part)
    normalise(1, 1)
    for h in halves:
        all_rows(1, h)
        sent(1, h, h * part, part)

    root = math.sqrt(2.0 / math.pi)
    def mlp_block(at, gate, up):
        u, v = None, None
        for k in range(len(gate)):
            n = d_model // len(gate)
            lhs = hbuf[:, k * n:(k + 1) * n]
            y = jnp.dot(lhs, gate[k], preferred_element_type=F32)
            z = jnp.dot(lhs, up[k], preferred_element_type=F32)
            u, v = (y, z) if u is None else (u + y, v + z)
        gelu = 0.5 * u * (1.0 + jnp.tanh(root * (u + 0.044715 * (u * u * u))))
        act[:, pl.ds(at, COLS)] = (gelu * v).astype(BF16)

    def mlp_tall(pair):
        for i in range(2 * g_cut):
            gu_tall(pair, i).wait()
        base = (pair % n_pair) * 2 * g_cut

        def block(n, carry):
            here = pl.ds(pl.multiple_of(n * COLS, COLS), COLS)
            mlp_block(pl.multiple_of(WIDE + pair * g_cols + n * COLS, COLS), [gw[base + i, :, here] for i in range(g_cut)],
                      [gw[base + g_cut + i, :, here] for i in range(g_cut)])
            return carry
        lax.fori_loop(0, g_cols // COLS, block, 0)

    def mlp_square():
        for i in range(2 * n_sq):
            gu_square(i).wait()

        def block(n, carry):
            here = pl.ds(pl.multiple_of(n * COLS, COLS), COLS)
            mlp_block(pl.multiple_of(n * COLS, COLS), [pw[i, :, here] for i in range(n_sq)],
                      [pw[n_sq + i, :, here] for i in range(n_sq)])
            return carry
        lax.fori_loop(0, WIDE // COLS, block, 0)

    n_tall = (d_ff - WIDE) // g_cols
    for pair in range(n_pair):
        mlp_tall(pair)
        if pair + n_pair < n_tall:
            for i in range(2 * g_cut):
                gu_tall(pair + n_pair, i).start()
    mlp_square()
    for c in (2, 3):
        for i in range(d_cut):
            d_square(c, i).start()
    for pair in range(n_pair, n_tall):
        mlp_tall(pair)

    n_last = 2 * AR_CHUNKS
    w_last = d_model // n_last
    per_piece = w_last // COLS

    def last_piece(j):
        return pl.ds(j * w_last, w_last)

    def last_to_partner(j):
        return pltpu.make_async_remote_copy(
            src_ref=pbuf.at[theirs(0, half), last_piece(j)], dst_ref=rx1.at[0, :, last_piece(j)],
            send_sem=s1_send.at[0, j // AR_CHUNKS, j % AR_CHUNKS], recv_sem=s1_recv.at[0, j // AR_CHUNKS, j % AR_CHUNKS],
            device_id=partner, device_id_type=MESH)

    def last_to_across(j):
        return pltpu.make_async_remote_copy(
            src_ref=tx2.at[0, :, last_piece(j)], dst_ref=rx2.at[0, :, last_piece(j)],
            send_sem=s2_send.at[0, j // AR_CHUNKS, j % AR_CHUNKS], recv_sem=s2_recv.at[0, j // AR_CHUNKS, j % AR_CHUNKS],
            device_id=across, device_id_type=MESH)

    def last_back(j):
        return pltpu.make_async_remote_copy(
            src_ref=hbuf.at[mine(0, half), last_piece(j)], dst_ref=out_hbm.at[mine(0, half), last_piece(j)],
            send_sem=s3_send.at[0, j // AR_CHUNKS, j % AR_CHUNKS], recv_sem=s3_recv.at[0, j // AR_CHUNKS, j % AR_CHUNKS],
            device_id=partner, device_id_type=MESH)

    def last_own(j):
        return pltpu.make_async_copy(hbuf.at[mine(0, half), last_piece(j)], out_hbm.at[mine(0, half), last_piece(j)], out_sem.at[j])

    def last_chip_sum(j):
        last_to_partner(j).wait_recv()

        def add(r):
            own = pbuf[mine(r, 16), last_piece(j)].astype(F32)
            tx2[0, pl.ds(r, 16), last_piece(j)] = (own + rx1[0, pl.ds(r, 16), last_piece(j)].astype(F32)).astype(BF16)
        blocks(0, half, add)
        last_to_across(j).start()

    for c in range(n_last):
        at = c * w_last
        block_c, in_block = at // WIDE, at % WIDE
        if block_c >= 2 and in_block == 0:
            for i in range(d_cut):
                d_square(block_c, i).wait()

        def down(i, carry):
            n = c * per_piece + i
            if block_c < 2:
                landed(2 * n, d_ff)
                landed(2 * n + 1, d_ff)
                y = jnp.dot(act[...], beside(2 * n, 2 * n + 1, d_ff), preferred_element_type=F32)
            else:
                y = None
                for k in range(d_cut):
                    row, rest = k * WIDE, min(WIDE, d_ff - k * WIDE)
                    w = pw[(block_c - 2) * d_cut + k, 0:rest, pl.ds(pl.multiple_of(in_block + i * COLS, COLS), COLS)]
                    z = jnp.dot(act[:, row:row + rest], w, preferred_element_type=F32)
                    y = z if y is None else y + z
            pbuf[:, pl.ds(pl.multiple_of(n * COLS, COLS), COLS)] = y.astype(BF16)
            return carry
        lax.fori_loop(0, per_piece, down, 0)
        last_to_partner(c).start()
        if c > 1:
            last_chip_sum(c - 2)
    last_chip_sum(n_last - 2)
    last_chip_sum(n_last - 1)

    for j in range(n_last):
        last_to_across(j).wait_recv()

        def add(r):
            both = tx2[0, pl.ds(r, 16), last_piece(j)].astype(F32) + rx2[0, pl.ds(r, 16), last_piece(j)].astype(F32)
            hbuf[mine(r, 16), last_piece(j)] = (res[pl.ds(r, 16), last_piece(j)] + both).astype(BF16)
        blocks(0, half, add)
        last_back(j).start()
        last_own(j).start()
    for j in range(n_last):
        last_to_partner(j).wait_send()
        last_to_across(j).wait_send()
        last_back(j).wait()
        last_own(j).wait()


def rest_of_layer(x_in, part, norm_cross, norm_mlp, enc_mask, cross_k, cross_v, cross_q, cross_o, w_gate, w_up, w_down):
    rows, d_model = x_in.shape
    _, src_len, n_head, d_head = cross_k.shape
    inner = n_head * d_head
    d_ff = w_gate.shape[1]
    half = rows // 2
    flat = (rows * inner, src_len)
    k_flat = cross_k.transpose(0, 2, 3, 1).reshape(flat)
    v_flat = cross_v.transpose(0, 2, 3, 1).reshape(flat)
    square = (d_model // 128, 128)
    return pl.pallas_call(
        functools.partial(cross_kernel, n_head),
        out_shape=jax.ShapeDtypeStruct((rows, d_model), BF16),
        in_specs=[ANY] * 12,
        out_specs=ANY,
        scratch_shapes=[
            pltpu.VMEM((RING, d_model, LANES), BF16),
            pltpu.VMEM((8, WIDE, WIDE), BF16),
            pltpu.VMEM((8, d_model // 2, 512), BF16),
            pltpu.VMEM((rows, d_model), BF16),
            pltpu.VMEM((rows, d_model), BF16),
            pltpu.VMEM((half, d_model), F32),
            pltpu.VMEM((half, d_model), BF16),
            pltpu.VMEM((2, half, d_model), BF16),
            pltpu.VMEM((2, half, d_model), BF16),
            pltpu.VMEM((2, half, d_model), BF16),
            pltpu.VMEM((rows, inner), F32),
            pltpu.VMEM((rows, inner), F32),
            pltpu.VMEM((rows, d_ff), BF16),
            pltpu.VMEM((2,) + square, BF16),
            pltpu.VMEM((2, d_model), F32),
            pltpu.VMEM((rows, src_len), jnp.int32),
            pltpu.SemaphoreType.DMA((RING,)),
            pltpu.SemaphoreType.DMA((8,)),
            pltpu.SemaphoreType.DMA((8,)),
            pltpu.SemaphoreType.DMA((AR_CHUNKS,)),
            pltpu.SemaphoreType.DMA((4,)),
            pltpu.SemaphoreType.DMA((2, 2, AR_CHUNKS)),
            pltpu.SemaphoreType.DMA((2, 2, AR_CHUNKS)),
            pltpu.SemaphoreType.DMA((2, 2, AR_CHUNKS)),
            pltpu.SemaphoreType.DMA((2, 2, AR_CHUNKS)),
            pltpu.SemaphoreType.DMA((2, 2, AR_CHUNKS)),
            pltpu.SemaphoreType.DMA((2, 2, AR_CHUNKS)),
            pltpu.SemaphoreType.DMA((2 * AR_CHUNKS,)),
        ],
        compiler_params=pltpu.CompilerParams(vmem_limit_bytes=67_000_000, collective_id=0, has_side_effects=True),
        name="rest_part",
    )(x_in, part, norm_cross.reshape(square), norm_mlp.reshape(square), enc_mask, cross_q, k_flat, v_flat, cross_o, w_gate, w_up, w_down)


def solution(mesh):
    def local_layer(x_in, tok_pos, self_k, self_v, cross_k, cross_v, enc_mask, rel_bias, w_q, w_k, w_v, w_o, cross_q, cross_o, w_gate, w_up, w_down, norm_self, norm_cross, norm_mlp):
        part, new_self_k, new_self_v = self_attention(x_in, norm_self, tok_pos, rel_bias, w_q, w_k, w_v, w_o, self_k, self_v)
        x_out = rest_of_layer(x_in, part, norm_cross, norm_mlp, enc_mask, cross_k, cross_v, cross_q, cross_o, w_gate, w_up, w_down)
        return x_out, new_self_k, new_self_v

    cache_spec = P('dp', None, 'tp', None)
    split_cols = P(None, 'tp')
    split_rows = P('tp', None)
    in_specs = (P('dp', None), P('dp'), cache_spec, cache_spec, cache_spec, cache_spec, P('dp', None), split_cols, split_cols, split_cols, split_cols, split_rows, split_cols, split_rows, split_cols, split_cols, split_rows, P(None), P(None), P(None))
    out_specs = (P('dp', None), cache_spec, cache_spec)
    return jax.shard_map(local_layer, mesh=mesh, in_specs=in_specs, out_specs=out_specs, check_vma=False)
```

```python
import functools
import math
import jax
import jax.numpy as jnp
from jax import lax
from jax.experimental import pallas as pl
from jax.experimental.pallas import tpu as pltpu
from jax.sharding import PartitionSpec as P

BUCKET_EDGES = tuple(int(math.ceil(16.0 * 8.0 ** (bucket_step / 16.0))) for bucket_step in range(1, 16))
NEG_FILL = -1e30
F32 = jnp.float32
BF16 = jnp.bfloat16
ANY = pl.BlockSpec(memory_space=pl.ANY)
VMEM = pl.BlockSpec(memory_space=pltpu.VMEM)
COLS = 256
T_BLOCK = 8


def multiple_of(at, n):
    return at if isinstance(at, int) else pl.multiple_of(at, n)


def twice(n, body):
    def pair(i, carry):
        body(2 * i, carry)
        body(2 * i + 1, carry)
        return carry
    if n == 2:
        pair(0, 0)
    else:
        lax.fori_loop(0, n // 2, pair, 0)


def lay_row(dst, at, norm):
    values = norm[...].astype(F32)
    for i in range(values.shape[0]):
        dst[at:at + 1, i * 128:(i + 1) * 128] = values[i:i + 1, :]


def self_kernel(x_hbm, norm_hbm, pos_hbm, rel_hbm, wq_hbm, wk_hbm, wv_hbm, wo_hbm, k_hbm, v_hbm,
                part_hbm, newk_hbm, newv_hbm,
                xbuf, hbuf, wbuf, kvbuf, sum_ref, q_ref, kn_ref, hit_ref, score_ref, acc_ref,
                norm_ref, nrow, pos_ref, rel_ref,
                x_sem, small_sem, w_sem, kv_sem, out_sem, part_sem, window):
    rows, d_model = xbuf.shape
    n_w = wbuf.shape[0]
    per_mat = n_w // 3
    n_chunk = kvbuf.shape[0] // 2
    n_head, t_len = score_ref.shape[0], score_ref.shape[1]
    inner = acc_ref.shape[0]
    d_head = inner // n_head
    chunk_rows = kvbuf.shape[1]
    sub = d_head // 16
    k_rows = wbuf.shape[1]
    n_wo = wo_hbm.shape[1] // inner

    def w_copy(c):
        src = (wq_hbm, wk_hbm, wv_hbm)[c // per_mat]
        return pltpu.make_async_copy(src.at[pl.ds((c % per_mat) * k_rows, k_rows)], wbuf.at[c], w_sem.at[c])

    def kv_copy(i):
        src = k_hbm if i < n_chunk else v_hbm
        return pltpu.make_async_copy(src.at[pl.ds((i % n_chunk) * chunk_rows, chunk_rows)], kvbuf.at[i], kv_sem.at[i])

    def wo_copies(i):
        return [pltpu.make_async_copy(wo_hbm.at[:, pl.ds(i * inner, inner)], wbuf.at[i], w_sem.at[i])]

    loads = [[w_copy(c)] for c in range(n_w)] + [[kv_copy(i)] for i in range(2 * n_chunk)] + [wo_copies(i) for i in range(n_wo)]
    issued = [0]

    def issue(upto):
        while issued[0] < min(upto, len(loads)):
            for copy in loads[issued[0]]:
                copy.start()
            issued[0] += 1

    x_copy = pltpu.make_async_copy(x_hbm, xbuf, x_sem)
    x_copy.start()
    small = [pltpu.make_async_copy(src, dst, small_sem.at[i]) for i, (src, dst) in enumerate(
        ((pos_hbm, pos_ref), (rel_hbm, rel_ref), (norm_hbm, norm_ref)))]
    for copy in small:
        copy.start()
    issue(window)
    for copy in small:
        copy.wait()

    lay_row(nrow, 0, norm_ref)
    pos = pos_ref[...]
    pos16 = jnp.broadcast_to(pos, (16, rows))

    def set_hit(t, carry):
        hit_ref[t] = jnp.where(pos16 == t, 1.0, 0.0).astype(BF16)
        return carry
    lax.fori_loop(0, t_len, set_hit, 0)

    lane = lax.broadcasted_iota(jnp.int32, (n_head, 128), 1)
    bucket = jnp.full((n_head, 128), 16, jnp.int32)
    for edge in BUCKET_EDGES:
        bucket = bucket + (lane >= edge).astype(jnp.int32)
    bucket = jnp.where(lane < 16, lane, bucket)
    rel = rel_ref[...]
    table = jnp.zeros((n_head, 128), F32)
    for b in range(rel.shape[1]):
        table = jnp.where(bucket == b, rel[:, b:b + 1], table)
    acc_ref[0:n_head, :] = table

    x_copy.wait()
    block = 16
    norm = nrow[0:1, :]

    def norm_rows(i, carry):
        at = pl.ds(multiple_of(i * block, block), block)
        r = xbuf[at, :].astype(F32)
        inv = lax.rsqrt(jnp.mean(r * r, axis=-1, keepdims=True) + 1e-6)
        hbuf[at, :] = (r * inv * norm).astype(BF16)
        return carry
    lax.fori_loop(0, rows // block, norm_rows, 0)

    for c in range(n_w):
        w_copy(c).wait()
        issue(c + 1 + window)
        k = c % per_mat
        for n in range(inner // COLS):
            here = slice(n * COLS, (n + 1) * COLS)
            y = jnp.dot(hbuf[:, k * k_rows:(k + 1) * k_rows], wbuf[c, :, here], preferred_element_type=F32)
            if k > 0:
                y = y + sum_ref[:, here]
            if k < per_mat - 1:
                sum_ref[:, here] = y
                continue
            y = y.astype(BF16).astype(F32).T
            if c < per_mat:
                q_ref[here, :] = y
            else:
                kn_ref[c // per_mat - 1, here, :] = y.astype(BF16)

    def chunk_out(i):
        dst = newk_hbm if i < n_chunk else newv_hbm
        return pltpu.make_async_copy(kvbuf.at[i], dst.at[pl.ds((i % n_chunk) * chunk_rows, chunk_rows)], out_sem.at[i])

    for j in range(n_chunk):
        kv_copy(j).wait()
        issue(n_w + j + 1 + window)

        def k_head(h, carry):
            at = multiple_of(h * d_head, d_head)
            q = q_ref[pl.ds(at, d_head), :]
            kn = kn_ref[0, pl.ds(at, d_head), :].reshape(sub, 16, rows)
            rows_out = []
            for tt in range(T_BLOCK):
                here = pl.ds(multiple_of(tt * inner + at, d_head), d_head)
                old = kvbuf[j, here, :].reshape(sub, 16, rows)
                hit = hit_ref[j * T_BLOCK + tt] != 0
                new = jnp.where(hit[None], kn, old)
                kvbuf[j, here, :] = new.reshape(d_head, rows)
                prod = new.reshape(d_head, rows).astype(F32) * q
                rows_out.append(jnp.sum(prod, axis=0, keepdims=True))
            score_ref[h, j * T_BLOCK:(j + 1) * T_BLOCK, :] = jnp.concatenate(rows_out, axis=0)
            return carry
        twice(n_head, k_head)
        chunk_out(j).start(priority=1)

    t_iota = lax.broadcasted_iota(jnp.int32, (t_len, rows), 0)
    causal = t_iota <= pos
    back = jnp.maximum(pos - t_iota, 0)

    def soft_head(h, carry):
        line = jnp.broadcast_to(acc_ref[pl.ds(h, 1), :], (t_len, 128))
        s = score_ref[h] + jnp.take_along_axis(line, back, axis=1)
        s = jnp.where(causal, s, NEG_FILL)
        e = jnp.exp(s - jnp.max(s, axis=0, keepdims=True))
        p = e / jnp.sum(e, axis=0, keepdims=True)
        score_ref[h] = p.astype(BF16).astype(F32)
        return carry
    lax.fori_loop(0, n_head, soft_head, 0)

    acc_ref[...] = jnp.zeros_like(acc_ref)
    for j in range(n_chunk):
        kv_copy(n_chunk + j).wait()
        issue(n_w + n_chunk + j + 1 + window)

        def v_head(h, carry):
            at = multiple_of(h * d_head, d_head)
            vn = kn_ref[1, pl.ds(at, d_head), :].reshape(sub, 16, rows)
            p = score_ref[h, j * T_BLOCK:(j + 1) * T_BLOCK, :]
            acc = acc_ref[pl.ds(at, d_head), :]
            for tt in range(T_BLOCK):
                here = pl.ds(multiple_of(tt * inner + at, d_head), d_head)
                old = kvbuf[n_chunk + j, here, :].reshape(sub, 16, rows)
                hit = hit_ref[j * T_BLOCK + tt] != 0
                new = jnp.where(hit[None], vn, old)
                kvbuf[n_chunk + j, here, :] = new.reshape(d_head, rows)
                acc = acc + new.reshape(d_head, rows).astype(F32) * p[tt:tt + 1, :]
            acc_ref[pl.ds(at, d_head), :] = acc
            return carry
        twice(n_head, v_head)
        chunk_out(n_chunk + j).start(priority=1)

    issue(len(loads))
    hbuf[:, 0:inner] = acc_ref[...].T.astype(BF16)
    part_copies = []
    for i in range(n_wo):
        for copy in wo_copies(i):
            copy.wait()
        for r in range(inner // COLS):
            at = i * inner + r * COLS
            y = jnp.dot(hbuf[:, 0:inner], wbuf[i, :, r * COLS:(r + 1) * COLS], preferred_element_type=F32)
            xbuf[:, at:at + COLS] = y.astype(BF16)
        here = pl.ds(i * inner, inner)
        copy = pltpu.make_async_copy(xbuf.at[:, here], part_hbm.at[:, here], part_sem.at[i])
        copy.start()
        part_copies.append(copy)
    for i in range(2 * n_chunk):
        chunk_out(i).wait()
    for copy in part_copies:
        copy.wait()


def self_attention(x_in, norm_self, tok_pos, rel_bias, w_q, w_k, w_v, w_o, self_k, self_v):
    rows, t_len, n_head, d_head = self_k.shape
    d_model = x_in.shape[1]
    inner = n_head * d_head
    flat = (t_len * inner, rows)
    k_flat = self_k.transpose(1, 2, 3, 0).reshape(flat)
    v_flat = self_v.transpose(1, 2, 3, 0).reshape(flat)
    n_w = 3 * (d_model // inner)
    n_chunk = t_len // T_BLOCK
    n_wo = w_o.shape[1] // inner

    def body(*refs):
        self_kernel(*refs, window=8)

    part, new_k, new_v = pl.pallas_call(
        body,
        out_shape=(jax.ShapeDtypeStruct((rows, w_o.shape[1]), BF16),
                   jax.ShapeDtypeStruct(flat, BF16), jax.ShapeDtypeStruct(flat, BF16)),
        in_specs=[ANY] * 10,
        out_specs=(ANY, ANY, ANY),
        scratch_shapes=[
            pltpu.VMEM((rows, d_model), BF16),
            pltpu.VMEM((rows, d_model), BF16),
            pltpu.VMEM((n_w, inner, inner), BF16),
            pltpu.VMEM((2 * n_chunk, T_BLOCK * inner, rows), BF16),
            pltpu.VMEM((rows, inner), F32),
            pltpu.VMEM((inner, rows), F32),
            pltpu.VMEM((2, inner, rows), BF16),
            pltpu.VMEM((t_len, 16, rows), BF16),
            pltpu.VMEM((n_head, t_len, rows), F32),
            pltpu.VMEM((inner, rows), F32),
            pltpu.VMEM((d_model // 128, 128), BF16),
            pltpu.VMEM((1, d_model), F32),
            pltpu.VMEM((1, rows), jnp.int32),
            pltpu.VMEM(rel_bias.shape[::-1], F32),
            pltpu.SemaphoreType.DMA,
            pltpu.SemaphoreType.DMA((3,)),
            pltpu.SemaphoreType.DMA((n_w,)),
            pltpu.SemaphoreType.DMA((2 * n_chunk,)),
            pltpu.SemaphoreType.DMA((2 * n_chunk,)),
            pltpu.SemaphoreType.DMA((n_wo,)),
        ],
        compiler_params=pltpu.CompilerParams(vmem_limit_bytes=66_900_000),
        cost_estimate=pl.CostEstimate(flops=4_400_000_000, bytes_accessed=104_000_000, transcendentals=131_072),
        name="self_part",
    )(x_in, norm_self.reshape(d_model // 128, 128), tok_pos.reshape(1, rows), rel_bias.T, w_q, w_k, w_v, w_o, k_flat, v_flat)

    def unflat(cache):
        return cache.reshape(t_len, n_head, d_head, rows).transpose(3, 0, 1, 2)
    return part, unflat(new_k), unflat(new_v)


RING = 20
WIDE = 1024
GROUP = 8
AR_CHUNKS = 4
LANES = 128


def cross_kernel(n_head, x_hbm, part_hbm, ncross_hbm, nmlp_hbm, mask_hbm, cq_hbm, ck_hbm, cv_hbm, co_hbm, wg_hbm, wu_hbm, wd_hbm,
                 out_hbm,
                 ring, pw, gw, pbuf, hbuf, res, xhalf, rx1, tx2, rx2, q_ref, mix_ref, p_ref, act, norm_in, nrow, mask_ref,
                 ring_sem, p_sem, g_sem, load_sem, small_sem, s1_send, s1_recv, s2_send, s2_recv, s3_send, s3_recv, out_sem):
    rows, d_model = hbuf.shape
    half = rows // 2
    part = half // 2
    depth = ring.shape[1]
    inner = q_ref.shape[1]
    d_ff = act.shape[1]
    width = d_model // AR_CHUNKS
    MESH = pl.DeviceIdType.MESH

    me = lax.axis_index("tp")
    core = lax.rem(me, 2)
    chip = me // 2
    partner = {"tp": chip * 2 + (1 - core)}
    across = {"tp": (1 - chip) * 2 + core}

    def mine(at, n):
        return pl.ds(multiple_of(core * half + at, 16), n)

    def theirs(at, n):
        return pl.ds(multiple_of((1 - core) * half + at, 16), n)

    def piece(j):
        return pl.ds(j * width, width)

    per_step = GROUP * inner // depth
    n_step = rows // GROUP
    ahead = RING // (2 * per_step)
    n_sq = pw.shape[0] // 2
    g_rows, g_cols = gw.shape[1:]
    g_cut = d_model // g_rows
    n_pair = gw.shape[0] // (2 * g_cut)

    def copy_in(src, slot, used=None):
        dst = ring.at[slot] if used is None else ring.at[slot, used]
        pltpu.make_async_copy(src, dst, ring_sem.at[slot]).start()

    def landed(slot, used=depth):
        pltpu.make_async_copy(ck_hbm.at[pl.ds(0, used)], ring.at[slot, pl.ds(0, used)], ring_sem.at[slot]).wait()

    def group_of(step):
        per_half, u = n_step // 2, step % (n_step // 2)
        return (step // per_half) * (part // GROUP) + u + (u // (part // GROUP)) * (part // GROUP)

    def kv_slot(step, value):
        return (ahead * value + step % ahead) * per_step

    def issue_kv(step, value):
        src = cv_hbm if value else ck_hbm
        for i in range(per_step):
            at = multiple_of((group_of(step) * per_step + i) * depth, depth)
            copy_in(src.at[pl.ds(at, depth)], kv_slot(step, value) + i)

    def q_copy(k):
        return pltpu.make_async_copy(cq_hbm.at[pl.ds(k * WIDE, WIDE)], pw.at[k], p_sem.at[k])

    def o_copy(i):
        return pltpu.make_async_copy(co_hbm.at[:, pl.ds(i * WIDE, WIDE)], pw.at[n_sq + i], p_sem.at[n_sq + i])

    def gu_square(i):
        src = wg_hbm if i < n_sq else wu_hbm
        return pltpu.make_async_copy(src.at[pl.ds((i % n_sq) * WIDE, WIDE), pl.ds(0, WIDE)], pw.at[i], p_sem.at[i])

    def gu_tall(pair, i):
        src = wg_hbm if i < g_cut else wu_hbm
        slot = (pair % n_pair) * 2 * g_cut + i
        return pltpu.make_async_copy(src.at[pl.ds((i % g_cut) * g_rows, g_rows), pl.ds(WIDE + pair * g_cols, g_cols)],
                                     gw.at[slot], g_sem.at[slot])

    d_cut = -(-d_ff // WIDE)
    d_narrow = 2 * WIDE // LANES

    def d_square(c, i):
        slot = (c - 2) * d_cut + i
        n = min(WIDE, d_ff - i * WIDE)
        return pltpu.make_async_copy(wd_hbm.at[pl.ds(i * WIDE, n), pl.ds(c * WIDE, WIDE)],
                                     pw.at[slot, pl.ds(0, n)], p_sem.at[slot])

    def issue_d(i):
        copy_in(wd_hbm.at[:, pl.ds(i * LANES, LANES)], i, pl.ds(0, d_ff))

    def to_partner(a, h, j, at, n):
        return pltpu.make_async_remote_copy(
            src_ref=pbuf.at[theirs(at, n), piece(j)], dst_ref=rx1.at[a % 2, pl.ds(at, n), piece(j)],
            send_sem=s1_send.at[a % 2, h, j], recv_sem=s1_recv.at[a % 2, h, j], device_id=partner, device_id_type=MESH)

    def to_across(a, h, j, at, n):
        return pltpu.make_async_remote_copy(
            src_ref=tx2.at[a % 2, pl.ds(at, n), piece(j)], dst_ref=rx2.at[a % 2, pl.ds(at, n), piece(j)],
            send_sem=s2_send.at[a % 2, h, j], recv_sem=s2_recv.at[a % 2, h, j], device_id=across, device_id_type=MESH)

    def blocks(at, n, fn):
        def body(i, carry):
            fn(multiple_of(at + i * 16, 16))
            return carry
        lax.fori_loop(0, n // 16, body, 0)

    def chip_sum(a, h, j, at, n):
        to_partner(a, h, j, at, n).wait_recv()

        def add(r):
            own = pbuf[mine(r, 16), piece(j)].astype(F32)
            tx2[a % 2, pl.ds(r, 16), piece(j)] = (own + rx1[a % 2, pl.ds(r, 16), piece(j)].astype(F32)).astype(BF16)
        blocks(at, n, add)
        to_across(a, h, j, at, n).start()

    def full_sum(a, h, j, at, n):
        to_across(a, h, j, at, n).wait_recv()

        def add(r):
            both = tx2[a % 2, pl.ds(r, 16), piece(j)].astype(F32) + rx2[a % 2, pl.ds(r, 16), piece(j)].astype(F32)
            res[pl.ds(r, 16), piece(j)] = res[pl.ds(r, 16), piece(j)] + both
        blocks(at, n, add)

    def sent(a, h, at, n):
        for j in range(AR_CHUNKS):
            to_partner(a, h, j, at, n).wait_send()
            to_across(a, h, j, at, n).wait_send()

    def rows_back(a, h, i):
        at = mine(h * part + i * 16, 16)
        return pltpu.make_async_remote_copy(
            src_ref=hbuf.at[at], dst_ref=hbuf.at[at], send_sem=s3_send.at[a % 2, h, i],
            recv_sem=s3_recv.at[a % 2, h, i], device_id=partner, device_id_type=MESH)

    def normalise(a, h):
        norm = nrow[a:a + 1, :]
        for i in range(part // 16):
            r = res[h * part + i * 16:h * part + (i + 1) * 16, :]
            inv = lax.rsqrt(jnp.mean(r * r, axis=-1, keepdims=True) + 1e-6)
            hbuf[mine(h * part + i * 16, 16), :] = (r * inv * norm).astype(BF16)
            rows_back(a, h, i).start()

    def all_rows(a, h):
        for i in range(part // 16):
            rows_back(a, h, i).wait()

    pieces = range(AR_CHUNKS)
    halves = range(2)
    first = [pltpu.make_async_copy(part_hbm.at[:, piece(j)], pbuf.at[:, piece(j)], load_sem.at[j]) for j in pieces]
    for copy in first:
        copy.start()
    small = [pltpu.make_async_copy(src, dst, small_sem.at[i]) for i, (src, dst) in enumerate(
        ((x_hbm.at[mine(0, half)], xhalf), (ncross_hbm, norm_in.at[0]), (nmlp_hbm, norm_in.at[1]), (mask_hbm, mask_ref)))]
    for copy in small:
        copy.start()
    barrier = pltpu.get_barrier_semaphore()
    for other in (partner, across):
        pl.semaphore_signal(barrier, inc=1, device_id=other, device_id_type=MESH)
    pl.semaphore_wait(barrier, 2)

    for j in pieces:
        first[j].wait()
        to_partner(0, 0, j, 0, part).start()
    for j in pieces:
        to_partner(0, 1, j, part, part).start()
    for k in range(n_sq):
        q_copy(k).start()
    for step in range(ahead):
        issue_kv(step, 0)
        issue_kv(step, 1)
    for i in range(n_sq):
        o_copy(i).start()
    for i in range(2 * g_cut):
        gu_tall(0, i).start()
    for h in halves:
        for j in pieces:
            chip_sum(0, h, j, h * part, part)
    for copy in small:
        copy.wait()
    lay_row(nrow, 0, norm_in.at[0])
    lay_row(nrow, 1, norm_in.at[1])
    blocks(0, half, lambda r: res.__setitem__((pl.ds(r, 16), slice(None)), xhalf[pl.ds(r, 16), :].astype(F32)))

    def beside(a, b, used=depth):
        return jnp.concatenate([ring[a, 0:used, :], ring[b, 0:used, :]], axis=1)

    def both_cores(ref, h, at=slice(None)):
        return jnp.concatenate([ref[h * part:(h + 1) * part, at], ref[half + h * part:half + (h + 1) * part, at]], axis=0)

    def project_q(h):
        if h == 0:
            for k in range(n_sq):
                q_copy(k).wait()

        def block(n, carry):
            here = pl.ds(multiple_of(n * COLS, COLS), COLS)
            y = None
            for k in range(n_sq):
                z = jnp.dot(both_cores(hbuf, h, slice(k * WIDE, (k + 1) * WIDE)), pw[k, :, here], preferred_element_type=F32)
                y = z if y is None else y + z
            y = y.astype(BF16).astype(F32)
            q_ref[h * part:(h + 1) * part, here] = y[0:part]
            q_ref[half + h * part:half + (h + 1) * part, here] = y[part:]
            return carry
        twice(inner // COLS, block)

    own_head = (lax.broadcasted_iota(jnp.int32, (n_head, inner), 1) // (inner // n_head)
                == lax.broadcasted_iota(jnp.int32, (n_head, inner), 0))
    in_slot = GROUP // per_step

    def rows_of(slot, r):
        here = pl.ds(r * inner, inner)
        return jnp.concatenate([ring[slot, here, :], ring[slot + 1, here, :]], axis=1)

    def group_rows(step):
        return pl.ds(multiple_of(group_of(step) * GROUP, GROUP), GROUP)

    def score_dots(step):
        q8 = q_ref[group_rows(step), :]

        def spread(r):
            return jnp.where(own_head, jnp.broadcast_to(q8[r:r + 1, :], (n_head, inner)), 0.0).astype(BF16)
        return [jnp.dot(jnp.concatenate([spread(r), spread(r + in_slot)], axis=0), rows_of(kv_slot(step, 0), r),
                        preferred_element_type=F32) for r in range(in_slot)]

    def probabilities(step, dots):
        m8 = mask_ref[group_rows(step), :]
        scores = [s[0:n_head, 0:LANES] for s in dots] + [s[n_head:, LANES:] for s in dots]
        s = jnp.concatenate([jnp.where(m8[r:r + 1, :] != 0, scores[r], NEG_FILL) for r in range(GROUP)], axis=0)
        e = jnp.exp(s - jnp.max(s, axis=1, keepdims=True))
        p_ref[...] = (e / jnp.sum(e, axis=1, keepdims=True)).astype(BF16)

    def value_dots(step, p):
        none = jnp.zeros((n_head, LANES), BF16)
        out = []
        for r in range(in_slot):
            pa = p[r * n_head:(r + 1) * n_head, :]
            pb = p[(r + in_slot) * n_head:(r + in_slot + 1) * n_head, :]
            lhs = jnp.concatenate([jnp.concatenate([pa, none], axis=1), jnp.concatenate([none, pb], axis=1)], axis=0)
            out.append(lax.dot_general(lhs, rows_of(kv_slot(step, 1), r), (((1,), (1,)), ((), ())), preferred_element_type=F32))
        return out

    def store_mixed(step, dots):
        mixed = [y[0:n_head] for y in dots] + [y[n_head:] for y in dots]
        mix_ref[group_rows(step), :] = jnp.concatenate(
            [jnp.sum(jnp.where(own_head, y, 0.0), axis=0, keepdims=True) for y in mixed], axis=0)

    def wait_kv(step, value):
        for i in range(per_step):
            landed(kv_slot(step, value) + i)

    def refill(step, value):
        if isinstance(step, int):
            if step < n_step:
                issue_kv(step, value)
            return

        @pl.when(step < n_step)
        def _():
            issue_kv(step, value)

    def attend(lo, hi):
        wait_kv(lo, 0)
        probabilities(lo, score_dots(lo))
        refill(lo + ahead, 0)

        def body(step, carry):
            wait_kv(step + 1, 0)
            wait_kv(step, 1)
            p = p_ref[...]
            dots = score_dots(step + 1)
            values = value_dots(step, p)
            probabilities(step + 1, dots)
            store_mixed(step, values)
            refill(step + 1 + ahead, 0)
            refill(step + ahead, 1)
            return carry
        lax.fori_loop(lo, hi - 1, body, 0)
        wait_kv(hi - 1, 1)
        store_mixed(hi - 1, value_dots(hi - 1, p_ref[...]))
        refill(hi - 1 + ahead, 1)

    def project_o(h, after):
        lhs = both_cores(mix_ref, h).astype(BF16)
        for j in pieces:
            if h == 0:
                o_copy(j).wait()
            for n in range(WIDE // COLS):
                y = jnp.dot(lhs, pw[n_sq + j, :, n * COLS:(n + 1) * COLS], preferred_element_type=F32).astype(BF16)
                here = slice(j * WIDE + n * COLS, j * WIDE + (n + 1) * COLS)
                pbuf[h * part:(h + 1) * part, here] = y[0:part]
                pbuf[half + h * part:half + (h + 1) * part, here] = y[part:]
            to_partner(1, h, j, h * part, part).start()
            if after and j > 0:
                chip_sum(1, h, j - 1, h * part, part)
        if after:
            chip_sum(1, h, AR_CHUNKS - 1, h * part, part)

    for j in pieces:
        full_sum(0, 0, j, 0, part)
    normalise(0, 0)
    all_rows(0, 0)
    project_q(0)
    attend(0, n_step // 2)
    sent(0, 0, 0, part)
    project_o(0, False)
    for j in pieces:
        full_sum(0, 1, j, part, part)
    normalise(0, 1)
    for j in pieces:
        chip_sum(1, 0, j, 0, part)
    all_rows(0, 1)
    project_q(1)
    attend(n_step // 2, n_step)
    for pair in range(1, n_pair):
        for i in range(2 * g_cut):
            gu_tall(pair, i).start()
    for i in range(n_sq):
        gu_square(i).start()
    sent(0, 1, part, part)
    project_o(1, True)
    for i in range(n_sq):
        gu_square(n_sq + i).start()
    for i in range(d_narrow):
        issue_d(i)
    for j in pieces:
        full_sum(1, 0, j, 0, part)
    normalise(1, 0)
    for j in pieces:
        full_sum(1, 1, j, part, part)
    normalise(1, 1)
    for h in halves:
        all_rows(1, h)
        sent(1, h, h * part, part)

    root = math.sqrt(2.0 / math.pi)
    def mlp_block(at, gate, up):
        u, v = None, None
        for k in range(len(gate)):
            n = d_model // len(gate)
            lhs = hbuf[:, k * n:(k + 1) * n]
            y = jnp.dot(lhs, gate[k], preferred_element_type=F32)
            z = jnp.dot(lhs, up[k], preferred_element_type=F32)
            u, v = (y, z) if u is None else (u + y, v + z)
        gelu = 0.5 * u * (1.0 + jnp.tanh(root * (u + 0.044715 * (u * u * u))))
        act[:, pl.ds(at, COLS)] = (gelu * v).astype(BF16)

    def mlp_tall(pair):
        for i in range(2 * g_cut):
            gu_tall(pair, i).wait()
        base = (pair % n_pair) * 2 * g_cut

        def block(n, carry):
            here = pl.ds(multiple_of(n * COLS, COLS), COLS)
            mlp_block(multiple_of(WIDE + pair * g_cols + n * COLS, COLS), [gw[base + i, :, here] for i in range(g_cut)],
                      [gw[base + g_cut + i, :, here] for i in range(g_cut)])
            return carry
        twice(g_cols // COLS, block)

    def mlp_square():
        for i in range(2 * n_sq):
            gu_square(i).wait()

        def block(n, carry):
            here = pl.ds(multiple_of(n * COLS, COLS), COLS)
            mlp_block(multiple_of(n * COLS, COLS), [pw[i, :, here] for i in range(n_sq)],
                      [pw[n_sq + i, :, here] for i in range(n_sq)])
            return carry
        twice(WIDE // COLS, block)

    n_tall = (d_ff - WIDE) // g_cols
    for pair in range(n_pair):
        mlp_tall(pair)
        if pair + n_pair < n_tall:
            for i in range(2 * g_cut):
                gu_tall(pair + n_pair, i).start()
    mlp_square()
    for c in (2, 3):
        for i in range(d_cut):
            d_square(c, i).start()
    for pair in range(n_pair, n_tall):
        mlp_tall(pair)

    n_last = 2 * AR_CHUNKS
    w_last = d_model // n_last
    per_piece = w_last // COLS

    def last_piece(j):
        return pl.ds(j * w_last, w_last)

    def last_to_partner(j):
        return pltpu.make_async_remote_copy(
            src_ref=pbuf.at[theirs(0, half), last_piece(j)], dst_ref=rx1.at[0, :, last_piece(j)],
            send_sem=s1_send.at[0, j // AR_CHUNKS, j % AR_CHUNKS], recv_sem=s1_recv.at[0, j // AR_CHUNKS, j % AR_CHUNKS],
            device_id=partner, device_id_type=MESH)

    def last_to_across(j):
        return pltpu.make_async_remote_copy(
            src_ref=tx2.at[0, :, last_piece(j)], dst_ref=rx2.at[0, :, last_piece(j)],
            send_sem=s2_send.at[0, j // AR_CHUNKS, j % AR_CHUNKS], recv_sem=s2_recv.at[0, j // AR_CHUNKS, j % AR_CHUNKS],
            device_id=across, device_id_type=MESH)

    def last_back(j):
        return pltpu.make_async_remote_copy(
            src_ref=hbuf.at[mine(0, half), last_piece(j)], dst_ref=out_hbm.at[mine(0, half), last_piece(j)],
            send_sem=s3_send.at[0, j // AR_CHUNKS, j % AR_CHUNKS], recv_sem=s3_recv.at[0, j // AR_CHUNKS, j % AR_CHUNKS],
            device_id=partner, device_id_type=MESH)

    def last_own(j):
        return pltpu.make_async_copy(hbuf.at[mine(0, half), last_piece(j)], out_hbm.at[mine(0, half), last_piece(j)], out_sem.at[j])

    def last_chip_sum(j):
        last_to_partner(j).wait_recv()

        def add(r):
            own = pbuf[mine(r, 16), last_piece(j)].astype(F32)
            tx2[0, pl.ds(r, 16), last_piece(j)] = (own + rx1[0, pl.ds(r, 16), last_piece(j)].astype(F32)).astype(BF16)
        blocks(0, half, add)
        last_to_across(j).start()

    for c in range(n_last):
        at = c * w_last
        block_c, in_block = at // WIDE, at % WIDE
        if block_c >= 2 and in_block == 0:
            for i in range(d_cut):
                d_square(block_c, i).wait()

        def down(i, carry):
            n = c * per_piece + i
            if block_c < 2:
                landed(2 * n, d_ff)
                landed(2 * n + 1, d_ff)
                y = jnp.dot(act[...], beside(2 * n, 2 * n + 1, d_ff), preferred_element_type=F32)
            else:
                y = None
                for k in range(d_cut):
                    row, rest = k * WIDE, min(WIDE, d_ff - k * WIDE)
                    w = pw[(block_c - 2) * d_cut + k, 0:rest, pl.ds(multiple_of(in_block + i * COLS, COLS), COLS)]
                    z = jnp.dot(act[:, row:row + rest], w, preferred_element_type=F32)
                    y = z if y is None else y + z
            pbuf[:, pl.ds(multiple_of(n * COLS, COLS), COLS)] = y.astype(BF16)
            return carry
        twice(per_piece, down)
        last_to_partner(c).start()
        if c > 1:
            last_chip_sum(c - 2)
    last_chip_sum(n_last - 2)
    last_chip_sum(n_last - 1)

    for j in range(n_last):
        last_to_across(j).wait_recv()

        def add(r):
            both = tx2[0, pl.ds(r, 16), last_piece(j)].astype(F32) + rx2[0, pl.ds(r, 16), last_piece(j)].astype(F32)
            hbuf[mine(r, 16), last_piece(j)] = (res[pl.ds(r, 16), last_piece(j)] + both).astype(BF16)
        blocks(0, half, add)
        last_back(j).start()
        last_own(j).start()
    for j in range(n_last):
        last_to_partner(j).wait_send()
        last_to_across(j).wait_send()
        last_back(j).wait()
        last_own(j).wait()


def rest_of_layer(x_in, part, norm_cross, norm_mlp, enc_mask, cross_k, cross_v, cross_q, cross_o, w_gate, w_up, w_down):
    rows, d_model = x_in.shape
    _, src_len, n_head, d_head = cross_k.shape
    inner = n_head * d_head
    d_ff = w_gate.shape[1]
    half = rows // 2
    flat = (rows * inner, src_len)
    k_flat = cross_k.transpose(0, 2, 3, 1).reshape(flat)
    v_flat = cross_v.transpose(0, 2, 3, 1).reshape(flat)
    square = (d_model // 128, 128)
    return pl.pallas_call(
        functools.partial(cross_kernel, n_head),
        out_shape=jax.ShapeDtypeStruct((rows, d_model), BF16),
        in_specs=[ANY] * 12,
        out_specs=ANY,
        scratch_shapes=[
            pltpu.VMEM((RING, d_model, LANES), BF16),
            pltpu.VMEM((8, WIDE, WIDE), BF16),
            pltpu.VMEM((8, d_model // 2, 512), BF16),
            pltpu.VMEM((rows, d_model), BF16),
            pltpu.VMEM((rows, d_model), BF16),
            pltpu.VMEM((half, d_model), F32),
            pltpu.VMEM((half, d_model), BF16),
            pltpu.VMEM((2, half, d_model), BF16),
            pltpu.VMEM((2, half, d_model), BF16),
            pltpu.VMEM((2, half, d_model), BF16),
            pltpu.VMEM((rows, inner), F32),
            pltpu.VMEM((rows, inner), F32),
            pltpu.VMEM((GROUP * n_head, src_len), BF16),
            pltpu.VMEM((rows, d_ff), BF16),
            pltpu.VMEM((2,) + square, BF16),
            pltpu.VMEM((2, d_model), F32),
            pltpu.VMEM((rows, src_len), jnp.int32),
            pltpu.SemaphoreType.DMA((RING,)),
            pltpu.SemaphoreType.DMA((8,)),
            pltpu.SemaphoreType.DMA((8,)),
            pltpu.SemaphoreType.DMA((AR_CHUNKS,)),
            pltpu.SemaphoreType.DMA((4,)),
            pltpu.SemaphoreType.DMA((2, 2, AR_CHUNKS)),
            pltpu.SemaphoreType.DMA((2, 2, AR_CHUNKS)),
            pltpu.SemaphoreType.DMA((2, 2, AR_CHUNKS)),
            pltpu.SemaphoreType.DMA((2, 2, AR_CHUNKS)),
            pltpu.SemaphoreType.DMA((2, 2, AR_CHUNKS)),
            pltpu.SemaphoreType.DMA((2, 2, AR_CHUNKS)),
            pltpu.SemaphoreType.DMA((2 * AR_CHUNKS,)),
        ],
        compiler_params=pltpu.CompilerParams(vmem_limit_bytes=67_000_000, collective_id=0, has_side_effects=True),
        name="rest_part",
    )(x_in, part, norm_cross.reshape(square), norm_mlp.reshape(square), enc_mask, cross_q, k_flat, v_flat, cross_o, w_gate, w_up, w_down)


def solution(mesh):
    def local_layer(x_in, tok_pos, self_k, self_v, cross_k, cross_v, enc_mask, rel_bias, w_q, w_k, w_v, w_o, cross_q, cross_o, w_gate, w_up, w_down, norm_self, norm_cross, norm_mlp):
        part, new_self_k, new_self_v = self_attention(x_in, norm_self, tok_pos, rel_bias, w_q, w_k, w_v, w_o, self_k, self_v)
        x_out = rest_of_layer(x_in, part, norm_cross, norm_mlp, enc_mask, cross_k, cross_v, cross_q, cross_o, w_gate, w_up, w_down)
        return x_out, new_self_k, new_self_v

    cache_spec = P('dp', None, 'tp', None)
    split_cols = P(None, 'tp')
    split_rows = P('tp', None)
    in_specs = (P('dp', None), P('dp'), cache_spec, cache_spec, cache_spec, cache_spec, P('dp', None), split_cols, split_cols, split_cols, split_cols, split_rows, split_cols, split_rows, split_cols, split_cols, split_rows, P(None), P(None), P(None))
    out_specs = (P('dp', None), cache_spec, cache_spec)
    return jax.shard_map(local_layer, mesh=mesh, in_specs=in_specs, out_specs=out_specs, check_vma=False)
```

```python
import functools
import math
import jax
import jax.numpy as jnp
from jax import lax
from jax.experimental import pallas as pl
from jax.experimental.pallas import tpu as pltpu
from jax.sharding import PartitionSpec as P

BUCKET_EDGES = tuple(int(math.ceil(16.0 * 8.0 ** (bucket_step / 16.0))) for bucket_step in range(1, 16))
NEG_FILL = -1e30
F32 = jnp.float32
BF16 = jnp.bfloat16
ANY = pl.BlockSpec(memory_space=pl.ANY)
VMEM = pl.BlockSpec(memory_space=pltpu.VMEM)
COLS = 256
T_BLOCK = 8


def multiple_of(at, n):
    return at if isinstance(at, int) else pl.multiple_of(at, n)


def twice(n, body):
    def pair(i, carry):
        body(2 * i, carry)
        body(2 * i + 1, carry)
        return carry
    if n == 2:
        pair(0, 0)
    else:
        lax.fori_loop(0, n // 2, pair, 0)


def lay_row(dst, at, norm):
    values = norm[...].astype(F32)
    for i in range(values.shape[0]):
        dst[at:at + 1, i * 128:(i + 1) * 128] = values[i:i + 1, :]


def self_kernel(x_hbm, norm_hbm, pos_hbm, rel_hbm, wq_hbm, wk_hbm, wv_hbm, k_hbm, v_hbm,
                mixed_hbm, newk_hbm, newv_hbm,
                xbuf, hbuf, wbuf, kvbuf, sum_ref, q_ref, kn_ref, hit_ref, score_ref, acc_ref,
                norm_ref, nrow, pos_ref, rel_ref,
                x_sem, small_sem, w_sem, kv_sem, out_sem, part_sem, window):
    rows, d_model = xbuf.shape
    n_w = wbuf.shape[0]
    per_mat = n_w // 3
    n_chunk = kvbuf.shape[0] // 2
    n_head, t_len = score_ref.shape[0], score_ref.shape[1]
    inner = acc_ref.shape[0]
    d_head = inner // n_head
    chunk_rows = kvbuf.shape[1]
    sub = d_head // 16
    k_rows = wbuf.shape[1]

    def w_copy(c):
        src = (wq_hbm, wk_hbm, wv_hbm)[c // per_mat]
        return pltpu.make_async_copy(src.at[pl.ds((c % per_mat) * k_rows, k_rows)], wbuf.at[c], w_sem.at[c])

    def kv_copy(i):
        src = k_hbm if i < n_chunk else v_hbm
        return pltpu.make_async_copy(src.at[pl.ds((i % n_chunk) * chunk_rows, chunk_rows)], kvbuf.at[i], kv_sem.at[i])

    loads = [[w_copy(c)] for c in range(n_w)] + [[kv_copy(i)] for i in range(2 * n_chunk)]
    issued = [0]

    def issue(upto):
        while issued[0] < min(upto, len(loads)):
            for copy in loads[issued[0]]:
                copy.start()
            issued[0] += 1

    x_copy = pltpu.make_async_copy(x_hbm, xbuf, x_sem)
    x_copy.start()
    small = [pltpu.make_async_copy(src, dst, small_sem.at[i]) for i, (src, dst) in enumerate(
        ((pos_hbm, pos_ref), (rel_hbm, rel_ref), (norm_hbm, norm_ref)))]
    for copy in small:
        copy.start()
    issue(window)
    for copy in small:
        copy.wait()

    lay_row(nrow, 0, norm_ref)
    pos = pos_ref[...]
    pos16 = jnp.broadcast_to(pos, (16, rows))

    def set_hit(t, carry):
        hit_ref[t] = jnp.where(pos16 == t, 1.0, 0.0).astype(BF16)
        return carry
    lax.fori_loop(0, t_len, set_hit, 0)

    lane = lax.broadcasted_iota(jnp.int32, (n_head, 128), 1)
    bucket = jnp.full((n_head, 128), 16, jnp.int32)
    for edge in BUCKET_EDGES:
        bucket = bucket + (lane >= edge).astype(jnp.int32)
    bucket = jnp.where(lane < 16, lane, bucket)
    rel = rel_ref[...]
    table = jnp.zeros((n_head, 128), F32)
    for b in range(rel.shape[1]):
        table = jnp.where(bucket == b, rel[:, b:b + 1], table)
    acc_ref[0:n_head, :] = table

    x_copy.wait()
    block = 16
    norm = nrow[0:1, :]

    def norm_rows(i, carry):
        at = pl.ds(multiple_of(i * block, block), block)
        r = xbuf[at, :].astype(F32)
        inv = lax.rsqrt(jnp.mean(r * r, axis=-1, keepdims=True) + 1e-6)
        hbuf[at, :] = (r * inv * norm).astype(BF16)
        return carry
    lax.fori_loop(0, rows // block, norm_rows, 0)

    for c in range(n_w):
        w_copy(c).wait()
        issue(c + 1 + window)
        k = c % per_mat
        for n in range(inner // COLS):
            here = slice(n * COLS, (n + 1) * COLS)
            y = jnp.dot(hbuf[:, k * k_rows:(k + 1) * k_rows], wbuf[c, :, here], preferred_element_type=F32)
            if k > 0:
                y = y + sum_ref[:, here]
            if k < per_mat - 1:
                sum_ref[:, here] = y
                continue
            y = y.astype(BF16).astype(F32).T
            if c < per_mat:
                q_ref[here, :] = y
            else:
                kn_ref[c // per_mat - 1, here, :] = y.astype(BF16)

    def chunk_out(i):
        dst = newk_hbm if i < n_chunk else newv_hbm
        return pltpu.make_async_copy(kvbuf.at[i], dst.at[pl.ds((i % n_chunk) * chunk_rows, chunk_rows)], out_sem.at[i])

    for j in range(n_chunk):
        kv_copy(j).wait()
        issue(n_w + j + 1 + window)

        def k_head(h, carry):
            at = multiple_of(h * d_head, d_head)
            q = q_ref[pl.ds(at, d_head), :]
            kn = kn_ref[0, pl.ds(at, d_head), :].reshape(sub, 16, rows)
            rows_out = []
            for tt in range(T_BLOCK):
                here = pl.ds(multiple_of(tt * inner + at, d_head), d_head)
                old = kvbuf[j, here, :].reshape(sub, 16, rows)
                hit = hit_ref[j * T_BLOCK + tt] != 0
                new = jnp.where(hit[None], kn, old)
                kvbuf[j, here, :] = new.reshape(d_head, rows)
                prod = new.reshape(d_head, rows).astype(F32) * q
                rows_out.append(jnp.sum(prod, axis=0, keepdims=True))
            score_ref[h, j * T_BLOCK:(j + 1) * T_BLOCK, :] = jnp.concatenate(rows_out, axis=0)
            return carry
        twice(n_head, k_head)
        chunk_out(j).start(priority=1)

    t_iota = lax.broadcasted_iota(jnp.int32, (t_len, rows), 0)
    causal = t_iota <= pos
    back = jnp.maximum(pos - t_iota, 0)

    def soft_head(h, carry):
        line = jnp.broadcast_to(acc_ref[pl.ds(h, 1), :], (t_len, 128))
        s = score_ref[h] + jnp.take_along_axis(line, back, axis=1)
        s = jnp.where(causal, s, NEG_FILL)
        e = jnp.exp(s - jnp.max(s, axis=0, keepdims=True))
        p = e / jnp.sum(e, axis=0, keepdims=True)
        score_ref[h] = p.astype(BF16).astype(F32)
        return carry
    lax.fori_loop(0, n_head, soft_head, 0)

    acc_ref[...] = jnp.zeros_like(acc_ref)
    for j in range(n_chunk):
        kv_copy(n_chunk + j).wait()
        issue(n_w + n_chunk + j + 1 + window)

        def v_head(h, carry):
            at = multiple_of(h * d_head, d_head)
            vn = kn_ref[1, pl.ds(at, d_head), :].reshape(sub, 16, rows)
            p = score_ref[h, j * T_BLOCK:(j + 1) * T_BLOCK, :]
            acc = acc_ref[pl.ds(at, d_head), :]
            for tt in range(T_BLOCK):
                here = pl.ds(multiple_of(tt * inner + at, d_head), d_head)
                old = kvbuf[n_chunk + j, here, :].reshape(sub, 16, rows)
                hit = hit_ref[j * T_BLOCK + tt] != 0
                new = jnp.where(hit[None], vn, old)
                kvbuf[n_chunk + j, here, :] = new.reshape(d_head, rows)
                acc = acc + new.reshape(d_head, rows).astype(F32) * p[tt:tt + 1, :]
            acc_ref[pl.ds(at, d_head), :] = acc
            return carry
        twice(n_head, v_head)
        chunk_out(n_chunk + j).start(priority=1)

    issue(len(loads))
    hbuf[:, 0:inner] = acc_ref[...].T.astype(BF16)
    mixed_copy = pltpu.make_async_copy(hbuf.at[:, pl.ds(0, inner)], mixed_hbm, part_sem)
    mixed_copy.start()
    for i in range(2 * n_chunk):
        chunk_out(i).wait()
    mixed_copy.wait()


def self_attention(x_in, norm_self, tok_pos, rel_bias, w_q, w_k, w_v, self_k, self_v):
    rows, t_len, n_head, d_head = self_k.shape
    d_model = x_in.shape[1]
    inner = n_head * d_head
    flat = (t_len * inner, rows)
    k_flat = self_k.transpose(1, 2, 3, 0).reshape(flat)
    v_flat = self_v.transpose(1, 2, 3, 0).reshape(flat)
    n_w = 3 * (d_model // inner)
    n_chunk = t_len // T_BLOCK

    def body(*refs):
        self_kernel(*refs, window=8)

    mixed, new_k, new_v = pl.pallas_call(
        body,
        out_shape=(jax.ShapeDtypeStruct((rows, inner), BF16),
                   jax.ShapeDtypeStruct(flat, BF16), jax.ShapeDtypeStruct(flat, BF16)),
        in_specs=[ANY] * 9,
        out_specs=(ANY, ANY, ANY),
        scratch_shapes=[
            pltpu.VMEM((rows, d_model), BF16),
            pltpu.VMEM((rows, d_model), BF16),
            pltpu.VMEM((n_w, inner, inner), BF16),
            pltpu.VMEM((2 * n_chunk, T_BLOCK * inner, rows), BF16),
            pltpu.VMEM((rows, inner), F32),
            pltpu.VMEM((inner, rows), F32),
            pltpu.VMEM((2, inner, rows), BF16),
            pltpu.VMEM((t_len, 16, rows), BF16),
            pltpu.VMEM((n_head, t_len, rows), F32),
            pltpu.VMEM((inner, rows), F32),
            pltpu.VMEM((d_model // 128, 128), BF16),
            pltpu.VMEM((1, d_model), F32),
            pltpu.VMEM((1, rows), jnp.int32),
            pltpu.VMEM(rel_bias.shape[::-1], F32),
            pltpu.SemaphoreType.DMA,
            pltpu.SemaphoreType.DMA((3,)),
            pltpu.SemaphoreType.DMA((n_w,)),
            pltpu.SemaphoreType.DMA((2 * n_chunk,)),
            pltpu.SemaphoreType.DMA((2 * n_chunk,)),
            pltpu.SemaphoreType.DMA,
        ],
        compiler_params=pltpu.CompilerParams(vmem_limit_bytes=66_900_000),
        cost_estimate=pl.CostEstimate(flops=3_300_000_000, bytes_accessed=95_000_000, transcendentals=131_072),
        name="self_part",
    )(x_in, norm_self.reshape(d_model // 128, 128), tok_pos.reshape(1, rows), rel_bias.T, w_q, w_k, w_v, k_flat, v_flat)

    def unflat(cache):
        return cache.reshape(t_len, n_head, d_head, rows).transpose(3, 0, 1, 2)
    return mixed, unflat(new_k), unflat(new_v)


RING = 20
WIDE = 1024
GROUP = 8
AR_CHUNKS = 4
LANES = 128


def cross_kernel(n_head, x_hbm, mixed_hbm, wo_hbm, ncross_hbm, nmlp_hbm, mask_hbm, cq_hbm, ck_hbm, cv_hbm, co_hbm, wg_hbm, wu_hbm, wd_hbm,
                 out_hbm,
                 ring, pw, gw, mixbf, pbuf, hbuf, res, xhalf, rx1, tx2, rx2, q_ref, mix_ref, p_ref, act, norm_in, nrow, mask_ref,
                 ring_sem, p_sem, g_sem, load_sem, small_sem, s1_send, s1_recv, s2_send, s2_recv, s3_send, s3_recv, out_sem):
    rows, d_model = hbuf.shape
    half = rows // 2
    part = half // 2
    depth = ring.shape[1]
    inner = q_ref.shape[1]
    d_ff = act.shape[1]
    width = d_model // AR_CHUNKS
    MESH = pl.DeviceIdType.MESH

    me = lax.axis_index("tp")
    core = lax.rem(me, 2)
    chip = me // 2
    partner = {"tp": chip * 2 + (1 - core)}
    across = {"tp": (1 - chip) * 2 + core}

    def mine(at, n):
        return pl.ds(multiple_of(core * half + at, 16), n)

    def theirs(at, n):
        return pl.ds(multiple_of((1 - core) * half + at, 16), n)

    def piece(j):
        return pl.ds(j * width, width)

    per_step = GROUP * inner // depth
    n_step = rows // GROUP
    ahead = RING // (2 * per_step)
    n_sq = pw.shape[0] // 2
    g_rows, g_cols = gw.shape[1:]
    g_cut = d_model // g_rows
    n_pair = gw.shape[0] // (2 * g_cut)

    def copy_in(src, slot, used=None):
        dst = ring.at[slot] if used is None else ring.at[slot, used]
        pltpu.make_async_copy(src, dst, ring_sem.at[slot]).start()

    def landed(slot, used=depth):
        pltpu.make_async_copy(ck_hbm.at[pl.ds(0, used)], ring.at[slot, pl.ds(0, used)], ring_sem.at[slot]).wait()

    def group_of(step):
        per_half, u = n_step // 2, step % (n_step // 2)
        return (step // per_half) * (part // GROUP) + u + (u // (part // GROUP)) * (part // GROUP)

    def kv_slot(step, value):
        return (ahead * value + step % ahead) * per_step

    def issue_kv(step, value):
        src = cv_hbm if value else ck_hbm
        for i in range(per_step):
            at = multiple_of((group_of(step) * per_step + i) * depth, depth)
            copy_in(src.at[pl.ds(at, depth)], kv_slot(step, value) + i)

    def q_copy(k):
        return pltpu.make_async_copy(cq_hbm.at[pl.ds(k * WIDE, WIDE)], pw.at[k], p_sem.at[k])

    def o_copy(i):
        return pltpu.make_async_copy(co_hbm.at[:, pl.ds(i * WIDE, WIDE)], pw.at[n_sq + i], p_sem.at[n_sq + i])

    def gu_square(i):
        src = wg_hbm if i < n_sq else wu_hbm
        return pltpu.make_async_copy(src.at[pl.ds((i % n_sq) * WIDE, WIDE), pl.ds(0, WIDE)], pw.at[i], p_sem.at[i])

    def gu_tall(pair, i):
        src = wg_hbm if i < g_cut else wu_hbm
        slot = (pair % n_pair) * 2 * g_cut + i
        return pltpu.make_async_copy(src.at[pl.ds((i % g_cut) * g_rows, g_rows), pl.ds(WIDE + pair * g_cols, g_cols)],
                                     gw.at[slot], g_sem.at[slot])

    d_cut = -(-d_ff // WIDE)
    d_narrow = 2 * WIDE // LANES

    def d_square(c, i):
        slot = (c - 2) * d_cut + i
        n = min(WIDE, d_ff - i * WIDE)
        return pltpu.make_async_copy(wd_hbm.at[pl.ds(i * WIDE, n), pl.ds(c * WIDE, WIDE)],
                                     pw.at[slot, pl.ds(0, n)], p_sem.at[slot])

    def issue_d(i):
        copy_in(wd_hbm.at[:, pl.ds(i * LANES, LANES)], i, pl.ds(0, d_ff))

    def to_partner(a, h, j, at, n):
        return pltpu.make_async_remote_copy(
            src_ref=pbuf.at[theirs(at, n), piece(j)], dst_ref=rx1.at[a % 2, pl.ds(at, n), piece(j)],
            send_sem=s1_send.at[a % 2, h, j], recv_sem=s1_recv.at[a % 2, h, j], device_id=partner, device_id_type=MESH)

    def to_across(a, h, j, at, n):
        return pltpu.make_async_remote_copy(
            src_ref=tx2.at[a % 2, pl.ds(at, n), piece(j)], dst_ref=rx2.at[a % 2, pl.ds(at, n), piece(j)],
            send_sem=s2_send.at[a % 2, h, j], recv_sem=s2_recv.at[a % 2, h, j], device_id=across, device_id_type=MESH)

    def blocks(at, n, fn):
        def body(i, carry):
            fn(multiple_of(at + i * 16, 16))
            return carry
        lax.fori_loop(0, n // 16, body, 0)

    def chip_sum(a, h, j, at, n):
        to_partner(a, h, j, at, n).wait_recv()

        def add(r):
            own = pbuf[mine(r, 16), piece(j)].astype(F32)
            tx2[a % 2, pl.ds(r, 16), piece(j)] = (own + rx1[a % 2, pl.ds(r, 16), piece(j)].astype(F32)).astype(BF16)
        blocks(at, n, add)
        to_across(a, h, j, at, n).start()

    def full_sum(a, h, j, at, n):
        to_across(a, h, j, at, n).wait_recv()

        def add(r):
            both = tx2[a % 2, pl.ds(r, 16), piece(j)].astype(F32) + rx2[a % 2, pl.ds(r, 16), piece(j)].astype(F32)
            res[pl.ds(r, 16), piece(j)] = res[pl.ds(r, 16), piece(j)] + both
        blocks(at, n, add)

    def sent(a, h, at, n):
        for j in range(AR_CHUNKS):
            to_partner(a, h, j, at, n).wait_send()
            to_across(a, h, j, at, n).wait_send()

    def rows_back(a, h, i):
        at = mine(h * part + i * 16, 16)
        return pltpu.make_async_remote_copy(
            src_ref=hbuf.at[at], dst_ref=hbuf.at[at], send_sem=s3_send.at[a % 2, h, i],
            recv_sem=s3_recv.at[a % 2, h, i], device_id=partner, device_id_type=MESH)

    def normalise(a, h):
        norm = nrow[a:a + 1, :]
        for i in range(part // 16):
            r = res[h * part + i * 16:h * part + (i + 1) * 16, :]
            inv = lax.rsqrt(jnp.mean(r * r, axis=-1, keepdims=True) + 1e-6)
            hbuf[mine(h * part + i * 16, 16), :] = (r * inv * norm).astype(BF16)
            rows_back(a, h, i).start()

    def all_rows(a, h):
        for i in range(part // 16):
            rows_back(a, h, i).wait()

    pieces = range(AR_CHUNKS)
    halves = range(2)
    n_wo = d_model // g_cols
    mixed_copy = pltpu.make_async_copy(mixed_hbm, mixbf, load_sem.at[n_wo])
    mixed_copy.start()

    def wo_copy(i):
        per_slot = g_rows // inner
        return pltpu.make_async_copy(wo_hbm.at[:, pl.ds(i * g_cols, g_cols)],
                                     gw.at[i // per_slot, pl.ds(i % per_slot * inner, inner)], load_sem.at[i])
    for i in range(n_wo):
        wo_copy(i).start()
    small = [pltpu.make_async_copy(src, dst, small_sem.at[i]) for i, (src, dst) in enumerate(
        ((x_hbm.at[mine(0, half)], xhalf), (ncross_hbm, norm_in.at[0]), (nmlp_hbm, norm_in.at[1]), (mask_hbm, mask_ref)))]
    for copy in small:
        copy.start()
    barrier = pltpu.get_barrier_semaphore()
    for other in (partner, across):
        pl.semaphore_signal(barrier, inc=1, device_id=other, device_id_type=MESH)
    pl.semaphore_wait(barrier, 2)

    for k in range(n_sq):
        q_copy(k).start()
    for step in range(ahead):
        issue_kv(step, 0)
        issue_kv(step, 1)
    for i in range(n_sq):
        o_copy(i).start()
    mixed_copy.wait()
    for i in range(n_wo):
        wo_copy(i).wait()
        per_slot = g_rows // inner
        for n in range(g_cols // COLS):
            w = gw[i // per_slot, i % per_slot * inner:(i % per_slot + 1) * inner, n * COLS:(n + 1) * COLS]
            y = jnp.dot(mixbf[...], w, preferred_element_type=F32)
            pbuf[:, i * g_cols + n * COLS:i * g_cols + (n + 1) * COLS] = y.astype(BF16)
        if (i + 1) * g_cols % width == 0:
            j = (i + 1) * g_cols // width - 1
            to_partner(0, 0, j, 0, part).start()
            if j > 0:
                chip_sum(0, 0, j - 1, 0, part)
    for j in pieces:
        to_partner(0, 1, j, part, part).start()
    for i in range(2 * g_cut):
        gu_tall(0, i).start()
    chip_sum(0, 0, AR_CHUNKS - 1, 0, part)
    for j in pieces:
        chip_sum(0, 1, j, part, part)
    for copy in small:
        copy.wait()
    lay_row(nrow, 0, norm_in.at[0])
    lay_row(nrow, 1, norm_in.at[1])
    blocks(0, half, lambda r: res.__setitem__((pl.ds(r, 16), slice(None)), xhalf[pl.ds(r, 16), :].astype(F32)))

    def beside(a, b, used=depth):
        return jnp.concatenate([ring[a, 0:used, :], ring[b, 0:used, :]], axis=1)

    def both_cores(ref, h, at=slice(None)):
        return jnp.concatenate([ref[h * part:(h + 1) * part, at], ref[half + h * part:half + (h + 1) * part, at]], axis=0)

    def project_q(h):
        if h == 0:
            for k in range(n_sq):
                q_copy(k).wait()

        def block(n, carry):
            here = pl.ds(multiple_of(n * COLS, COLS), COLS)
            y = None
            for k in range(n_sq):
                z = jnp.dot(both_cores(hbuf, h, slice(k * WIDE, (k + 1) * WIDE)), pw[k, :, here], preferred_element_type=F32)
                y = z if y is None else y + z
            y = y.astype(BF16).astype(F32)
            q_ref[h * part:(h + 1) * part, here] = y[0:part]
            q_ref[half + h * part:half + (h + 1) * part, here] = y[part:]
            return carry
        twice(inner // COLS, block)

    own_head = (lax.broadcasted_iota(jnp.int32, (n_head, inner), 1) // (inner // n_head)
                == lax.broadcasted_iota(jnp.int32, (n_head, inner), 0))
    in_slot = GROUP // per_step

    def rows_of(slot, r):
        here = pl.ds(r * inner, inner)
        return jnp.concatenate([ring[slot, here, :], ring[slot + 1, here, :]], axis=1)

    def group_rows(step):
        return pl.ds(multiple_of(group_of(step) * GROUP, GROUP), GROUP)

    def score_dots(step):
        q8 = q_ref[group_rows(step), :]

        def spread(r):
            return jnp.where(own_head, jnp.broadcast_to(q8[r:r + 1, :], (n_head, inner)), 0.0).astype(BF16)
        return [jnp.dot(jnp.concatenate([spread(r), spread(r + in_slot)], axis=0), rows_of(kv_slot(step, 0), r),
                        preferred_element_type=F32) for r in range(in_slot)]

    def probabilities(step, dots):
        m8 = mask_ref[group_rows(step), :]
        scores = [s[0:n_head, 0:LANES] for s in dots] + [s[n_head:, LANES:] for s in dots]
        s = jnp.concatenate([jnp.where(m8[r:r + 1, :] != 0, scores[r], NEG_FILL) for r in range(GROUP)], axis=0)
        e = jnp.exp(s - jnp.max(s, axis=1, keepdims=True))
        p_ref[...] = (e / jnp.sum(e, axis=1, keepdims=True)).astype(BF16)

    def value_dots(step, p):
        none = jnp.zeros((n_head, LANES), BF16)
        out = []
        for r in range(in_slot):
            pa = p[r * n_head:(r + 1) * n_head, :]
            pb = p[(r + in_slot) * n_head:(r + in_slot + 1) * n_head, :]
            lhs = jnp.concatenate([jnp.concatenate([pa, none], axis=1), jnp.concatenate([none, pb], axis=1)], axis=0)
            out.append(lax.dot_general(lhs, rows_of(kv_slot(step, 1), r), (((1,), (1,)), ((), ())), preferred_element_type=F32))
        return out

    def store_mixed(step, dots):
        mixed = [y[0:n_head] for y in dots] + [y[n_head:] for y in dots]
        mix_ref[group_rows(step), :] = jnp.concatenate(
            [jnp.sum(jnp.where(own_head, y, 0.0), axis=0, keepdims=True) for y in mixed], axis=0)

    def wait_kv(step, value):
        for i in range(per_step):
            landed(kv_slot(step, value) + i)

    def refill(step, value):
        if isinstance(step, int):
            if step < n_step:
                issue_kv(step, value)
            return

        @pl.when(step < n_step)
        def _():
            issue_kv(step, value)

    def attend(lo, hi, at=None, hook=None):
        wait_kv(lo, 0)
        probabilities(lo, score_dots(lo))
        refill(lo + ahead, 0)

        def body(step, carry):
            wait_kv(step + 1, 0)
            wait_kv(step, 1)
            p = p_ref[...]
            dots = score_dots(step + 1)
            values = value_dots(step, p)
            probabilities(step + 1, dots)
            store_mixed(step, values)
            if hook is not None:
                pl.when(step == at)(hook)
            refill(step + 1 + ahead, 0)
            refill(step + ahead, 1)
            return carry
        lax.fori_loop(lo, hi - 1, body, 0)
        wait_kv(hi - 1, 1)
        store_mixed(hi - 1, value_dots(hi - 1, p_ref[...]))
        refill(hi - 1 + ahead, 1)

    def project_o(h, after):
        lhs = both_cores(mix_ref, h).astype(BF16)
        for j in pieces:
            if h == 0:
                o_copy(j).wait()
            for n in range(WIDE // COLS):
                y = jnp.dot(lhs, pw[n_sq + j, :, n * COLS:(n + 1) * COLS], preferred_element_type=F32).astype(BF16)
                here = slice(j * WIDE + n * COLS, j * WIDE + (n + 1) * COLS)
                pbuf[h * part:(h + 1) * part, here] = y[0:part]
                pbuf[half + h * part:half + (h + 1) * part, here] = y[part:]
            to_partner(1, h, j, h * part, part).start()
            if after and j > 0:
                chip_sum(1, h, j - 1, h * part, part)
        if after:
            chip_sum(1, h, AR_CHUNKS - 1, h * part, part)

    for j in pieces:
        full_sum(0, 0, j, 0, part)
    normalise(0, 0)
    all_rows(0, 0)
    project_q(0)

    def second_half():
        for j in pieces:
            full_sum(0, 1, j, part, part)
        normalise(0, 1)
    attend(0, n_step // 2, n_step // 2 - 3, second_half)
    sent(0, 0, 0, part)
    project_o(0, False)
    all_rows(0, 1)
    project_q(1)
    for j in pieces:
        chip_sum(1, 0, j, 0, part)
    attend(n_step // 2, n_step)
    for pair in range(1, n_pair):
        for i in range(2 * g_cut):
            gu_tall(pair, i).start()
    for i in range(n_sq):
        gu_square(i).start()
    sent(0, 1, part, part)
    project_o(1, True)
    for i in range(n_sq):
        gu_square(n_sq + i).start()
    for i in range(d_narrow):
        issue_d(i)
    for j in pieces:
        full_sum(1, 0, j, 0, part)
    normalise(1, 0)
    for j in pieces:
        full_sum(1, 1, j, part, part)
    normalise(1, 1)
    for h in halves:
        all_rows(1, h)
        sent(1, h, h * part, part)

    root = math.sqrt(2.0 / math.pi)
    def mlp_block(at, gate, up):
        u, v = None, None
        for k in range(len(gate)):
            n = d_model // len(gate)
            lhs = hbuf[:, k * n:(k + 1) * n]
            y = jnp.dot(lhs, gate[k], preferred_element_type=F32)
            z = jnp.dot(lhs, up[k], preferred_element_type=F32)
            u, v = (y, z) if u is None else (u + y, v + z)
        gelu = 0.5 * u * (1.0 + jnp.tanh(root * (u + 0.044715 * (u * u * u))))
        act[:, pl.ds(at, COLS)] = (gelu * v).astype(BF16)

    def mlp_tall(pair):
        for i in range(2 * g_cut):
            gu_tall(pair, i).wait()
        base = (pair % n_pair) * 2 * g_cut

        def block(n, carry):
            here = pl.ds(multiple_of(n * COLS, COLS), COLS)
            mlp_block(multiple_of(WIDE + pair * g_cols + n * COLS, COLS), [gw[base + i, :, here] for i in range(g_cut)],
                      [gw[base + g_cut + i, :, here] for i in range(g_cut)])
            return carry
        twice(g_cols // COLS, block)

    def mlp_square():
        for i in range(2 * n_sq):
            gu_square(i).wait()

        def block(n, carry):
            here = pl.ds(multiple_of(n * COLS, COLS), COLS)
            mlp_block(multiple_of(n * COLS, COLS), [pw[i, :, here] for i in range(n_sq)],
                      [pw[n_sq + i, :, here] for i in range(n_sq)])
            return carry
        twice(WIDE // COLS, block)

    n_tall = (d_ff - WIDE) // g_cols
    for pair in range(n_pair):
        mlp_tall(pair)
        if pair + n_pair < n_tall:
            for i in range(2 * g_cut):
                gu_tall(pair + n_pair, i).start()
    mlp_square()
    for c in (2, 3):
        for i in range(d_cut):
            d_square(c, i).start()
    for pair in range(n_pair, n_tall):
        mlp_tall(pair)

    n_last = 2 * AR_CHUNKS
    w_last = d_model // n_last
    per_piece = w_last // COLS

    def last_piece(j):
        return pl.ds(j * w_last, w_last)

    def last_to_partner(j):
        return pltpu.make_async_remote_copy(
            src_ref=pbuf.at[theirs(0, half), last_piece(j)], dst_ref=rx1.at[0, :, last_piece(j)],
            send_sem=s1_send.at[0, j // AR_CHUNKS, j % AR_CHUNKS], recv_sem=s1_recv.at[0, j // AR_CHUNKS, j % AR_CHUNKS],
            device_id=partner, device_id_type=MESH)

    def last_to_across(j):
        return pltpu.make_async_remote_copy(
            src_ref=tx2.at[0, :, last_piece(j)], dst_ref=rx2.at[0, :, last_piece(j)],
            send_sem=s2_send.at[0, j // AR_CHUNKS, j % AR_CHUNKS], recv_sem=s2_recv.at[0, j // AR_CHUNKS, j % AR_CHUNKS],
            device_id=across, device_id_type=MESH)

    def last_back(j):
        return pltpu.make_async_remote_copy(
            src_ref=hbuf.at[mine(0, half), last_piece(j)], dst_ref=out_hbm.at[mine(0, half), last_piece(j)],
            send_sem=s3_send.at[0, j // AR_CHUNKS, j % AR_CHUNKS], recv_sem=s3_recv.at[0, j // AR_CHUNKS, j % AR_CHUNKS],
            device_id=partner, device_id_type=MESH)

    def last_own(j):
        return pltpu.make_async_copy(hbuf.at[mine(0, half), last_piece(j)], out_hbm.at[mine(0, half), last_piece(j)], out_sem.at[j])

    def last_chip_sum(j):
        last_to_partner(j).wait_recv()

        def add(r):
            own = pbuf[mine(r, 16), last_piece(j)].astype(F32)
            tx2[0, pl.ds(r, 16), last_piece(j)] = (own + rx1[0, pl.ds(r, 16), last_piece(j)].astype(F32)).astype(BF16)
        blocks(0, half, add)
        last_to_across(j).start()

    for c in range(n_last):
        at = c * w_last
        block_c, in_block = at // WIDE, at % WIDE
        if block_c >= 2 and in_block == 0:
            for i in range(d_cut):
                d_square(block_c, i).wait()

        def down(i, carry):
            n = c * per_piece + i
            if block_c < 2:
                landed(2 * n, d_ff)
                landed(2 * n + 1, d_ff)
                y = jnp.dot(act[...], beside(2 * n, 2 * n + 1, d_ff), preferred_element_type=F32)
            else:
                y = None
                for k in range(d_cut):
                    row, rest = k * WIDE, min(WIDE, d_ff - k * WIDE)
                    w = pw[(block_c - 2) * d_cut + k, 0:rest, pl.ds(multiple_of(in_block + i * COLS, COLS), COLS)]
                    z = jnp.dot(act[:, row:row + rest], w, preferred_element_type=F32)
                    y = z if y is None else y + z
            pbuf[:, pl.ds(multiple_of(n * COLS, COLS), COLS)] = y.astype(BF16)
            return carry
        twice(per_piece, down)
        last_to_partner(c).start()
        if c > 1:
            last_chip_sum(c - 2)
    last_chip_sum(n_last - 2)
    last_chip_sum(n_last - 1)

    for j in range(n_last):
        last_to_across(j).wait_recv()

        def add(r):
            both = tx2[0, pl.ds(r, 16), last_piece(j)].astype(F32) + rx2[0, pl.ds(r, 16), last_piece(j)].astype(F32)
            hbuf[mine(r, 16), last_piece(j)] = (res[pl.ds(r, 16), last_piece(j)] + both).astype(BF16)
        blocks(0, half, add)
        last_back(j).start()
        last_own(j).start()
    for j in range(n_last):
        last_to_partner(j).wait_send()
        last_to_across(j).wait_send()
        last_back(j).wait()
        last_own(j).wait()


def rest_of_layer(x_in, mixed, w_o, norm_cross, norm_mlp, enc_mask, cross_k, cross_v, cross_q, cross_o, w_gate, w_up, w_down):
    rows, d_model = x_in.shape
    _, src_len, n_head, d_head = cross_k.shape
    inner = n_head * d_head
    d_ff = w_gate.shape[1]
    half = rows // 2
    flat = (rows * inner, src_len)
    k_flat = cross_k.transpose(0, 2, 3, 1).reshape(flat)
    v_flat = cross_v.transpose(0, 2, 3, 1).reshape(flat)
    square = (d_model // 128, 128)
    return pl.pallas_call(
        functools.partial(cross_kernel, n_head),
        out_shape=jax.ShapeDtypeStruct((rows, d_model), BF16),
        in_specs=[ANY] * 13,
        out_specs=ANY,
        scratch_shapes=[
            pltpu.VMEM((RING, d_model, LANES), BF16),
            pltpu.VMEM((8, WIDE, WIDE), BF16),
            pltpu.VMEM((8, d_model // 2, 512), BF16),
            pltpu.VMEM((rows, inner), BF16),
            pltpu.VMEM((rows, d_model), BF16),
            pltpu.VMEM((rows, d_model), BF16),
            pltpu.VMEM((half, d_model), F32),
            pltpu.VMEM((half, d_model), BF16),
            pltpu.VMEM((2, half, d_model), BF16),
            pltpu.VMEM((2, half, d_model), BF16),
            pltpu.VMEM((2, half, d_model), BF16),
            pltpu.VMEM((rows, inner), F32),
            pltpu.VMEM((rows, inner), F32),
            pltpu.VMEM((GROUP * n_head, src_len), BF16),
            pltpu.VMEM((rows, d_ff), BF16),
            pltpu.VMEM((2,) + square, BF16),
            pltpu.VMEM((2, d_model), F32),
            pltpu.VMEM((rows, src_len), jnp.int32),
            pltpu.SemaphoreType.DMA((RING,)),
            pltpu.SemaphoreType.DMA((8,)),
            pltpu.SemaphoreType.DMA((8,)),
            pltpu.SemaphoreType.DMA((d_model // 512 + 1,)),
            pltpu.SemaphoreType.DMA((4,)),
            pltpu.SemaphoreType.DMA((2, 2, AR_CHUNKS)),
            pltpu.SemaphoreType.DMA((2, 2, AR_CHUNKS)),
            pltpu.SemaphoreType.DMA((2, 2, AR_CHUNKS)),
            pltpu.SemaphoreType.DMA((2, 2, AR_CHUNKS)),
            pltpu.SemaphoreType.DMA((2, 2, AR_CHUNKS)),
            pltpu.SemaphoreType.DMA((2, 2, AR_CHUNKS)),
            pltpu.SemaphoreType.DMA((2 * AR_CHUNKS,)),
        ],
        compiler_params=pltpu.CompilerParams(vmem_limit_bytes=67_000_000, collective_id=0, has_side_effects=True),
        name="rest_part",
    )(x_in, mixed, w_o, norm_cross.reshape(square), norm_mlp.reshape(square), enc_mask, cross_q, k_flat, v_flat, cross_o, w_gate, w_up, w_down)


def solution(mesh):
    def local_layer(x_in, tok_pos, self_k, self_v, cross_k, cross_v, enc_mask, rel_bias, w_q, w_k, w_v, w_o, cross_q, cross_o, w_gate, w_up, w_down, norm_self, norm_cross, norm_mlp):
        mixed, new_self_k, new_self_v = self_attention(x_in, norm_self, tok_pos, rel_bias, w_q, w_k, w_v, self_k, self_v)
        x_out = rest_of_layer(x_in, mixed, w_o, norm_cross, norm_mlp, enc_mask, cross_k, cross_v, cross_q, cross_o, w_gate, w_up, w_down)
        return x_out, new_self_k, new_self_v

    cache_spec = P('dp', None, 'tp', None)
    split_cols = P(None, 'tp')
    split_rows = P('tp', None)
    in_specs = (P('dp', None), P('dp'), cache_spec, cache_spec, cache_spec, cache_spec, P('dp', None), split_cols, split_cols, split_cols, split_cols, split_rows, split_cols, split_rows, split_cols, split_cols, split_rows, P(None), P(None), P(None))
    out_specs = (P('dp', None), cache_spec, cache_spec)
    return jax.shard_map(local_layer, mesh=mesh, in_specs=in_specs, out_specs=out_specs, check_vma=False)
```

```python
import functools
import math
import jax
import jax.numpy as jnp
from jax import lax
from jax.experimental import pallas as pl
from jax.experimental.pallas import tpu as pltpu
from jax.sharding import PartitionSpec as P

BUCKET_EDGES = tuple(int(math.ceil(16.0 * 8.0 ** (bucket_step / 16.0))) for bucket_step in range(1, 16))
NEG_FILL = -1e30
F32 = jnp.float32
BF16 = jnp.bfloat16
ANY = pl.BlockSpec(memory_space=pl.ANY)
VMEM = pl.BlockSpec(memory_space=pltpu.VMEM)
COLS = 256
T_BLOCK = 8


def multiple_of(at, n):
    return at if isinstance(at, int) else pl.multiple_of(at, n)


def twice(n, body):
    def pair(i, carry):
        body(2 * i, carry)
        body(2 * i + 1, carry)
        return carry
    if n == 2:
        pair(0, 0)
    else:
        lax.fori_loop(0, n // 2, pair, 0)


def lay_row(dst, at, norm):
    values = norm[...].astype(F32)
    for i in range(values.shape[0]):
        dst[at:at + 1, i * 128:(i + 1) * 128] = values[i:i + 1, :]


def self_kernel(x_hbm, norm_hbm, pos_hbm, rel_hbm, wq_hbm, wk_hbm, wv_hbm, k_hbm, v_hbm,
                mixed_hbm, newk_hbm, newv_hbm,
                xbuf, hbuf, wbuf, kvbuf, sum_ref, q_ref, kn_ref, hit_ref, score_ref, acc_ref,
                norm_ref, nrow, pos_ref, rel_ref,
                x_sem, small_sem, w_sem, kv_sem, out_sem, part_sem, window):
    rows, d_model = xbuf.shape
    n_w = wbuf.shape[0]
    per_mat = n_w // 3
    n_chunk = kvbuf.shape[0] // 2
    n_head, t_len = score_ref.shape[0], score_ref.shape[1]
    inner = acc_ref.shape[0]
    d_head = inner // n_head
    chunk_rows = kvbuf.shape[1]
    sub = d_head // 16
    k_rows = wbuf.shape[1]

    def w_copy(c):
        src = (wq_hbm, wk_hbm, wv_hbm)[c // per_mat]
        return pltpu.make_async_copy(src.at[pl.ds((c % per_mat) * k_rows, k_rows)], wbuf.at[c], w_sem.at[c])

    def kv_copy(i):
        src = k_hbm if i < n_chunk else v_hbm
        return pltpu.make_async_copy(src.at[pl.ds((i % n_chunk) * chunk_rows, chunk_rows)], kvbuf.at[i], kv_sem.at[i])

    loads = [[w_copy(c)] for c in range(n_w)] + [[kv_copy(i)] for i in range(2 * n_chunk)]
    issued = [0]

    def issue(upto):
        while issued[0] < min(upto, len(loads)):
            for copy in loads[issued[0]]:
                copy.start()
            issued[0] += 1

    x_copy = pltpu.make_async_copy(x_hbm, xbuf, x_sem)
    x_copy.start()
    small = [pltpu.make_async_copy(src, dst, small_sem.at[i]) for i, (src, dst) in enumerate(
        ((pos_hbm, pos_ref), (rel_hbm, rel_ref), (norm_hbm, norm_ref)))]
    for copy in small:
        copy.start()
    issue(window)
    for copy in small:
        copy.wait()

    lay_row(nrow, 0, norm_ref)
    pos = pos_ref[...]
    pos16 = jnp.broadcast_to(pos, (16, rows))

    def set_hit(t, carry):
        hit_ref[t] = jnp.where(pos16 == t, 1.0, 0.0).astype(BF16)
        return carry
    lax.fori_loop(0, t_len, set_hit, 0)

    lane = lax.broadcasted_iota(jnp.int32, (n_head, 128), 1)
    bucket = jnp.full((n_head, 128), 16, jnp.int32)
    for edge in BUCKET_EDGES:
        bucket = bucket + (lane >= edge).astype(jnp.int32)
    bucket = jnp.where(lane < 16, lane, bucket)
    rel = rel_ref[...]
    table = jnp.zeros((n_head, 128), F32)
    for b in range(rel.shape[1]):
        table = jnp.where(bucket == b, rel[:, b:b + 1], table)
    acc_ref[0:n_head, :] = table

    x_copy.wait()
    block = 16
    norm = nrow[0:1, :]

    def norm_rows(i, carry):
        at = pl.ds(multiple_of(i * block, block), block)
        r = xbuf[at, :].astype(F32)
        inv = lax.rsqrt(jnp.mean(r * r, axis=-1, keepdims=True) + 1e-6)
        hbuf[at, :] = (r * inv * norm).astype(BF16)
        return carry
    lax.fori_loop(0, rows // block, norm_rows, 0)

    for c in range(n_w):
        w_copy(c).wait()
        issue(c + 1 + window)
        k = c % per_mat
        for n in range(inner // COLS):
            here = slice(n * COLS, (n + 1) * COLS)
            y = jnp.dot(hbuf[:, k * k_rows:(k + 1) * k_rows], wbuf[c, :, here], preferred_element_type=F32)
            if k > 0:
                y = y + sum_ref[:, here]
            if k < per_mat - 1:
                sum_ref[:, here] = y
                continue
            y = y.astype(BF16).astype(F32).T
            if c < per_mat:
                q_ref[here, :] = y
            else:
                kn_ref[c // per_mat - 1, here, :] = y.astype(BF16)

    def chunk_out(i):
        dst = newk_hbm if i < n_chunk else newv_hbm
        return pltpu.make_async_copy(kvbuf.at[i], dst.at[pl.ds((i % n_chunk) * chunk_rows, chunk_rows)], out_sem.at[i])

    for j in range(n_chunk):
        kv_copy(j).wait()
        issue(n_w + j + 1 + window)

        def k_head(h, carry):
            at = multiple_of(h * d_head, d_head)
            q = q_ref[pl.ds(at, d_head), :]
            kn = kn_ref[0, pl.ds(at, d_head), :].reshape(sub, 16, rows)
            rows_out = []
            for tt in range(T_BLOCK):
                here = pl.ds(multiple_of(tt * inner + at, d_head), d_head)
                old = kvbuf[j, here, :].reshape(sub, 16, rows)
                hit = hit_ref[j * T_BLOCK + tt] != 0
                new = jnp.where(hit[None], kn, old)
                kvbuf[j, here, :] = new.reshape(d_head, rows)
                prod = new.reshape(d_head, rows).astype(F32) * q
                rows_out.append(jnp.sum(prod, axis=0, keepdims=True))
            score_ref[h, j * T_BLOCK:(j + 1) * T_BLOCK, :] = jnp.concatenate(rows_out, axis=0)
            return carry
        twice(n_head, k_head)
        chunk_out(j).start(priority=1)

    t_iota = lax.broadcasted_iota(jnp.int32, (t_len, rows), 0)
    causal = t_iota <= pos
    back = jnp.maximum(pos - t_iota, 0)

    def soft_head(h, carry):
        line = jnp.broadcast_to(acc_ref[pl.ds(h, 1), :], (t_len, 128))
        s = score_ref[h] + jnp.take_along_axis(line, back, axis=1)
        s = jnp.where(causal, s, NEG_FILL)
        e = jnp.exp(s - jnp.max(s, axis=0, keepdims=True))
        p = e / jnp.sum(e, axis=0, keepdims=True)
        score_ref[h] = p.astype(BF16).astype(F32)
        return carry
    lax.fori_loop(0, n_head, soft_head, 0)

    acc_ref[...] = jnp.zeros_like(acc_ref)
    for j in range(n_chunk):
        kv_copy(n_chunk + j).wait()
        issue(n_w + n_chunk + j + 1 + window)

        def v_head(h, carry):
            at = multiple_of(h * d_head, d_head)
            vn = kn_ref[1, pl.ds(at, d_head), :].reshape(sub, 16, rows)
            p = score_ref[h, j * T_BLOCK:(j + 1) * T_BLOCK, :]
            acc = acc_ref[pl.ds(at, d_head), :]
            for tt in range(T_BLOCK):
                here = pl.ds(multiple_of(tt * inner + at, d_head), d_head)
                old = kvbuf[n_chunk + j, here, :].reshape(sub, 16, rows)
                hit = hit_ref[j * T_BLOCK + tt] != 0
                new = jnp.where(hit[None], vn, old)
                kvbuf[n_chunk + j, here, :] = new.reshape(d_head, rows)
                acc = acc + new.reshape(d_head, rows).astype(F32) * p[tt:tt + 1, :]
            acc_ref[pl.ds(at, d_head), :] = acc
            return carry
        twice(n_head, v_head)
        chunk_out(n_chunk + j).start(priority=1)

    issue(len(loads))
    hbuf[:, 0:inner] = acc_ref[...].T.astype(BF16)
    mixed_copy = pltpu.make_async_copy(hbuf.at[:, pl.ds(0, inner)], mixed_hbm, part_sem)
    mixed_copy.start()
    for i in range(2 * n_chunk):
        chunk_out(i).wait()
    mixed_copy.wait()


def self_attention(x_in, norm_self, tok_pos, rel_bias, w_q, w_k, w_v, self_k, self_v):
    rows, t_len, n_head, d_head = self_k.shape
    d_model = x_in.shape[1]
    inner = n_head * d_head
    flat = (t_len * inner, rows)
    k_flat = self_k.transpose(1, 2, 3, 0).reshape(flat)
    v_flat = self_v.transpose(1, 2, 3, 0).reshape(flat)
    n_w = 3 * (d_model // inner)
    n_chunk = t_len // T_BLOCK

    def body(*refs):
        self_kernel(*refs, window=5)

    mixed, new_k, new_v = pl.pallas_call(
        body,
        out_shape=(jax.ShapeDtypeStruct((rows, inner), BF16),
                   jax.ShapeDtypeStruct(flat, BF16), jax.ShapeDtypeStruct(flat, BF16)),
        in_specs=[ANY] * 9,
        out_specs=(ANY, ANY, ANY),
        scratch_shapes=[
            pltpu.VMEM((rows, d_model), BF16),
            pltpu.VMEM((rows, d_model), BF16),
            pltpu.VMEM((n_w, inner, inner), BF16),
            pltpu.VMEM((2 * n_chunk, T_BLOCK * inner, rows), BF16),
            pltpu.VMEM((rows, inner), F32),
            pltpu.VMEM((inner, rows), F32),
            pltpu.VMEM((2, inner, rows), BF16),
            pltpu.VMEM((t_len, 16, rows), BF16),
            pltpu.VMEM((n_head, t_len, rows), F32),
            pltpu.VMEM((inner, rows), F32),
            pltpu.VMEM((d_model // 128, 128), BF16),
            pltpu.VMEM((1, d_model), F32),
            pltpu.VMEM((1, rows), jnp.int32),
            pltpu.VMEM(rel_bias.shape[::-1], F32),
            pltpu.SemaphoreType.DMA,
            pltpu.SemaphoreType.DMA((3,)),
            pltpu.SemaphoreType.DMA((n_w,)),
            pltpu.SemaphoreType.DMA((2 * n_chunk,)),
            pltpu.SemaphoreType.DMA((2 * n_chunk,)),
            pltpu.SemaphoreType.DMA,
        ],
        compiler_params=pltpu.CompilerParams(vmem_limit_bytes=66_900_000),
        cost_estimate=pl.CostEstimate(flops=3_300_000_000, bytes_accessed=95_000_000, transcendentals=131_072),
        name="self_part",
    )(x_in, norm_self.reshape(d_model // 128, 128), tok_pos.reshape(1, rows), rel_bias.T, w_q, w_k, w_v, k_flat, v_flat)

    def unflat(cache):
        return cache.reshape(t_len, n_head, d_head, rows).transpose(3, 0, 1, 2)
    return mixed, unflat(new_k), unflat(new_v)


RING = 20
WIDE = 1024
GROUP = 8
AR_CHUNKS = 4
LANES = 128


def cross_kernel(n_head, x_hbm, mixed_hbm, wo_hbm, ncross_hbm, nmlp_hbm, mask_hbm, cq_hbm, ck_hbm, cv_hbm, co_hbm, wg_hbm, wu_hbm, wd_hbm,
                 out_hbm,
                 ring, pw, gw, mixbf, pbuf, hbuf, res, xhalf, rx1, tx2, rx2, q_ref, mix_ref, p_ref, act, norm_in, nrow, mask_ref,
                 ring_sem, p_sem, g_sem, load_sem, small_sem, s1_send, s1_recv, s2_send, s2_recv, s3_send, s3_recv, out_sem):
    rows, d_model = hbuf.shape
    half = rows // 2
    part = half // 2
    quarter = part // 2
    depth = ring.shape[1]
    inner = q_ref.shape[1]
    d_ff = act.shape[1]
    width = d_model // AR_CHUNKS
    MESH = pl.DeviceIdType.MESH

    me = lax.axis_index("tp")
    core = lax.rem(me, 2)
    chip = me // 2
    partner = {"tp": chip * 2 + (1 - core)}
    across = {"tp": (1 - chip) * 2 + core}

    def mine(at, n):
        return pl.ds(multiple_of(core * half + at, 16), n)

    def theirs(at, n):
        return pl.ds(multiple_of((1 - core) * half + at, 16), n)

    def piece(j):
        return pl.ds(j * width, width)

    per_step = GROUP * inner // depth
    n_step = rows // GROUP
    ahead = RING // (2 * per_step)
    n_sq = pw.shape[0] // 2
    g_rows, g_cols = gw.shape[1:]
    g_cut = d_model // g_rows
    n_pair = gw.shape[0] // (2 * g_cut)

    def copy_in(src, slot, used=None):
        dst = ring.at[slot] if used is None else ring.at[slot, used]
        pltpu.make_async_copy(src, dst, ring_sem.at[slot]).start()

    def landed(slot, used=depth):
        pltpu.make_async_copy(ck_hbm.at[pl.ds(0, used)], ring.at[slot, pl.ds(0, used)], ring_sem.at[slot]).wait()

    def group_of(step):
        per_quarter = quarter // GROUP
        w = step % (2 * per_quarter)
        return step // (2 * per_quarter) * per_quarter + w // per_quarter * (half // GROUP) + w % per_quarter

    def kv_slot(step, value):
        return (ahead * value + step % ahead) * per_step

    def issue_kv(step, value):
        src = cv_hbm if value else ck_hbm
        for i in range(per_step):
            at = multiple_of((group_of(step) * per_step + i) * depth, depth)
            copy_in(src.at[pl.ds(at, depth)], kv_slot(step, value) + i)

    def q_copy(k):
        return pltpu.make_async_copy(cq_hbm.at[pl.ds(k * WIDE, WIDE)], pw.at[k], p_sem.at[k])

    def o_copy(i):
        return pltpu.make_async_copy(co_hbm.at[:, pl.ds(i * WIDE, WIDE)], pw.at[n_sq + i], p_sem.at[n_sq + i])

    def gu_square(i):
        src = wg_hbm if i < n_sq else wu_hbm
        return pltpu.make_async_copy(src.at[pl.ds((i % n_sq) * WIDE, WIDE), pl.ds(0, WIDE)], pw.at[i], p_sem.at[i])

    def gu_tall(pair, i):
        src = wg_hbm if i < g_cut else wu_hbm
        slot = (pair % n_pair) * 2 * g_cut + i
        return pltpu.make_async_copy(src.at[pl.ds((i % g_cut) * g_rows, g_rows), pl.ds(WIDE + pair * g_cols, g_cols)],
                                     gw.at[slot], g_sem.at[slot])

    d_cut = -(-d_ff // WIDE)
    d_narrow = 2 * WIDE // LANES

    def d_square(c, i):
        slot = (c - 2) * d_cut + i
        n = min(WIDE, d_ff - i * WIDE)
        return pltpu.make_async_copy(wd_hbm.at[pl.ds(i * WIDE, n), pl.ds(c * WIDE, WIDE)],
                                     pw.at[slot, pl.ds(0, n)], p_sem.at[slot])

    def issue_d(i):
        copy_in(wd_hbm.at[:, pl.ds(i * LANES, LANES)], i, pl.ds(0, d_ff))

    def to_partner(a, h, j, at, n):
        return pltpu.make_async_remote_copy(
            src_ref=pbuf.at[theirs(at, n), piece(j)], dst_ref=rx1.at[a % 2, pl.ds(at, n), piece(j)],
            send_sem=s1_send.at[a % 2, h, j], recv_sem=s1_recv.at[a % 2, h, j], device_id=partner, device_id_type=MESH)

    def to_across(a, h, j, at, n):
        return pltpu.make_async_remote_copy(
            src_ref=tx2.at[a % 2, pl.ds(at, n), piece(j)], dst_ref=rx2.at[a % 2, pl.ds(at, n), piece(j)],
            send_sem=s2_send.at[a % 2, h, j], recv_sem=s2_recv.at[a % 2, h, j], device_id=across, device_id_type=MESH)

    def blocks(at, n, fn):
        def body(i, carry):
            fn(multiple_of(at + i * 16, 16))
            return carry
        lax.fori_loop(0, n // 16, body, 0)

    def chip_sum(a, h, j, at, n):
        to_partner(a, h, j, at, n).wait_recv()

        def add(r):
            own = pbuf[mine(r, 16), piece(j)].astype(F32)
            tx2[a % 2, pl.ds(r, 16), piece(j)] = (own + rx1[a % 2, pl.ds(r, 16), piece(j)].astype(F32)).astype(BF16)
        blocks(at, n, add)
        to_across(a, h, j, at, n).start()

    def full_sum(a, h, j, at, n):
        to_across(a, h, j, at, n).wait_recv()

        def add(r):
            both = tx2[a % 2, pl.ds(r, 16), piece(j)].astype(F32) + rx2[a % 2, pl.ds(r, 16), piece(j)].astype(F32)
            res[pl.ds(r, 16), piece(j)] = res[pl.ds(r, 16), piece(j)] + both
        blocks(at, n, add)

    def sent(a, h, at, n):
        for j in range(AR_CHUNKS):
            to_partner(a, h, j, at, n).wait_send()
            to_across(a, h, j, at, n).wait_send()

    def rows_back(a, h, i, at):
        at = mine(at + i * 16, 16)
        return pltpu.make_async_remote_copy(
            src_ref=hbuf.at[at], dst_ref=hbuf.at[at], send_sem=s3_send.at[a % 2, h, i],
            recv_sem=s3_recv.at[a % 2, h, i], device_id=partner, device_id_type=MESH)

    def normalise(a, h, at, n):
        norm = nrow[a:a + 1, :]
        for i in range(n // 16):
            r = res[at + i * 16:at + (i + 1) * 16, :]
            inv = lax.rsqrt(jnp.mean(r * r, axis=-1, keepdims=True) + 1e-6)
            hbuf[mine(at + i * 16, 16), :] = (r * inv * norm).astype(BF16)
            rows_back(a, h, i, at).start()

    def all_rows(a, h, at, n):
        for i in range(n // 16):
            rows_back(a, h, i, at).wait()

    pieces = range(AR_CHUNKS)
    halves = range(2)
    n_wo = d_model // g_cols
    mixed_copy = pltpu.make_async_copy(mixed_hbm, mixbf, load_sem.at[n_wo])
    mixed_copy.start()

    def wo_copy(i):
        per_slot = g_rows // inner
        return pltpu.make_async_copy(wo_hbm.at[:, pl.ds(i * g_cols, g_cols)],
                                     gw.at[i // per_slot, pl.ds(i % per_slot * inner, inner)], load_sem.at[i])
    for i in range(n_wo):
        wo_copy(i).start()
    small = [pltpu.make_async_copy(src, dst, small_sem.at[i]) for i, (src, dst) in enumerate(
        ((x_hbm.at[mine(0, half)], xhalf), (ncross_hbm, norm_in.at[0]), (nmlp_hbm, norm_in.at[1]), (mask_hbm, mask_ref)))]
    for copy in small:
        copy.start()
    barrier = pltpu.get_barrier_semaphore()
    for other in (partner, across):
        pl.semaphore_signal(barrier, inc=1, device_id=other, device_id_type=MESH)
    pl.semaphore_wait(barrier, 2)

    for k in range(n_sq):
        q_copy(k).start()
    for step in range(ahead):
        issue_kv(step, 0)
        issue_kv(step, 1)
    for i in range(n_sq):
        o_copy(i).start()
    mixed_copy.wait()
    for i in range(n_wo):
        wo_copy(i).wait()
        per_slot = g_rows // inner
        for n in range(g_cols // COLS):
            w = gw[i // per_slot, i % per_slot * inner:(i % per_slot + 1) * inner, n * COLS:(n + 1) * COLS]
            y = jnp.dot(mixbf[...], w, preferred_element_type=F32)
            pbuf[:, i * g_cols + n * COLS:i * g_cols + (n + 1) * COLS] = y.astype(BF16)
        if (i + 1) * g_cols % width == 0:
            j = (i + 1) * g_cols // width - 1
            to_partner(0, 0, j, 0, part).start()
            if j > 0:
                chip_sum(0, 0, j - 1, 0, part)
    for j in pieces:
        to_partner(0, 1, j, part, part).start()
    for i in range(2 * g_cut):
        gu_tall(0, i).start()
    chip_sum(0, 0, AR_CHUNKS - 1, 0, part)
    for j in pieces:
        chip_sum(0, 1, j, part, part)
    for copy in small:
        copy.wait()
    lay_row(nrow, 0, norm_in.at[0])
    lay_row(nrow, 1, norm_in.at[1])
    blocks(0, half, lambda r: res.__setitem__((pl.ds(r, 16), slice(None)), xhalf[pl.ds(r, 16), :].astype(F32)))

    def beside(a, b, used=depth):
        return jnp.concatenate([ring[a, 0:used, :], ring[b, 0:used, :]], axis=1)

    def both_cores(ref, at, n, here=slice(None)):
        return jnp.concatenate([ref[at:at + n, here], ref[half + at:half + at + n, here]], axis=0)

    def project_q(h):
        if h == 0:
            for k in range(n_sq):
                q_copy(k).wait()

        def block(n, carry):
            here = pl.ds(multiple_of(n * COLS, COLS), COLS)
            y = None
            for k in range(n_sq):
                z = jnp.dot(both_cores(hbuf, h * part, part, slice(k * WIDE, (k + 1) * WIDE)), pw[k, :, here], preferred_element_type=F32)
                y = z if y is None else y + z
            y = y.astype(BF16).astype(F32)
            q_ref[h * part:(h + 1) * part, here] = y[0:part]
            q_ref[half + h * part:half + (h + 1) * part, here] = y[part:]
            return carry
        twice(inner // COLS, block)

    own_head = (lax.broadcasted_iota(jnp.int32, (n_head, inner), 1) // (inner // n_head)
                == lax.broadcasted_iota(jnp.int32, (n_head, inner), 0))
    in_slot = GROUP // per_step

    def rows_of(slot, r):
        here = pl.ds(r * inner, inner)
        return jnp.concatenate([ring[slot, here, :], ring[slot + 1, here, :]], axis=1)

    def group_rows(step):
        return pl.ds(multiple_of(group_of(step) * GROUP, GROUP), GROUP)

    def score_dots(step):
        q8 = q_ref[group_rows(step), :]

        def spread(r):
            return jnp.where(own_head, jnp.broadcast_to(q8[r:r + 1, :], (n_head, inner)), 0.0).astype(BF16)
        return [jnp.dot(jnp.concatenate([spread(r), spread(r + in_slot)], axis=0), rows_of(kv_slot(step, 0), r),
                        preferred_element_type=F32) for r in range(in_slot)]

    def probabilities(step, dots):
        m8 = mask_ref[group_rows(step), :]
        scores = [s[0:n_head, 0:LANES] for s in dots] + [s[n_head:, LANES:] for s in dots]
        s = jnp.concatenate([jnp.where(m8[r:r + 1, :] != 0, scores[r], NEG_FILL) for r in range(GROUP)], axis=0)
        e = jnp.exp(s - jnp.max(s, axis=1, keepdims=True))
        p_ref[...] = (e / jnp.sum(e, axis=1, keepdims=True)).astype(BF16)

    def value_dots(step, p):
        none = jnp.zeros((n_head, LANES), BF16)
        out = []
        for r in range(in_slot):
            pa = p[r * n_head:(r + 1) * n_head, :]
            pb = p[(r + in_slot) * n_head:(r + in_slot + 1) * n_head, :]
            lhs = jnp.concatenate([jnp.concatenate([pa, none], axis=1), jnp.concatenate([none, pb], axis=1)], axis=0)
            out.append(lax.dot_general(lhs, rows_of(kv_slot(step, 1), r), (((1,), (1,)), ((), ())), preferred_element_type=F32))
        return out

    def store_mixed(step, dots):
        mixed = [y[0:n_head] for y in dots] + [y[n_head:] for y in dots]
        mix_ref[group_rows(step), :] = jnp.concatenate(
            [jnp.sum(jnp.where(own_head, y, 0.0), axis=0, keepdims=True) for y in mixed], axis=0)

    def wait_kv(step, value):
        for i in range(per_step):
            landed(kv_slot(step, value) + i)

    def refill(step, value):
        if isinstance(step, int):
            if step < n_step:
                issue_kv(step, value)
            return

        @pl.when(step < n_step)
        def _():
            issue_kv(step, value)

    def attend(lo, hi, hooks):
        wait_kv(lo, 0)
        probabilities(lo, score_dots(lo))
        refill(lo + ahead, 0)

        def body(step, carry):
            wait_kv(step + 1, 0)
            wait_kv(step, 1)
            p = p_ref[...]
            dots = score_dots(step + 1)
            values = value_dots(step, p)
            probabilities(step + 1, dots)
            store_mixed(step, values)
            for at, hook in hooks.items():
                pl.when(step == at)(hook)
            refill(step + 1 + ahead, 0)
            refill(step + ahead, 1)
            return carry
        lax.fori_loop(lo, hi - 1, body, 0)
        wait_kv(hi - 1, 1)
        store_mixed(hi - 1, value_dots(hi - 1, p_ref[...]))
        refill(hi - 1 + ahead, 1)

    def project_o(h, at, n, after):
        lhs = both_cores(mix_ref, at, n).astype(BF16)
        for j in pieces:
            if h == 0:
                o_copy(j).wait()
            for i in range(WIDE // COLS):
                y = jnp.dot(lhs, pw[n_sq + j, :, i * COLS:(i + 1) * COLS], preferred_element_type=F32).astype(BF16)
                here = slice(j * WIDE + i * COLS, j * WIDE + (i + 1) * COLS)
                pbuf[at:at + n, here] = y[0:n]
                pbuf[half + at:half + at + n, here] = y[n:]
            to_partner(1, h, j, at, n).start()
            if after and j > 0:
                chip_sum(1, h, j - 1, at, n)
        if after:
            chip_sum(1, h, AR_CHUNKS - 1, at, n)

    def finish(a, h, at, n):
        for j in pieces:
            full_sum(a, h, j, at, n)
        normalise(a, h, at, n)

    finish(0, 0, 0, part)
    all_rows(0, 0, 0, part)
    project_q(0)
    attend(0, n_step // 2, {n_step // 2 - 3: lambda: finish(0, 1, part, part)})
    sent(0, 0, 0, part)
    project_o(0, 0, part, False)
    all_rows(0, 1, part, part)
    project_q(1)
    for j in pieces:
        chip_sum(1, 0, j, 0, part)

    def third_quarter():
        sent(0, 1, part, part)
        project_o(1, part, quarter, False)

    def third_quarter_sum():
        for j in pieces:
            chip_sum(1, 1, j, part, quarter)
    attend(n_step // 2, n_step, {3 * n_step // 4 - 1: third_quarter, 3 * n_step // 4: third_quarter_sum})
    for pair in range(1, n_pair):
        for i in range(2 * g_cut):
            gu_tall(pair, i).start()
    for i in range(n_sq):
        gu_square(i).start()
    project_o(2, part + quarter, quarter, True)
    for i in range(n_sq):
        gu_square(n_sq + i).start()
    for i in range(d_narrow):
        issue_d(i)
    shares = ((0, 0, part), (1, part, quarter), (2, part + quarter, quarter))
    for share in shares:
        finish(1, *share)
    for share in shares:
        all_rows(1, *share)
        sent(1, *share)

    root = math.sqrt(2.0 / math.pi)
    def mlp_block(at, gate, up):
        u, v = None, None
        for k in range(len(gate)):
            n = d_model // len(gate)
            lhs = hbuf[:, k * n:(k + 1) * n]
            y = jnp.dot(lhs, gate[k], preferred_element_type=F32)
            z = jnp.dot(lhs, up[k], preferred_element_type=F32)
            u, v = (y, z) if u is None else (u + y, v + z)
        gelu = 0.5 * u * (1.0 + jnp.tanh(root * (u + 0.044715 * (u * u * u))))
        act[:, pl.ds(at, COLS)] = (gelu * v).astype(BF16)

    def mlp_tall(pair):
        for i in range(2 * g_cut):
            gu_tall(pair, i).wait()
        base = (pair % n_pair) * 2 * g_cut

        def block(n, carry):
            here = pl.ds(multiple_of(n * COLS, COLS), COLS)
            mlp_block(multiple_of(WIDE + pair * g_cols + n * COLS, COLS), [gw[base + i, :, here] for i in range(g_cut)],
                      [gw[base + g_cut + i, :, here] for i in range(g_cut)])
            return carry
        twice(g_cols // COLS, block)

    def mlp_square():
        for i in range(2 * n_sq):
            gu_square(i).wait()

        def block(n, carry):
            here = pl.ds(multiple_of(n * COLS, COLS), COLS)
            mlp_block(multiple_of(n * COLS, COLS), [pw[i, :, here] for i in range(n_sq)],
                      [pw[n_sq + i, :, here] for i in range(n_sq)])
            return carry
        twice(WIDE // COLS, block)

    n_tall = (d_ff - WIDE) // g_cols
    for pair in range(n_pair):
        mlp_tall(pair)
        if pair + n_pair < n_tall:
            for i in range(2 * g_cut):
                gu_tall(pair + n_pair, i).start()
    mlp_square()
    for c in (2, 3):
        for i in range(d_cut):
            d_square(c, i).start()
    for pair in range(n_pair, n_tall):
        mlp_tall(pair)

    n_last = 2 * AR_CHUNKS
    w_last = d_model // n_last
    per_piece = w_last // COLS

    def last_piece(j):
        return pl.ds(j * w_last, w_last)

    def last_to_partner(j):
        return pltpu.make_async_remote_copy(
            src_ref=pbuf.at[theirs(0, half), last_piece(j)], dst_ref=rx1.at[0, :, last_piece(j)],
            send_sem=s1_send.at[0, j // AR_CHUNKS, j % AR_CHUNKS], recv_sem=s1_recv.at[0, j // AR_CHUNKS, j % AR_CHUNKS],
            device_id=partner, device_id_type=MESH)

    def last_to_across(j):
        return pltpu.make_async_remote_copy(
            src_ref=tx2.at[0, :, last_piece(j)], dst_ref=rx2.at[0, :, last_piece(j)],
            send_sem=s2_send.at[0, j // AR_CHUNKS, j % AR_CHUNKS], recv_sem=s2_recv.at[0, j // AR_CHUNKS, j % AR_CHUNKS],
            device_id=across, device_id_type=MESH)

    def last_back(j):
        return pltpu.make_async_remote_copy(
            src_ref=hbuf.at[mine(0, half), last_piece(j)], dst_ref=out_hbm.at[mine(0, half), last_piece(j)],
            send_sem=s3_send.at[0, j // AR_CHUNKS, j % AR_CHUNKS], recv_sem=s3_recv.at[0, j // AR_CHUNKS, j % AR_CHUNKS],
            device_id=partner, device_id_type=MESH)

    def last_own(j):
        return pltpu.make_async_copy(hbuf.at[mine(0, half), last_piece(j)], out_hbm.at[mine(0, half), last_piece(j)], out_sem.at[j])

    def last_chip_sum(j):
        last_to_partner(j).wait_recv()

        def add(r):
            own = pbuf[mine(r, 16), last_piece(j)].astype(F32)
            tx2[0, pl.ds(r, 16), last_piece(j)] = (own + rx1[0, pl.ds(r, 16), last_piece(j)].astype(F32)).astype(BF16)
        blocks(0, half, add)
        last_to_across(j).start()

    for c in range(n_last):
        at = c * w_last
        block_c, in_block = at // WIDE, at % WIDE
        if block_c >= 2 and in_block == 0:
            for i in range(d_cut):
                d_square(block_c, i).wait()

        def down(i, carry):
            n = c * per_piece + i
            if block_c < 2:
                landed(2 * n, d_ff)
                landed(2 * n + 1, d_ff)
                y = jnp.dot(act[...], beside(2 * n, 2 * n + 1, d_ff), preferred_element_type=F32)
            else:
                y = None
                for k in range(d_cut):
                    row, rest = k * WIDE, min(WIDE, d_ff - k * WIDE)
                    w = pw[(block_c - 2) * d_cut + k, 0:rest, pl.ds(multiple_of(in_block + i * COLS, COLS), COLS)]
                    z = jnp.dot(act[:, row:row + rest], w, preferred_element_type=F32)
                    y = z if y is None else y + z
            pbuf[:, pl.ds(multiple_of(n * COLS, COLS), COLS)] = y.astype(BF16)
            return carry
        twice(per_piece, down)
        last_to_partner(c).start()
        if c > 1:
            last_chip_sum(c - 2)
    last_chip_sum(n_last - 2)
    last_chip_sum(n_last - 1)

    for j in range(n_last):
        last_to_across(j).wait_recv()

        def add(r):
            both = tx2[0, pl.ds(r, 16), last_piece(j)].astype(F32) + rx2[0, pl.ds(r, 16), last_piece(j)].astype(F32)
            hbuf[mine(r, 16), last_piece(j)] = (res[pl.ds(r, 16), last_piece(j)] + both).astype(BF16)
        blocks(0, half, add)
        last_back(j).start()
        last_own(j).start()
    for j in range(n_last):
        last_to_partner(j).wait_send()
        last_to_across(j).wait_send()
        last_back(j).wait()
        last_own(j).wait()


def rest_of_layer(x_in, mixed, w_o, norm_cross, norm_mlp, enc_mask, cross_k, cross_v, cross_q, cross_o, w_gate, w_up, w_down):
    rows, d_model = x_in.shape
    _, src_len, n_head, d_head = cross_k.shape
    inner = n_head * d_head
    d_ff = w_gate.shape[1]
    half = rows // 2
    flat = (rows * inner, src_len)
    k_flat = cross_k.transpose(0, 2, 3, 1).reshape(flat)
    v_flat = cross_v.transpose(0, 2, 3, 1).reshape(flat)
    square = (d_model // 128, 128)
    return pl.pallas_call(
        functools.partial(cross_kernel, n_head),
        out_shape=jax.ShapeDtypeStruct((rows, d_model), BF16),
        in_specs=[ANY] * 13,
        out_specs=ANY,
        scratch_shapes=[
            pltpu.VMEM((RING, d_model, LANES), BF16),
            pltpu.VMEM((8, WIDE, WIDE), BF16),
            pltpu.VMEM((8, d_model // 2, 512), BF16),
            pltpu.VMEM((rows, inner), BF16),
            pltpu.VMEM((rows, d_model), BF16),
            pltpu.VMEM((rows, d_model), BF16),
            pltpu.VMEM((half, d_model), F32),
            pltpu.VMEM((half, d_model), BF16),
            pltpu.VMEM((2, half, d_model), BF16),
            pltpu.VMEM((2, half, d_model), BF16),
            pltpu.VMEM((2, half, d_model), BF16),
            pltpu.VMEM((rows, inner), F32),
            pltpu.VMEM((rows, inner), F32),
            pltpu.VMEM((GROUP * n_head, src_len), BF16),
            pltpu.VMEM((rows, d_ff), BF16),
            pltpu.VMEM((2,) + square, BF16),
            pltpu.VMEM((2, d_model), F32),
            pltpu.VMEM((rows, src_len), jnp.int32),
            pltpu.SemaphoreType.DMA((RING,)),
            pltpu.SemaphoreType.DMA((8,)),
            pltpu.SemaphoreType.DMA((8,)),
            pltpu.SemaphoreType.DMA((d_model // 512 + 1,)),
            pltpu.SemaphoreType.DMA((4,)),
            pltpu.SemaphoreType.DMA((2, 3, AR_CHUNKS)),
            pltpu.SemaphoreType.DMA((2, 3, AR_CHUNKS)),
            pltpu.SemaphoreType.DMA((2, 3, AR_CHUNKS)),
            pltpu.SemaphoreType.DMA((2, 3, AR_CHUNKS)),
            pltpu.SemaphoreType.DMA((2, 3, AR_CHUNKS)),
            pltpu.SemaphoreType.DMA((2, 3, AR_CHUNKS)),
            pltpu.SemaphoreType.DMA((2 * AR_CHUNKS,)),
        ],
        compiler_params=pltpu.CompilerParams(vmem_limit_bytes=67_000_000, collective_id=0, has_side_effects=True),
        name="rest_part",
    )(x_in, mixed, w_o, norm_cross.reshape(square), norm_mlp.reshape(square), enc_mask, cross_q, k_flat, v_flat, cross_o, w_gate, w_up, w_down)


def solution(mesh):
    def local_layer(x_in, tok_pos, self_k, self_v, cross_k, cross_v, enc_mask, rel_bias, w_q, w_k, w_v, w_o, cross_q, cross_o, w_gate, w_up, w_down, norm_self, norm_cross, norm_mlp):
        mixed, new_self_k, new_self_v = self_attention(x_in, norm_self, tok_pos, rel_bias, w_q, w_k, w_v, self_k, self_v)
        x_out = rest_of_layer(x_in, mixed, w_o, norm_cross, norm_mlp, enc_mask, cross_k, cross_v, cross_q, cross_o, w_gate, w_up, w_down)
        return x_out, new_self_k, new_self_v

    cache_spec = P('dp', None, 'tp', None)
    split_cols = P(None, 'tp')
    split_rows = P('tp', None)
    in_specs = (P('dp', None), P('dp'), cache_spec, cache_spec, cache_spec, cache_spec, P('dp', None), split_cols, split_cols, split_cols, split_cols, split_rows, split_cols, split_rows, split_cols, split_cols, split_rows, P(None), P(None), P(None))
    out_specs = (P('dp', None), cache_spec, cache_spec)
    return jax.shard_map(local_layer, mesh=mesh, in_specs=in_specs, out_specs=out_specs, check_vma=False)
```

```python
import functools
import math
import jax
import jax.numpy as jnp
from jax import lax
from jax.experimental import pallas as pl
from jax.experimental.pallas import tpu as pltpu
from jax.sharding import PartitionSpec as P

BUCKET_EDGES = tuple(int(math.ceil(16.0 * 8.0 ** (bucket_step / 16.0))) for bucket_step in range(1, 16))
NEG_FILL = -1e30
F32 = jnp.float32
BF16 = jnp.bfloat16
ANY = pl.BlockSpec(memory_space=pl.ANY)
VMEM = pl.BlockSpec(memory_space=pltpu.VMEM)
COLS = 256
T_BLOCK = 8


def multiple_of(at, n):
    return at if isinstance(at, int) else pl.multiple_of(at, n)


def twice(n, body):
    def pair(i, carry):
        body(2 * i, carry)
        body(2 * i + 1, carry)
        return carry
    if n == 2:
        pair(0, 0)
    else:
        lax.fori_loop(0, n // 2, pair, 0)


def lay_row(dst, at, norm):
    values = norm[...].astype(F32)
    for i in range(values.shape[0]):
        dst[at:at + 1, i * 128:(i + 1) * 128] = values[i:i + 1, :]


def self_kernel(x_hbm, norm_hbm, pos_hbm, rel_hbm, wq_hbm, wk_hbm, wv_hbm, k_hbm, v_hbm,
                mixed_hbm, newk_hbm, newv_hbm,
                xbuf, hbuf, wbuf, kvbuf, sum_ref, q_ref, kn_ref, hit_ref, score_ref, acc_ref,
                norm_ref, nrow, pos_ref, rel_ref,
                x_sem, small_sem, w_sem, kv_sem, out_sem, part_sem, window):
    rows, d_model = xbuf.shape
    n_w = wbuf.shape[0]
    per_mat = n_w // 3
    n_chunk = kvbuf.shape[0] // 2
    n_head, t_len = score_ref.shape[0], score_ref.shape[1]
    inner = acc_ref.shape[0]
    d_head = inner // n_head
    chunk_rows = kvbuf.shape[1]
    sub = d_head // 16
    k_rows = wbuf.shape[1]

    def w_copy(c):
        src = (wq_hbm, wk_hbm, wv_hbm)[c // per_mat]
        return pltpu.make_async_copy(src.at[pl.ds((c % per_mat) * k_rows, k_rows)], wbuf.at[c], w_sem.at[c])

    def kv_copy(i):
        src = k_hbm if i < n_chunk else v_hbm
        return pltpu.make_async_copy(src.at[pl.ds((i % n_chunk) * chunk_rows, chunk_rows)], kvbuf.at[i], kv_sem.at[i])

    loads = [[w_copy(c)] for c in range(n_w)] + [[kv_copy(i)] for i in range(2 * n_chunk)]
    issued = [0]

    def issue(upto):
        while issued[0] < min(upto, len(loads)):
            for copy in loads[issued[0]]:
                copy.start()
            issued[0] += 1

    x_copy = pltpu.make_async_copy(x_hbm, xbuf, x_sem)
    x_copy.start()
    small = [pltpu.make_async_copy(src, dst, small_sem.at[i]) for i, (src, dst) in enumerate(
        ((pos_hbm, pos_ref), (rel_hbm, rel_ref), (norm_hbm, norm_ref)))]
    for copy in small:
        copy.start()
    issue(window)
    for copy in small:
        copy.wait()

    lay_row(nrow, 0, norm_ref)
    pos = pos_ref[...]
    pos16 = jnp.broadcast_to(pos, (16, rows))

    def set_hit(t, carry):
        hit_ref[t] = jnp.where(pos16 == t, 1.0, 0.0).astype(BF16)
        return carry
    lax.fori_loop(0, t_len, set_hit, 0)

    lane = lax.broadcasted_iota(jnp.int32, (n_head, 128), 1)
    bucket = jnp.full((n_head, 128), 16, jnp.int32)
    for edge in BUCKET_EDGES:
        bucket = bucket + (lane >= edge).astype(jnp.int32)
    bucket = jnp.where(lane < 16, lane, bucket)
    rel = rel_ref[...]
    table = jnp.zeros((n_head, 128), F32)
    for b in range(rel.shape[1]):
        table = jnp.where(bucket == b, rel[:, b:b + 1], table)
    acc_ref[0:n_head, :] = table

    x_copy.wait()
    block = 16
    norm = nrow[0:1, :]

    def norm_rows(i, carry):
        at = pl.ds(multiple_of(i * block, block), block)
        r = xbuf[at, :].astype(F32)
        inv = lax.rsqrt(jnp.mean(r * r, axis=-1, keepdims=True) + 1e-6)
        hbuf[at, :] = (r * inv * norm).astype(BF16)
        return carry
    lax.fori_loop(0, rows // block, norm_rows, 0)

    for c in range(n_w):
        w_copy(c).wait()
        issue(c + 1 + window)
        k = c % per_mat
        for n in range(inner // COLS):
            here = slice(n * COLS, (n + 1) * COLS)
            y = jnp.dot(hbuf[:, k * k_rows:(k + 1) * k_rows], wbuf[c, :, here], preferred_element_type=F32)
            if k > 0:
                y = y + sum_ref[:, here]
            if k < per_mat - 1:
                sum_ref[:, here] = y
                continue
            y = y.astype(BF16).astype(F32).T
            if c < per_mat:
                q_ref[here, :] = y
            else:
                kn_ref[c // per_mat - 1, here, :] = y.astype(BF16)

    def chunk_out(i):
        dst = newk_hbm if i < n_chunk else newv_hbm
        return pltpu.make_async_copy(kvbuf.at[i], dst.at[pl.ds((i % n_chunk) * chunk_rows, chunk_rows)], out_sem.at[i])

    for j in range(n_chunk):
        kv_copy(j).wait()
        issue(n_w + j + 1 + window)

        def k_head(h, carry):
            at = multiple_of(h * d_head, d_head)
            q = q_ref[pl.ds(at, d_head), :]
            kn = kn_ref[0, pl.ds(at, d_head), :].reshape(sub, 16, rows)
            rows_out = []
            for tt in range(T_BLOCK):
                here = pl.ds(multiple_of(tt * inner + at, d_head), d_head)
                old = kvbuf[j, here, :].reshape(sub, 16, rows)
                hit = hit_ref[j * T_BLOCK + tt] != 0
                new = jnp.where(hit[None], kn, old)
                kvbuf[j, here, :] = new.reshape(d_head, rows)
                prod = new.reshape(d_head, rows).astype(F32) * q
                rows_out.append(jnp.sum(prod, axis=0, keepdims=True))
            score_ref[h, j * T_BLOCK:(j + 1) * T_BLOCK, :] = jnp.concatenate(rows_out, axis=0)
            return carry
        twice(n_head, k_head)
        chunk_out(j).start(priority=1)

    t_iota = lax.broadcasted_iota(jnp.int32, (t_len, rows), 0)
    causal = t_iota <= pos
    back = jnp.maximum(pos - t_iota, 0)

    def soft_head(h, carry):
        line = jnp.broadcast_to(acc_ref[pl.ds(h, 1), :], (t_len, 128))
        s = score_ref[h] + jnp.take_along_axis(line, back, axis=1)
        s = jnp.where(causal, s, NEG_FILL)
        e = jnp.exp(s - jnp.max(s, axis=0, keepdims=True))
        p = e / jnp.sum(e, axis=0, keepdims=True)
        score_ref[h] = p.astype(BF16).astype(F32)
        return carry
    lax.fori_loop(0, n_head, soft_head, 0)

    acc_ref[...] = jnp.zeros_like(acc_ref)
    for j in range(n_chunk):
        kv_copy(n_chunk + j).wait()
        issue(n_w + n_chunk + j + 1 + window)

        def v_head(h, carry):
            at = multiple_of(h * d_head, d_head)
            vn = kn_ref[1, pl.ds(at, d_head), :].reshape(sub, 16, rows)
            p = score_ref[h, j * T_BLOCK:(j + 1) * T_BLOCK, :]
            acc = acc_ref[pl.ds(at, d_head), :]
            for tt in range(T_BLOCK):
                here = pl.ds(multiple_of(tt * inner + at, d_head), d_head)
                old = kvbuf[n_chunk + j, here, :].reshape(sub, 16, rows)
                hit = hit_ref[j * T_BLOCK + tt] != 0
                new = jnp.where(hit[None], vn, old)
                kvbuf[n_chunk + j, here, :] = new.reshape(d_head, rows)
                acc = acc + new.reshape(d_head, rows).astype(F32) * p[tt:tt + 1, :]
            acc_ref[pl.ds(at, d_head), :] = acc
            return carry
        twice(n_head, v_head)
        chunk_out(n_chunk + j).start(priority=1)

    issue(len(loads))
    hbuf[:, 0:inner] = acc_ref[...].T.astype(BF16)
    mixed_copy = pltpu.make_async_copy(hbuf.at[:, pl.ds(0, inner)], mixed_hbm, part_sem)
    mixed_copy.start()
    for i in range(2 * n_chunk):
        chunk_out(i).wait()
    mixed_copy.wait()


def self_attention(x_in, norm_self, tok_pos, rel_bias, w_q, w_k, w_v, self_k, self_v):
    rows, t_len, n_head, d_head = self_k.shape
    d_model = x_in.shape[1]
    inner = n_head * d_head
    flat = (t_len * inner, rows)
    k_flat = self_k.transpose(1, 2, 3, 0).reshape(flat)
    v_flat = self_v.transpose(1, 2, 3, 0).reshape(flat)
    n_w = 3 * (d_model // inner)
    n_chunk = t_len // T_BLOCK

    def body(*refs):
        self_kernel(*refs, window=4)

    mixed, new_k, new_v = pl.pallas_call(
        body,
        out_shape=(jax.ShapeDtypeStruct((rows, inner), BF16),
                   jax.ShapeDtypeStruct(flat, BF16), jax.ShapeDtypeStruct(flat, BF16)),
        in_specs=[ANY] * 9,
        out_specs=(ANY, ANY, ANY),
        scratch_shapes=[
            pltpu.VMEM((rows, d_model), BF16),
            pltpu.VMEM((rows, d_model), BF16),
            pltpu.VMEM((n_w, inner, inner), BF16),
            pltpu.VMEM((2 * n_chunk, T_BLOCK * inner, rows), BF16),
            pltpu.VMEM((rows, inner), F32),
            pltpu.VMEM((inner, rows), F32),
            pltpu.VMEM((2, inner, rows), BF16),
            pltpu.VMEM((t_len, 16, rows), BF16),
            pltpu.VMEM((n_head, t_len, rows), F32),
            pltpu.VMEM((inner, rows), F32),
            pltpu.VMEM((d_model // 128, 128), BF16),
            pltpu.VMEM((1, d_model), F32),
            pltpu.VMEM((1, rows), jnp.int32),
            pltpu.VMEM(rel_bias.shape[::-1], F32),
            pltpu.SemaphoreType.DMA,
            pltpu.SemaphoreType.DMA((3,)),
            pltpu.SemaphoreType.DMA((n_w,)),
            pltpu.SemaphoreType.DMA((2 * n_chunk,)),
            pltpu.SemaphoreType.DMA((2 * n_chunk,)),
            pltpu.SemaphoreType.DMA,
        ],
        compiler_params=pltpu.CompilerParams(vmem_limit_bytes=66_900_000),
        cost_estimate=pl.CostEstimate(flops=3_300_000_000, bytes_accessed=95_000_000, transcendentals=131_072),
        name="self_part",
    )(x_in, norm_self.reshape(d_model // 128, 128), tok_pos.reshape(1, rows), rel_bias.T, w_q, w_k, w_v, k_flat, v_flat)

    def unflat(cache):
        return cache.reshape(t_len, n_head, d_head, rows).transpose(3, 0, 1, 2)
    return mixed, unflat(new_k), unflat(new_v)


RING = 20
WIDE = 1024
GROUP = 8
AR_CHUNKS = 4
LANES = 128


def cross_kernel(n_head, x_hbm, mixed_hbm, wo_hbm, ncross_hbm, nmlp_hbm, mask_hbm, cq_hbm, ck_hbm, cv_hbm, co_hbm, wg_hbm, wu_hbm, wd_hbm,
                 out_hbm,
                 ring, pw, gw, mixbf, pbuf, hbuf, res, xhalf, rx1, tx2, rx2, q_ref, mix_ref, p_ref, act, norm_in, nrow, mask_ref,
                 ring_sem, p_sem, g_sem, load_sem, small_sem, s1_send, s1_recv, s2_send, s2_recv, s3_send, s3_recv, out_sem):
    rows, d_model = hbuf.shape
    half = rows // 2
    part = half // 2
    depth = ring.shape[1]
    inner = q_ref.shape[1]
    d_ff = act.shape[1]
    width = d_model // AR_CHUNKS
    MESH = pl.DeviceIdType.MESH

    me = lax.axis_index("tp")
    core = lax.rem(me, 2)
    chip = me // 2
    partner = {"tp": chip * 2 + (1 - core)}
    across = {"tp": (1 - chip) * 2 + core}

    def mine(at, n):
        return pl.ds(multiple_of(core * half + at, 16), n)

    def theirs(at, n):
        return pl.ds(multiple_of((1 - core) * half + at, 16), n)

    def piece(j):
        return pl.ds(j * width, width)

    per_step = GROUP * inner // depth
    n_step = rows // GROUP
    ahead = RING // (2 * per_step)
    n_sq = pw.shape[0] // 2
    g_rows, g_cols = gw.shape[1:]
    g_cut = d_model // g_rows
    n_pair = gw.shape[0] // (2 * g_cut)

    def copy_in(src, slot, used=None):
        dst = ring.at[slot] if used is None else ring.at[slot, used]
        pltpu.make_async_copy(src, dst, ring_sem.at[slot]).start()

    def landed(slot, used=depth):
        pltpu.make_async_copy(ck_hbm.at[pl.ds(0, used)], ring.at[slot, pl.ds(0, used)], ring_sem.at[slot]).wait()

    def group_of(step):
        per_half, u = n_step // 2, step % (n_step // 2)
        return (step // per_half) * (part // GROUP) + u + (u // (part // GROUP)) * (part // GROUP)

    def kv_slot(step, value):
        return (ahead * value + step % ahead) * per_step

    def issue_kv(step, value):
        src = cv_hbm if value else ck_hbm
        for i in range(per_step):
            at = multiple_of((group_of(step) * per_step + i) * depth, depth)
            copy_in(src.at[pl.ds(at, depth)], kv_slot(step, value) + i)

    def q_copy(k):
        return pltpu.make_async_copy(cq_hbm.at[pl.ds(k * WIDE, WIDE)], pw.at[k], p_sem.at[k])

    def o_copy(i):
        return pltpu.make_async_copy(co_hbm.at[:, pl.ds(i * WIDE, WIDE)], pw.at[n_sq + i], p_sem.at[n_sq + i])

    def gu_square(i):
        src = wg_hbm if i < n_sq else wu_hbm
        return pltpu.make_async_copy(src.at[pl.ds((i % n_sq) * WIDE, WIDE), pl.ds(0, WIDE)], pw.at[i], p_sem.at[i])

    def gu_tall(pair, i):
        src = wg_hbm if i < g_cut else wu_hbm
        slot = (pair % n_pair) * 2 * g_cut + i
        return pltpu.make_async_copy(src.at[pl.ds((i % g_cut) * g_rows, g_rows), pl.ds(WIDE + pair * g_cols, g_cols)],
                                     gw.at[slot], g_sem.at[slot])

    d_cut = -(-d_ff // WIDE)
    d_narrow = 2 * WIDE // LANES

    def d_square(c, i):
        slot = (c - 2) * d_cut + i
        n = min(WIDE, d_ff - i * WIDE)
        return pltpu.make_async_copy(wd_hbm.at[pl.ds(i * WIDE, n), pl.ds(c * WIDE, WIDE)],
                                     pw.at[slot, pl.ds(0, n)], p_sem.at[slot])

    def issue_d(i):
        copy_in(wd_hbm.at[:, pl.ds(i * LANES, LANES)], i, pl.ds(0, d_ff))

    def to_partner(a, h, j, at, n):
        return pltpu.make_async_remote_copy(
            src_ref=pbuf.at[theirs(at, n), piece(j)], dst_ref=rx1.at[a % 2, pl.ds(at, n), piece(j)],
            send_sem=s1_send.at[a % 2, h, j], recv_sem=s1_recv.at[a % 2, h, j], device_id=partner, device_id_type=MESH)

    def to_across(a, h, j, at, n):
        return pltpu.make_async_remote_copy(
            src_ref=tx2.at[a % 2, pl.ds(at, n), piece(j)], dst_ref=rx2.at[a % 2, pl.ds(at, n), piece(j)],
            send_sem=s2_send.at[a % 2, h, j], recv_sem=s2_recv.at[a % 2, h, j], device_id=across, device_id_type=MESH)

    def blocks(at, n, fn):
        def body(i, carry):
            fn(multiple_of(at + i * 16, 16))
            return carry
        lax.fori_loop(0, n // 16, body, 0)

    def chip_sum(a, h, j, at, n):
        to_partner(a, h, j, at, n).wait_recv()

        def add(r):
            own = pbuf[mine(r, 16), piece(j)].astype(F32)
            tx2[a % 2, pl.ds(r, 16), piece(j)] = (own + rx1[a % 2, pl.ds(r, 16), piece(j)].astype(F32)).astype(BF16)
        blocks(at, n, add)
        to_across(a, h, j, at, n).start()

    def full_sum(a, h, j, at, n):
        to_across(a, h, j, at, n).wait_recv()

        def add(r):
            both = tx2[a % 2, pl.ds(r, 16), piece(j)].astype(F32) + rx2[a % 2, pl.ds(r, 16), piece(j)].astype(F32)
            res[pl.ds(r, 16), piece(j)] = res[pl.ds(r, 16), piece(j)] + both
        blocks(at, n, add)

    def sent(a, h, at, n):
        for j in range(AR_CHUNKS):
            to_partner(a, h, j, at, n).wait_send()
            to_across(a, h, j, at, n).wait_send()

    def rows_back(a, h, i):
        at = mine(h * part + i * 16, 16)
        return pltpu.make_async_remote_copy(
            src_ref=hbuf.at[at], dst_ref=hbuf.at[at], send_sem=s3_send.at[a % 2, h, i],
            recv_sem=s3_recv.at[a % 2, h, i], device_id=partner, device_id_type=MESH)

    def normalise(a, h):
        norm = nrow[a:a + 1, :]
        for i in range(part // 16):
            r = res[h * part + i * 16:h * part + (i + 1) * 16, :]
            inv = lax.rsqrt(jnp.mean(r * r, axis=-1, keepdims=True) + 1e-6)
            hbuf[mine(h * part + i * 16, 16), :] = (r * inv * norm).astype(BF16)
            rows_back(a, h, i).start()

    def all_rows(a, h):
        for i in range(part // 16):
            rows_back(a, h, i).wait()

    pieces = range(AR_CHUNKS)
    halves = range(2)
    n_wo = d_model // g_cols
    mixed_copy = pltpu.make_async_copy(mixed_hbm, mixbf, load_sem.at[n_wo])
    mixed_copy.start()

    def wo_copy(i):
        per_slot = g_rows // inner
        return pltpu.make_async_copy(wo_hbm.at[:, pl.ds(i * g_cols, g_cols)],
                                     gw.at[i // per_slot, pl.ds(i % per_slot * inner, inner)], load_sem.at[i])
    for i in range(n_wo):
        wo_copy(i).start()
    small = [pltpu.make_async_copy(src, dst, small_sem.at[i]) for i, (src, dst) in enumerate(
        ((x_hbm.at[mine(0, half)], xhalf), (ncross_hbm, norm_in.at[0]), (nmlp_hbm, norm_in.at[1]), (mask_hbm, mask_ref)))]
    for copy in small:
        copy.start()
    barrier = pltpu.get_barrier_semaphore()
    for other in (partner, across):
        pl.semaphore_signal(barrier, inc=1, device_id=other, device_id_type=MESH)
    pl.semaphore_wait(barrier, 2)

    for k in range(n_sq):
        q_copy(k).start()
    for step in range(ahead):
        issue_kv(step, 0)
        issue_kv(step, 1)
    for i in range(n_sq):
        o_copy(i).start()
    mixed_copy.wait()
    for i in range(n_wo):
        wo_copy(i).wait()
        per_slot = g_rows // inner
        for n in range(g_cols // COLS):
            w = gw[i // per_slot, i % per_slot * inner:(i % per_slot + 1) * inner, n * COLS:(n + 1) * COLS]
            y = jnp.dot(mixbf[...], w, preferred_element_type=F32)
            pbuf[:, i * g_cols + n * COLS:i * g_cols + (n + 1) * COLS] = y.astype(BF16)
        if (i + 1) * g_cols % width == 0:
            j = (i + 1) * g_cols // width - 1
            to_partner(0, 0, j, 0, part).start()
            if j > 0:
                chip_sum(0, 0, j - 1, 0, part)
    for j in pieces:
        to_partner(0, 1, j, part, part).start()
    chip_sum(0, 0, AR_CHUNKS - 1, 0, part)
    for j in pieces:
        chip_sum(0, 1, j, part, part)
    for copy in small:
        copy.wait()
    lay_row(nrow, 0, norm_in.at[0])
    lay_row(nrow, 1, norm_in.at[1])
    blocks(0, half, lambda r: res.__setitem__((pl.ds(r, 16), slice(None)), xhalf[pl.ds(r, 16), :].astype(F32)))

    def beside(a, b, used=depth):
        return jnp.concatenate([ring[a, 0:used, :], ring[b, 0:used, :]], axis=1)

    def both_cores(ref, h, at=slice(None)):
        return jnp.concatenate([ref[h * part:(h + 1) * part, at], ref[half + h * part:half + (h + 1) * part, at]], axis=0)

    def project_q(h):
        if h == 0:
            for k in range(n_sq):
                q_copy(k).wait()

        def block(n, carry):
            here = pl.ds(multiple_of(n * COLS, COLS), COLS)
            y = None
            for k in range(n_sq):
                z = jnp.dot(both_cores(hbuf, h, slice(k * WIDE, (k + 1) * WIDE)), pw[k, :, here], preferred_element_type=F32)
                y = z if y is None else y + z
            y = y.astype(BF16).astype(F32)
            q_ref[h * part:(h + 1) * part, here] = y[0:part]
            q_ref[half + h * part:half + (h + 1) * part, here] = y[part:]
            return carry
        twice(inner // COLS, block)

    own_head = (lax.broadcasted_iota(jnp.int32, (n_head, inner), 1) // (inner // n_head)
                == lax.broadcasted_iota(jnp.int32, (n_head, inner), 0))
    in_slot = GROUP // per_step

    def rows_of(slot, r):
        here = pl.ds(r * inner, inner)
        return jnp.concatenate([ring[slot, here, :], ring[slot + 1, here, :]], axis=1)

    def group_rows(step):
        return pl.ds(multiple_of(group_of(step) * GROUP, GROUP), GROUP)

    def score_dots(step):
        q8 = q_ref[group_rows(step), :]

        def spread(r):
            return jnp.where(own_head, jnp.broadcast_to(q8[r:r + 1, :], (n_head, inner)), 0.0).astype(BF16)
        return [jnp.dot(jnp.concatenate([spread(r), spread(r + in_slot)], axis=0), rows_of(kv_slot(step, 0), r),
                        preferred_element_type=F32) for r in range(in_slot)]

    def probabilities(step, dots):
        m8 = mask_ref[group_rows(step), :]
        scores = [s[0:n_head, 0:LANES] for s in dots] + [s[n_head:, LANES:] for s in dots]
        s = jnp.concatenate([jnp.where(m8[r:r + 1, :] != 0, scores[r], NEG_FILL) for r in range(GROUP)], axis=0)
        e = jnp.exp(s - jnp.max(s, axis=1, keepdims=True))
        p_ref[...] = (e / jnp.sum(e, axis=1, keepdims=True)).astype(BF16)

    def value_dots(step, p):
        none = jnp.zeros((n_head, LANES), BF16)
        out = []
        for r in range(in_slot):
            pa = p[r * n_head:(r + 1) * n_head, :]
            pb = p[(r + in_slot) * n_head:(r + in_slot + 1) * n_head, :]
            lhs = jnp.concatenate([jnp.concatenate([pa, none], axis=1), jnp.concatenate([none, pb], axis=1)], axis=0)
            out.append(lax.dot_general(lhs, rows_of(kv_slot(step, 1), r), (((1,), (1,)), ((), ())), preferred_element_type=F32))
        return out

    def store_mixed(step, dots):
        mixed = [y[0:n_head] for y in dots] + [y[n_head:] for y in dots]
        mix_ref[group_rows(step), :] = jnp.concatenate(
            [jnp.sum(jnp.where(own_head, y, 0.0), axis=0, keepdims=True) for y in mixed], axis=0)

    def wait_kv(step, value):
        for i in range(per_step):
            landed(kv_slot(step, value) + i)

    def refill(step, value):
        if isinstance(step, int):
            if step < n_step:
                issue_kv(step, value)
            return

        @pl.when(step < n_step)
        def _():
            issue_kv(step, value)

    def attend(lo, hi, at=None, hook=None):
        wait_kv(lo, 0)
        probabilities(lo, score_dots(lo))
        refill(lo + ahead, 0)

        def body(step, carry):
            wait_kv(step + 1, 0)
            wait_kv(step, 1)
            p = p_ref[...]
            dots = score_dots(step + 1)
            values = value_dots(step, p)
            probabilities(step + 1, dots)
            store_mixed(step, values)
            if hook is not None:
                pl.when(step == at)(hook)
            refill(step + 1 + ahead, 0)
            refill(step + ahead, 1)
            return carry
        lax.fori_loop(lo, hi - 1, body, 0)
        wait_kv(hi - 1, 1)
        store_mixed(hi - 1, value_dots(hi - 1, p_ref[...]))
        refill(hi - 1 + ahead, 1)

    def project_o(h, after):
        lhs = both_cores(mix_ref, h).astype(BF16)
        for j in pieces:
            if h == 0:
                o_copy(j).wait()
            for n in range(WIDE // COLS):
                y = jnp.dot(lhs, pw[n_sq + j, :, n * COLS:(n + 1) * COLS], preferred_element_type=F32).astype(BF16)
                here = slice(j * WIDE + n * COLS, j * WIDE + (n + 1) * COLS)
                pbuf[h * part:(h + 1) * part, here] = y[0:part]
                pbuf[half + h * part:half + (h + 1) * part, here] = y[part:]
            to_partner(1, h, j, h * part, part).start()
            if after and j > 0:
                chip_sum(1, h, j - 1, h * part, part)
        if after:
            chip_sum(1, h, AR_CHUNKS - 1, h * part, part)

    for j in pieces:
        full_sum(0, 0, j, 0, part)
    normalise(0, 0)
    all_rows(0, 0)
    project_q(0)

    def second_half():
        for j in pieces:
            full_sum(0, 1, j, part, part)
        normalise(0, 1)
    attend(0, n_step // 2, n_step // 2 - 3, second_half)
    sent(0, 0, 0, part)
    project_o(0, False)
    all_rows(0, 1)
    project_q(1)
    for j in pieces:
        chip_sum(1, 0, j, 0, part)
    attend(n_step // 2, n_step)
    for pair in range(n_pair):
        for i in range(2 * g_cut):
            gu_tall(pair, i).start()
    for i in range(n_sq):
        gu_square(i).start()
    sent(0, 1, part, part)
    project_o(1, True)
    for i in range(n_sq):
        gu_square(n_sq + i).start()
    for i in range(d_narrow):
        issue_d(i)
    for j in pieces:
        full_sum(1, 0, j, 0, part)
    normalise(1, 0)
    for j in pieces:
        full_sum(1, 1, j, part, part)
    normalise(1, 1)
    for h in halves:
        all_rows(1, h)
        sent(1, h, h * part, part)

    root = math.sqrt(2.0 / math.pi)
    def mlp_block(at, gate, up):
        u, v = None, None
        for k in range(len(gate)):
            n = d_model // len(gate)
            lhs = hbuf[:, k * n:(k + 1) * n]
            y = jnp.dot(lhs, gate[k], preferred_element_type=F32)
            z = jnp.dot(lhs, up[k], preferred_element_type=F32)
            u, v = (y, z) if u is None else (u + y, v + z)
        gelu = 0.5 * u * (1.0 + jnp.tanh(root * (u + 0.044715 * (u * u * u))))
        act[:, pl.ds(at, COLS)] = (gelu * v).astype(BF16)

    def mlp_tall(pair):
        for i in range(2 * g_cut):
            gu_tall(pair, i).wait()
        base = (pair % n_pair) * 2 * g_cut

        def block(n, carry):
            here = pl.ds(multiple_of(n * COLS, COLS), COLS)
            mlp_block(multiple_of(WIDE + pair * g_cols + n * COLS, COLS), [gw[base + i, :, here] for i in range(g_cut)],
                      [gw[base + g_cut + i, :, here] for i in range(g_cut)])
            return carry
        twice(g_cols // COLS, block)

    def mlp_square():
        for i in range(2 * n_sq):
            gu_square(i).wait()

        def block(n, carry):
            here = pl.ds(multiple_of(n * COLS, COLS), COLS)
            mlp_block(multiple_of(n * COLS, COLS), [pw[i, :, here] for i in range(n_sq)],
                      [pw[n_sq + i, :, here] for i in range(n_sq)])
            return carry
        twice(WIDE // COLS, block)

    n_tall = (d_ff - WIDE) // g_cols
    for pair in range(n_pair):
        mlp_tall(pair)
        if pair + n_pair < n_tall:
            for i in range(2 * g_cut):
                gu_tall(pair + n_pair, i).start()
    mlp_square()
    for c in (2, 3):
        for i in range(d_cut):
            d_square(c, i).start()
    for pair in range(n_pair, n_tall):
        mlp_tall(pair)

    n_last = 2 * AR_CHUNKS
    w_last = d_model // n_last
    per_piece = w_last // COLS

    def last_piece(j):
        return pl.ds(j * w_last, w_last)

    def last_to_partner(j):
        return pltpu.make_async_remote_copy(
            src_ref=pbuf.at[theirs(0, half), last_piece(j)], dst_ref=rx1.at[0, :, last_piece(j)],
            send_sem=s1_send.at[0, j // AR_CHUNKS, j % AR_CHUNKS], recv_sem=s1_recv.at[0, j // AR_CHUNKS, j % AR_CHUNKS],
            device_id=partner, device_id_type=MESH)

    def last_to_across(j):
        return pltpu.make_async_remote_copy(
            src_ref=tx2.at[0, :, last_piece(j)], dst_ref=rx2.at[0, :, last_piece(j)],
            send_sem=s2_send.at[0, j // AR_CHUNKS, j % AR_CHUNKS], recv_sem=s2_recv.at[0, j // AR_CHUNKS, j % AR_CHUNKS],
            device_id=across, device_id_type=MESH)

    def last_back(j):
        return pltpu.make_async_remote_copy(
            src_ref=hbuf.at[mine(0, half), last_piece(j)], dst_ref=out_hbm.at[mine(0, half), last_piece(j)],
            send_sem=s3_send.at[0, j // AR_CHUNKS, j % AR_CHUNKS], recv_sem=s3_recv.at[0, j // AR_CHUNKS, j % AR_CHUNKS],
            device_id=partner, device_id_type=MESH)

    def last_own(j):
        return pltpu.make_async_copy(hbuf.at[mine(0, half), last_piece(j)], out_hbm.at[mine(0, half), last_piece(j)], out_sem.at[j])

    def last_chip_sum(j):
        last_to_partner(j).wait_recv()

        def add(r):
            own = pbuf[mine(r, 16), last_piece(j)].astype(F32)
            tx2[0, pl.ds(r, 16), last_piece(j)] = (own + rx1[0, pl.ds(r, 16), last_piece(j)].astype(F32)).astype(BF16)
        blocks(0, half, add)
        last_to_across(j).start()

    for c in range(n_last):
        at = c * w_last
        block_c, in_block = at // WIDE, at % WIDE
        if block_c >= 2 and in_block == 0:
            for i in range(d_cut):
                d_square(block_c, i).wait()

        def down(i, carry):
            n = c * per_piece + i
            if block_c < 2:
                landed(2 * n, d_ff)
                landed(2 * n + 1, d_ff)
                y = jnp.dot(act[...], beside(2 * n, 2 * n + 1, d_ff), preferred_element_type=F32)
            else:
                y = None
                for k in range(d_cut):
                    row, rest = k * WIDE, min(WIDE, d_ff - k * WIDE)
                    w = pw[(block_c - 2) * d_cut + k, 0:rest, pl.ds(multiple_of(in_block + i * COLS, COLS), COLS)]
                    z = jnp.dot(act[:, row:row + rest], w, preferred_element_type=F32)
                    y = z if y is None else y + z
            pbuf[:, pl.ds(multiple_of(n * COLS, COLS), COLS)] = y.astype(BF16)
            return carry
        twice(per_piece, down)
        last_to_partner(c).start()
        if c > 1:
            last_chip_sum(c - 2)
    last_chip_sum(n_last - 2)
    last_chip_sum(n_last - 1)

    for j in range(n_last):
        last_to_across(j).wait_recv()

        def add(r):
            both = tx2[0, pl.ds(r, 16), last_piece(j)].astype(F32) + rx2[0, pl.ds(r, 16), last_piece(j)].astype(F32)
            hbuf[mine(r, 16), last_piece(j)] = (res[pl.ds(r, 16), last_piece(j)] + both).astype(BF16)
        blocks(0, half, add)
        last_back(j).start()
        last_own(j).start()
    for j in range(n_last):
        last_to_partner(j).wait_send()
        last_to_across(j).wait_send()
        last_back(j).wait()
        last_own(j).wait()


def rest_of_layer(x_in, mixed, w_o, norm_cross, norm_mlp, enc_mask, cross_k, cross_v, cross_q, cross_o, w_gate, w_up, w_down):
    rows, d_model = x_in.shape
    _, src_len, n_head, d_head = cross_k.shape
    inner = n_head * d_head
    d_ff = w_gate.shape[1]
    half = rows // 2
    flat = (rows * inner, src_len)
    k_flat = cross_k.transpose(0, 2, 3, 1).reshape(flat)
    v_flat = cross_v.transpose(0, 2, 3, 1).reshape(flat)
    square = (d_model // 128, 128)
    return pl.pallas_call(
        functools.partial(cross_kernel, n_head),
        out_shape=jax.ShapeDtypeStruct((rows, d_model), BF16),
        in_specs=[ANY] * 13,
        out_specs=ANY,
        scratch_shapes=[
            pltpu.VMEM((RING, d_model, LANES), BF16),
            pltpu.VMEM((8, WIDE, WIDE), BF16),
            pltpu.VMEM((8, d_model // 2, 512), BF16),
            pltpu.VMEM((rows, inner), BF16),
            pltpu.VMEM((rows, d_model), BF16),
            pltpu.VMEM((rows, d_model), BF16),
            pltpu.VMEM((half, d_model), F32),
            pltpu.VMEM((half, d_model), BF16),
            pltpu.VMEM((2, half, d_model), BF16),
            pltpu.VMEM((2, half, d_model), BF16),
            pltpu.VMEM((2, half, d_model), BF16),
            pltpu.VMEM((rows, inner), F32),
            pltpu.VMEM((rows, inner), F32),
            pltpu.VMEM((GROUP * n_head, src_len), BF16),
            pltpu.VMEM((rows, d_ff), BF16),
            pltpu.VMEM((2,) + square, BF16),
            pltpu.VMEM((2, d_model), F32),
            pltpu.VMEM((rows, src_len), jnp.int32),
            pltpu.SemaphoreType.DMA((RING,)),
            pltpu.SemaphoreType.DMA((8,)),
            pltpu.SemaphoreType.DMA((8,)),
            pltpu.SemaphoreType.DMA((d_model // 512 + 1,)),
            pltpu.SemaphoreType.DMA((4,)),
            pltpu.SemaphoreType.DMA((2, 2, AR_CHUNKS)),
            pltpu.SemaphoreType.DMA((2, 2, AR_CHUNKS)),
            pltpu.SemaphoreType.DMA((2, 2, AR_CHUNKS)),
            pltpu.SemaphoreType.DMA((2, 2, AR_CHUNKS)),
            pltpu.SemaphoreType.DMA((2, 2, AR_CHUNKS)),
            pltpu.SemaphoreType.DMA((2, 2, AR_CHUNKS)),
            pltpu.SemaphoreType.DMA((2 * AR_CHUNKS,)),
        ],
        compiler_params=pltpu.CompilerParams(vmem_limit_bytes=67_000_000, collective_id=0, has_side_effects=True),
        name="rest_part",
    )(x_in, mixed, w_o, norm_cross.reshape(square), norm_mlp.reshape(square), enc_mask, cross_q, k_flat, v_flat, cross_o, w_gate, w_up, w_down)


def solution(mesh):
    def local_layer(x_in, tok_pos, self_k, self_v, cross_k, cross_v, enc_mask, rel_bias, w_q, w_k, w_v, w_o, cross_q, cross_o, w_gate, w_up, w_down, norm_self, norm_cross, norm_mlp):
        mixed, new_self_k, new_self_v = self_attention(x_in, norm_self, tok_pos, rel_bias, w_q, w_k, w_v, self_k, self_v)
        x_out = rest_of_layer(x_in, mixed, w_o, norm_cross, norm_mlp, enc_mask, cross_k, cross_v, cross_q, cross_o, w_gate, w_up, w_down)
        return x_out, new_self_k, new_self_v

    cache_spec = P('dp', None, 'tp', None)
    split_cols = P(None, 'tp')
    split_rows = P('tp', None)
    in_specs = (P('dp', None), P('dp'), cache_spec, cache_spec, cache_spec, cache_spec, P('dp', None), split_cols, split_cols, split_cols, split_cols, split_rows, split_cols, split_rows, split_cols, split_cols, split_rows, P(None), P(None), P(None))
    out_specs = (P('dp', None), cache_spec, cache_spec)
    return jax.shard_map(local_layer, mesh=mesh, in_specs=in_specs, out_specs=out_specs, check_vma=False)
```

```python
import functools
import math
import jax
import jax.numpy as jnp
from jax import lax
from jax.experimental import pallas as pl
from jax.experimental.pallas import tpu as pltpu
from jax.sharding import PartitionSpec as P

BUCKET_EDGES = tuple(int(math.ceil(16.0 * 8.0 ** (bucket_step / 16.0))) for bucket_step in range(1, 16))
NEG_FILL = -1e30
F32 = jnp.float32
BF16 = jnp.bfloat16
ANY = pl.BlockSpec(memory_space=pl.ANY)
VMEM = pl.BlockSpec(memory_space=pltpu.VMEM)
COLS = 256
T_BLOCK = 8


def multiple_of(at, n):
    return at if isinstance(at, int) else pl.multiple_of(at, n)


def twice(n, body):
    def pair(i, carry):
        body(2 * i, carry)
        body(2 * i + 1, carry)
        return carry
    if n == 2:
        pair(0, 0)
    else:
        lax.fori_loop(0, n // 2, pair, 0)


def lay_row(dst, at, norm):
    values = norm[...].astype(F32)
    for i in range(values.shape[0]):
        dst[at:at + 1, i * 128:(i + 1) * 128] = values[i:i + 1, :]


def self_kernel(x_hbm, norm_hbm, pos_hbm, rel_hbm, wq_hbm, wk_hbm, wv_hbm, k_hbm, v_hbm,
                mixed_hbm, newk_hbm, newv_hbm,
                xbuf, hbuf, wbuf, kvbuf, sum_ref, q_ref, kn_ref, hit_ref, score_ref, acc_ref,
                norm_ref, nrow, pos_ref, rel_ref,
                x_sem, small_sem, w_sem, kv_sem, out_sem, part_sem, window):
    rows, d_model = xbuf.shape
    n_w = wbuf.shape[0]
    per_mat = n_w // 3
    n_chunk = kvbuf.shape[0] // 2
    n_head, t_len = score_ref.shape[0], score_ref.shape[1]
    inner = acc_ref.shape[0]
    d_head = inner // n_head
    chunk_rows = kvbuf.shape[1]
    sub = d_head // 16
    k_rows = wbuf.shape[1]

    def w_copy(c):
        src = (wq_hbm, wk_hbm, wv_hbm)[c // per_mat]
        return pltpu.make_async_copy(src.at[pl.ds((c % per_mat) * k_rows, k_rows)], wbuf.at[c], w_sem.at[c])

    def kv_copy(i):
        src = k_hbm if i < n_chunk else v_hbm
        return pltpu.make_async_copy(src.at[pl.ds((i % n_chunk) * chunk_rows, chunk_rows)], kvbuf.at[i], kv_sem.at[i])

    loads = [[w_copy(c)] for c in range(n_w)] + [[kv_copy(i)] for i in range(2 * n_chunk)]
    issued = [0]

    def issue(upto):
        while issued[0] < min(upto, len(loads)):
            for copy in loads[issued[0]]:
                copy.start()
            issued[0] += 1

    x_copy = pltpu.make_async_copy(x_hbm, xbuf, x_sem)
    x_copy.start()
    small = [pltpu.make_async_copy(src, dst, small_sem.at[i]) for i, (src, dst) in enumerate(
        ((pos_hbm, pos_ref), (rel_hbm, rel_ref), (norm_hbm, norm_ref)))]
    for copy in small:
        copy.start()
    issue(window)
    for copy in small:
        copy.wait()

    lay_row(nrow, 0, norm_ref)
    pos = pos_ref[...]
    pos16 = jnp.broadcast_to(pos, (16, rows))

    def set_hit(t, carry):
        hit_ref[t] = jnp.where(pos16 == t, 1.0, 0.0).astype(BF16)
        return carry
    lax.fori_loop(0, t_len, set_hit, 0)

    lane = lax.broadcasted_iota(jnp.int32, (n_head, 128), 1)
    bucket = jnp.full((n_head, 128), 16, jnp.int32)
    for edge in BUCKET_EDGES:
        bucket = bucket + (lane >= edge).astype(jnp.int32)
    bucket = jnp.where(lane < 16, lane, bucket)
    rel = rel_ref[...]
    table = jnp.zeros((n_head, 128), F32)
    for b in range(rel.shape[1]):
        table = jnp.where(bucket == b, rel[:, b:b + 1], table)
    acc_ref[0:n_head, :] = table

    x_copy.wait()
    block = 16
    norm = nrow[0:1, :]

    def norm_rows(i, carry):
        at = pl.ds(multiple_of(i * block, block), block)
        r = xbuf[at, :].astype(F32)
        inv = lax.rsqrt(jnp.mean(r * r, axis=-1, keepdims=True) + 1e-6)
        hbuf[at, :] = (r * inv * norm).astype(BF16)
        return carry
    lax.fori_loop(0, rows // block, norm_rows, 0)

    for c in range(n_w):
        w_copy(c).wait()
        issue(c + 1 + window)
        k = c % per_mat
        for n in range(inner // COLS):
            here = slice(n * COLS, (n + 1) * COLS)
            y = jnp.dot(hbuf[:, k * k_rows:(k + 1) * k_rows], wbuf[c, :, here], preferred_element_type=F32)
            if k > 0:
                y = y + sum_ref[:, here]
            if k < per_mat - 1:
                sum_ref[:, here] = y
                continue
            y = y.astype(BF16).astype(F32).T
            if c < per_mat:
                q_ref[here, :] = y
            else:
                kn_ref[c // per_mat - 1, here, :] = y.astype(BF16)

    def chunk_out(i):
        dst = newk_hbm if i < n_chunk else newv_hbm
        return pltpu.make_async_copy(kvbuf.at[i], dst.at[pl.ds((i % n_chunk) * chunk_rows, chunk_rows)], out_sem.at[i])

    for j in range(n_chunk):
        kv_copy(j).wait()
        issue(n_w + j + 1 + window)

        def k_head(h, carry):
            at = multiple_of(h * d_head, d_head)
            q = q_ref[pl.ds(at, d_head), :]
            kn = kn_ref[0, pl.ds(at, d_head), :].reshape(sub, 16, rows)
            rows_out = []
            for tt in range(T_BLOCK):
                here = pl.ds(multiple_of(tt * inner + at, d_head), d_head)
                old = kvbuf[j, here, :].reshape(sub, 16, rows)
                hit = hit_ref[j * T_BLOCK + tt] != 0
                new = jnp.where(hit[None], kn, old)
                kvbuf[j, here, :] = new.reshape(d_head, rows)
                prod = new.reshape(d_head, rows).astype(F32) * q
                rows_out.append(jnp.sum(prod, axis=0, keepdims=True))
            score_ref[h, j * T_BLOCK:(j + 1) * T_BLOCK, :] = jnp.concatenate(rows_out, axis=0)
            return carry
        twice(n_head, k_head)
        chunk_out(j).start(priority=1)

    t_iota = lax.broadcasted_iota(jnp.int32, (t_len, rows), 0)
    causal = t_iota <= pos
    back = jnp.maximum(pos - t_iota, 0)

    def soft_head(h, carry):
        line = jnp.broadcast_to(acc_ref[pl.ds(h, 1), :], (t_len, 128))
        s = score_ref[h] + jnp.take_along_axis(line, back, axis=1)
        s = jnp.where(causal, s, NEG_FILL)
        e = jnp.exp(s - jnp.max(s, axis=0, keepdims=True))
        p = e / jnp.sum(e, axis=0, keepdims=True)
        score_ref[h] = p.astype(BF16).astype(F32)
        return carry
    lax.fori_loop(0, n_head, soft_head, 0)

    acc_ref[...] = jnp.zeros_like(acc_ref)
    for j in range(n_chunk):
        kv_copy(n_chunk + j).wait()
        issue(n_w + n_chunk + j + 1 + window)

        def v_head(h, carry):
            at = multiple_of(h * d_head, d_head)
            vn = kn_ref[1, pl.ds(at, d_head), :].reshape(sub, 16, rows)
            p = score_ref[h, j * T_BLOCK:(j + 1) * T_BLOCK, :]
            acc = acc_ref[pl.ds(at, d_head), :]
            for tt in range(T_BLOCK):
                here = pl.ds(multiple_of(tt * inner + at, d_head), d_head)
                old = kvbuf[n_chunk + j, here, :].reshape(sub, 16, rows)
                hit = hit_ref[j * T_BLOCK + tt] != 0
                new = jnp.where(hit[None], vn, old)
                kvbuf[n_chunk + j, here, :] = new.reshape(d_head, rows)
                acc = acc + new.reshape(d_head, rows).astype(F32) * p[tt:tt + 1, :]
            acc_ref[pl.ds(at, d_head), :] = acc
            return carry
        twice(n_head, v_head)
        chunk_out(n_chunk + j).start(priority=1)

    issue(len(loads))
    hbuf[:, 0:inner] = acc_ref[...].T.astype(BF16)
    mixed_copy = pltpu.make_async_copy(hbuf.at[:, pl.ds(0, inner)], mixed_hbm, part_sem)
    mixed_copy.start()
    for i in range(2 * n_chunk):
        chunk_out(i).wait()
    mixed_copy.wait()


def self_attention(x_in, norm_self, tok_pos, rel_bias, w_q, w_k, w_v, self_k, self_v):
    rows, t_len, n_head, d_head = self_k.shape
    d_model = x_in.shape[1]
    inner = n_head * d_head
    flat = (t_len * inner, rows)
    k_flat = self_k.transpose(1, 2, 3, 0).reshape(flat)
    v_flat = self_v.transpose(1, 2, 3, 0).reshape(flat)
    n_w = 3 * (d_model // inner)
    n_chunk = t_len // T_BLOCK

    def body(*refs):
        self_kernel(*refs, window=5)

    mixed, new_k, new_v = pl.pallas_call(
        body,
        out_shape=(jax.ShapeDtypeStruct((rows, inner), BF16),
                   jax.ShapeDtypeStruct(flat, BF16), jax.ShapeDtypeStruct(flat, BF16)),
        in_specs=[ANY] * 9,
        out_specs=(ANY, ANY, ANY),
        scratch_shapes=[
            pltpu.VMEM((rows, d_model), BF16),
            pltpu.VMEM((rows, d_model), BF16),
            pltpu.VMEM((n_w, inner, inner), BF16),
            pltpu.VMEM((2 * n_chunk, T_BLOCK * inner, rows), BF16),
            pltpu.VMEM((rows, inner), F32),
            pltpu.VMEM((inner, rows), F32),
            pltpu.VMEM((2, inner, rows), BF16),
            pltpu.VMEM((t_len, 16, rows), BF16),
            pltpu.VMEM((n_head, t_len, rows), F32),
            pltpu.VMEM((inner, rows), F32),
            pltpu.VMEM((d_model // 128, 128), BF16),
            pltpu.VMEM((1, d_model), F32),
            pltpu.VMEM((1, rows), jnp.int32),
            pltpu.VMEM(rel_bias.shape[::-1], F32),
            pltpu.SemaphoreType.DMA,
            pltpu.SemaphoreType.DMA((3,)),
            pltpu.SemaphoreType.DMA((n_w,)),
            pltpu.SemaphoreType.DMA((2 * n_chunk,)),
            pltpu.SemaphoreType.DMA((2 * n_chunk,)),
            pltpu.SemaphoreType.DMA,
        ],
        compiler_params=pltpu.CompilerParams(vmem_limit_bytes=66_900_000),
        cost_estimate=pl.CostEstimate(flops=3_300_000_000, bytes_accessed=95_000_000, transcendentals=131_072),
        name="self_part",
    )(x_in, norm_self.reshape(d_model // 128, 128), tok_pos.reshape(1, rows), rel_bias.T, w_q, w_k, w_v, k_flat, v_flat)

    def unflat(cache):
        return cache.reshape(t_len, n_head, d_head, rows).transpose(3, 0, 1, 2)
    return mixed, unflat(new_k), unflat(new_v)


RING = 20
WIDE = 1024
GROUP = 8
AR_CHUNKS = 4
LANES = 128


def cross_kernel(n_head, x_hbm, mixed_hbm, wo_hbm, ncross_hbm, nmlp_hbm, mask_hbm, cq_hbm, ck_hbm, cv_hbm, co_hbm, wg_hbm, wu_hbm, wd_hbm,
                 out_hbm,
                 ring, pw, gw, mixbf, pbuf, hbuf, res, xhalf, rx1, tx2, rx2, q_ref, mix_ref, p_ref, act, norm_in, nrow, mask_ref,
                 ring_sem, p_sem, g_sem, load_sem, small_sem, s1_send, s1_recv, s2_send, s2_recv, s3_send, s3_recv, out_sem):
    rows, d_model = hbuf.shape
    half = rows // 2
    part = half // 2
    depth = ring.shape[1]
    inner = q_ref.shape[1]
    d_ff = act.shape[1]
    width = d_model // AR_CHUNKS
    MESH = pl.DeviceIdType.MESH

    me = lax.axis_index("tp")
    core = lax.rem(me, 2)
    chip = me // 2
    partner = {"tp": chip * 2 + (1 - core)}
    across = {"tp": (1 - chip) * 2 + core}

    def mine(at, n):
        return pl.ds(multiple_of(core * half + at, 16), n)

    def theirs(at, n):
        return pl.ds(multiple_of((1 - core) * half + at, 16), n)

    def piece(j):
        return pl.ds(j * width, width)

    per_step = GROUP * inner // depth
    n_step = rows // GROUP
    ahead = RING // (2 * per_step)
    n_sq = pw.shape[0] // 2
    g_rows, g_cols = gw.shape[1:]
    g_cut = d_model // g_rows
    n_pair = gw.shape[0] // (2 * g_cut)

    def copy_in(src, slot, used=None):
        dst = ring.at[slot] if used is None else ring.at[slot, used]
        pltpu.make_async_copy(src, dst, ring_sem.at[slot]).start()

    def landed(slot, used=depth):
        pltpu.make_async_copy(ck_hbm.at[pl.ds(0, used)], ring.at[slot, pl.ds(0, used)], ring_sem.at[slot]).wait()

    def group_of(step):
        per_half, u = n_step // 2, step % (n_step // 2)
        return (step // per_half) * (part // GROUP) + u + (u // (part // GROUP)) * (part // GROUP)

    def kv_slot(step, value):
        return (ahead * value + step % ahead) * per_step

    def issue_kv(step, value):
        src = cv_hbm if value else ck_hbm
        for i in range(per_step):
            at = multiple_of((group_of(step) * per_step + i) * depth, depth)
            copy_in(src.at[pl.ds(at, depth)], kv_slot(step, value) + i)

    def q_copy(k):
        return pltpu.make_async_copy(cq_hbm.at[pl.ds(k * WIDE, WIDE)], pw.at[k], p_sem.at[k])

    def o_copy(i):
        return pltpu.make_async_copy(co_hbm.at[:, pl.ds(i * WIDE, WIDE)], pw.at[n_sq + i], p_sem.at[n_sq + i])

    def gu_square(i):
        src = wg_hbm if i < n_sq else wu_hbm
        return pltpu.make_async_copy(src.at[pl.ds((i % n_sq) * WIDE, WIDE), pl.ds(0, WIDE)], pw.at[i], p_sem.at[i])

    def gu_tall(pair, i):
        src = wg_hbm if i < g_cut else wu_hbm
        slot = (pair % n_pair) * 2 * g_cut + i
        return pltpu.make_async_copy(src.at[pl.ds((i % g_cut) * g_rows, g_rows), pl.ds(WIDE + pair * g_cols, g_cols)],
                                     gw.at[slot], g_sem.at[slot])

    d_cut = -(-d_ff // WIDE)
    d_narrow = 2 * WIDE // LANES

    def d_square(c, i):
        slot = (c - 2) * d_cut + i
        n = min(WIDE, d_ff - i * WIDE)
        return pltpu.make_async_copy(wd_hbm.at[pl.ds(i * WIDE, n), pl.ds(c * WIDE, WIDE)],
                                     pw.at[slot, pl.ds(0, n)], p_sem.at[slot])

    def issue_d(i):
        copy_in(wd_hbm.at[:, pl.ds(i * LANES, LANES)], i, pl.ds(0, d_ff))

    def to_partner(a, h, j, at, n):
        return pltpu.make_async_remote_copy(
            src_ref=pbuf.at[theirs(at, n), piece(j)], dst_ref=rx1.at[a % 2, pl.ds(at, n), piece(j)],
            send_sem=s1_send.at[a % 2, h, j], recv_sem=s1_recv.at[a % 2, h, j], device_id=partner, device_id_type=MESH)

    def to_across(a, h, j, at, n):
        return pltpu.make_async_remote_copy(
            src_ref=tx2.at[a % 2, pl.ds(at, n), piece(j)], dst_ref=rx2.at[a % 2, pl.ds(at, n), piece(j)],
            send_sem=s2_send.at[a % 2, h, j], recv_sem=s2_recv.at[a % 2, h, j], device_id=across, device_id_type=MESH)

    def blocks(at, n, fn):
        def body(i, carry):
            fn(multiple_of(at + i * 16, 16))
            return carry
        lax.fori_loop(0, n // 16, body, 0)

    def chip_sum(a, h, j, at, n):
        to_partner(a, h, j, at, n).wait_recv()

        def add(r):
            own = pbuf[mine(r, 16), piece(j)].astype(F32)
            tx2[a % 2, pl.ds(r, 16), piece(j)] = (own + rx1[a % 2, pl.ds(r, 16), piece(j)].astype(F32)).astype(BF16)
        blocks(at, n, add)
        to_across(a, h, j, at, n).start()

    def full_sum(a, h, j, at, n):
        to_across(a, h, j, at, n).wait_recv()

        def add(r):
            both = tx2[a % 2, pl.ds(r, 16), piece(j)].astype(F32) + rx2[a % 2, pl.ds(r, 16), piece(j)].astype(F32)
            res[pl.ds(r, 16), piece(j)] = res[pl.ds(r, 16), piece(j)] + both
        blocks(at, n, add)

    def sent(a, h, at, n):
        for j in range(AR_CHUNKS):
            to_partner(a, h, j, at, n).wait_send()
            to_across(a, h, j, at, n).wait_send()

    def rows_back(a, h, i):
        at = mine(h * part + i * 16, 16)
        return pltpu.make_async_remote_copy(
            src_ref=hbuf.at[at], dst_ref=hbuf.at[at], send_sem=s3_send.at[a % 2, h, i],
            recv_sem=s3_recv.at[a % 2, h, i], device_id=partner, device_id_type=MESH)

    def normalise(a, h):
        norm = nrow[a:a + 1, :]
        for i in range(part // 16):
            r = res[h * part + i * 16:h * part + (i + 1) * 16, :]
            inv = lax.rsqrt(jnp.mean(r * r, axis=-1, keepdims=True) + 1e-6)
            hbuf[mine(h * part + i * 16, 16), :] = (r * inv * norm).astype(BF16)
            rows_back(a, h, i).start()

    def all_rows(a, h):
        for i in range(part // 16):
            rows_back(a, h, i).wait()

    pieces = range(AR_CHUNKS)
    halves = range(2)
    n_wo = d_model // g_cols
    mixed_copy = pltpu.make_async_copy(mixed_hbm, mixbf, load_sem.at[n_wo])
    mixed_copy.start()

    def wo_copy(i):
        per_slot = g_rows // inner
        return pltpu.make_async_copy(wo_hbm.at[:, pl.ds(i * g_cols, g_cols)],
                                     gw.at[i // per_slot, pl.ds(i % per_slot * inner, inner)], load_sem.at[i])
    for i in range(n_wo):
        wo_copy(i).start()
    small = [pltpu.make_async_copy(src, dst, small_sem.at[i]) for i, (src, dst) in enumerate(
        ((x_hbm.at[mine(0, half)], xhalf), (ncross_hbm, norm_in.at[0]), (nmlp_hbm, norm_in.at[1]), (mask_hbm, mask_ref)))]
    for copy in small:
        copy.start()
    barrier = pltpu.get_barrier_semaphore()
    for other in (partner, across):
        pl.semaphore_signal(barrier, inc=1, device_id=other, device_id_type=MESH)
    pl.semaphore_wait(barrier, 2)

    for k in range(n_sq):
        q_copy(k).start()
    for step in range(ahead):
        issue_kv(step, 0)
        issue_kv(step, 1)
    for i in range(n_sq):
        o_copy(i).start()
    mixed_copy.wait()
    for i in range(n_wo):
        wo_copy(i).wait()
        per_slot = g_rows // inner
        for n in range(g_cols // COLS):
            w = gw[i // per_slot, i % per_slot * inner:(i % per_slot + 1) * inner, n * COLS:(n + 1) * COLS]
            y = jnp.dot(mixbf[...], w, preferred_element_type=F32)
            pbuf[:, i * g_cols + n * COLS:i * g_cols + (n + 1) * COLS] = y.astype(BF16)
        if (i + 1) * g_cols % width == 0:
            j = (i + 1) * g_cols // width - 1
            to_partner(0, 0, j, 0, part).start()
            if j > 0:
                chip_sum(0, 0, j - 1, 0, part)
    for j in pieces:
        to_partner(0, 1, j, part, part).start()
    for i in range(2 * g_cut):
        gu_tall(0, i).start()
    chip_sum(0, 0, AR_CHUNKS - 1, 0, part)
    for j in pieces:
        chip_sum(0, 1, j, part, part)
    for copy in small:
        copy.wait()
    lay_row(nrow, 0, norm_in.at[0])
    lay_row(nrow, 1, norm_in.at[1])
    blocks(0, half, lambda r: res.__setitem__((pl.ds(r, 16), slice(None)), xhalf[pl.ds(r, 16), :].astype(F32)))

    def beside(a, b, used=depth):
        return jnp.concatenate([ring[a, 0:used, :], ring[b, 0:used, :]], axis=1)

    def both_cores(ref, h, at=slice(None)):
        return jnp.concatenate([ref[h * part:(h + 1) * part, at], ref[half + h * part:half + (h + 1) * part, at]], axis=0)

    def project_q(h):
        if h == 0:
            for k in range(n_sq):
                q_copy(k).wait()

        def block(n, carry):
            here = pl.ds(multiple_of(n * COLS, COLS), COLS)
            y = None
            for k in range(n_sq):
                z = jnp.dot(both_cores(hbuf, h, slice(k * WIDE, (k + 1) * WIDE)), pw[k, :, here], preferred_element_type=F32)
                y = z if y is None else y + z
            y = y.astype(BF16).astype(F32)
            q_ref[h * part:(h + 1) * part, here] = y[0:part]
            q_ref[half + h * part:half + (h + 1) * part, here] = y[part:]
            return carry
        twice(inner // COLS, block)

    own_head = (lax.broadcasted_iota(jnp.int32, (n_head, inner), 1) // (inner // n_head)
                == lax.broadcasted_iota(jnp.int32, (n_head, inner), 0))
    in_slot = GROUP // per_step

    def rows_of(slot, r):
        here = pl.ds(r * inner, inner)
        return jnp.concatenate([ring[slot, here, :], ring[slot + 1, here, :]], axis=1)

    def group_rows(step):
        return pl.ds(multiple_of(group_of(step) * GROUP, GROUP), GROUP)

    def score_dots(step):
        q8 = q_ref[group_rows(step), :]

        def spread(r):
            return jnp.where(own_head, jnp.broadcast_to(q8[r:r + 1, :], (n_head, inner)), 0.0).astype(BF16)
        return [jnp.dot(jnp.concatenate([spread(r), spread(r + in_slot)], axis=0), rows_of(kv_slot(step, 0), r),
                        preferred_element_type=F32) for r in range(in_slot)]

    def probabilities(step, dots):
        m8 = mask_ref[group_rows(step), :]
        scores = [s[0:n_head, 0:LANES] for s in dots] + [s[n_head:, LANES:] for s in dots]
        s = jnp.concatenate([jnp.where(m8[r:r + 1, :] != 0, scores[r], NEG_FILL) for r in range(GROUP)], axis=0)
        e = jnp.exp(s - jnp.max(s, axis=1, keepdims=True))
        p_ref[...] = (e / jnp.sum(e, axis=1, keepdims=True)).astype(BF16)

    def value_dots(step, p):
        none = jnp.zeros((n_head, LANES), BF16)
        out = []
        for r in range(in_slot):
            pa = p[r * n_head:(r + 1) * n_head, :]
            pb = p[(r + in_slot) * n_head:(r + in_slot + 1) * n_head, :]
            lhs = jnp.concatenate([jnp.concatenate([pa, none], axis=1), jnp.concatenate([none, pb], axis=1)], axis=0)
            out.append(lax.dot_general(lhs, rows_of(kv_slot(step, 1), r), (((1,), (1,)), ((), ())), preferred_element_type=F32))
        return out

    def store_mixed(step, dots):
        mixed = [y[0:n_head] for y in dots] + [y[n_head:] for y in dots]
        mix_ref[group_rows(step), :] = jnp.concatenate(
            [jnp.sum(jnp.where(own_head, y, 0.0), axis=0, keepdims=True) for y in mixed], axis=0)

    def wait_kv(step, value):
        for i in range(per_step):
            landed(kv_slot(step, value) + i)

    def refill(step, value):
        if isinstance(step, int):
            if step < n_step:
                issue_kv(step, value)
            return

        @pl.when(step < n_step)
        def _():
            issue_kv(step, value)

    def attend(lo, hi, at=None, hook=None):
        wait_kv(lo, 0)
        probabilities(lo, score_dots(lo))
        refill(lo + ahead, 0)

        def body(step, carry):
            wait_kv(step + 1, 0)
            wait_kv(step, 1)
            p = p_ref[...]
            dots = score_dots(step + 1)
            values = value_dots(step, p)
            probabilities(step + 1, dots)
            store_mixed(step, values)
            if hook is not None:
                pl.when(step == at)(hook)
            refill(step + 1 + ahead, 0)
            refill(step + ahead, 1)
            return carry
        lax.fori_loop(lo, hi - 1, body, 0)
        wait_kv(hi - 1, 1)
        store_mixed(hi - 1, value_dots(hi - 1, p_ref[...]))
        refill(hi - 1 + ahead, 1)

    def project_o(h, after):
        lhs = both_cores(mix_ref, h).astype(BF16)
        for j in pieces:
            if h == 0:
                o_copy(j).wait()
            for n in range(WIDE // COLS):
                y = jnp.dot(lhs, pw[n_sq + j, :, n * COLS:(n + 1) * COLS], preferred_element_type=F32).astype(BF16)
                here = slice(j * WIDE + n * COLS, j * WIDE + (n + 1) * COLS)
                pbuf[h * part:(h + 1) * part, here] = y[0:part]
                pbuf[half + h * part:half + (h + 1) * part, here] = y[part:]
            to_partner(1, h, j, h * part, part).start()
            if after and j > 0:
                chip_sum(1, h, j - 1, h * part, part)
        if after:
            chip_sum(1, h, AR_CHUNKS - 1, h * part, part)

    for j in pieces:
        full_sum(0, 0, j, 0, part)
    normalise(0, 0)
    all_rows(0, 0)
    project_q(0)

    def second_half():
        for j in pieces:
            full_sum(0, 1, j, part, part)
        normalise(0, 1)
    attend(0, n_step // 2, n_step // 2 - 3, second_half)
    sent(0, 0, 0, part)
    project_o(0, False)
    all_rows(0, 1)
    project_q(1)
    for j in pieces:
        chip_sum(1, 0, j, 0, part)

    def start_mlp():
        for pair in range(1, n_pair):
            for i in range(2 * g_cut):
                gu_tall(pair, i).start()
        for i in range(n_sq):
            gu_square(i).start()
    attend(n_step // 2, n_step, n_step - ahead, start_mlp)
    sent(0, 1, part, part)
    project_o(1, True)
    for i in range(n_sq):
        gu_square(n_sq + i).start()
    for i in range(d_narrow):
        issue_d(i)
    for j in pieces:
        full_sum(1, 0, j, 0, part)
    normalise(1, 0)
    for j in pieces:
        full_sum(1, 1, j, part, part)
    normalise(1, 1)
    for h in halves:
        all_rows(1, h)
        sent(1, h, h * part, part)

    root = math.sqrt(2.0 / math.pi)
    def mlp_block(at, gate, up):
        u, v = None, None
        for k in range(len(gate)):
            n = d_model // len(gate)
            lhs = hbuf[:, k * n:(k + 1) * n]
            y = jnp.dot(lhs, gate[k], preferred_element_type=F32)
            z = jnp.dot(lhs, up[k], preferred_element_type=F32)
            u, v = (y, z) if u is None else (u + y, v + z)
        gelu = 0.5 * u * (1.0 + jnp.tanh(root * (u + 0.044715 * (u * u * u))))
        act[:, pl.ds(at, COLS)] = (gelu * v).astype(BF16)

    def mlp_tall(pair):
        for i in range(2 * g_cut):
            gu_tall(pair, i).wait()
        base = (pair % n_pair) * 2 * g_cut

        def block(n, carry):
            here = pl.ds(multiple_of(n * COLS, COLS), COLS)
            mlp_block(multiple_of(WIDE + pair * g_cols + n * COLS, COLS), [gw[base + i, :, here] for i in range(g_cut)],
                      [gw[base + g_cut + i, :, here] for i in range(g_cut)])
            return carry
        twice(g_cols // COLS, block)

    def mlp_square():
        for i in range(2 * n_sq):
            gu_square(i).wait()

        def block(n, carry):
            here = pl.ds(multiple_of(n * COLS, COLS), COLS)
            mlp_block(multiple_of(n * COLS, COLS), [pw[i, :, here] for i in range(n_sq)],
                      [pw[n_sq + i, :, here] for i in range(n_sq)])
            return carry
        twice(WIDE // COLS, block)

    n_tall = (d_ff - WIDE) // g_cols
    for pair in range(n_pair):
        mlp_tall(pair)
        if pair + n_pair < n_tall:
            for i in range(2 * g_cut):
                gu_tall(pair + n_pair, i).start()
    mlp_square()
    for c in (2, 3):
        for i in range(d_cut):
            d_square(c, i).start()
    for pair in range(n_pair, n_tall):
        mlp_tall(pair)

    n_last = 2 * AR_CHUNKS
    w_last = d_model // n_last
    per_piece = w_last // COLS

    def last_piece(j):
        return pl.ds(j * w_last, w_last)

    def last_to_partner(j):
        return pltpu.make_async_remote_copy(
            src_ref=pbuf.at[theirs(0, half), last_piece(j)], dst_ref=rx1.at[0, :, last_piece(j)],
            send_sem=s1_send.at[0, j // AR_CHUNKS, j % AR_CHUNKS], recv_sem=s1_recv.at[0, j // AR_CHUNKS, j % AR_CHUNKS],
            device_id=partner, device_id_type=MESH)

    def last_to_across(j):
        return pltpu.make_async_remote_copy(
            src_ref=tx2.at[0, :, last_piece(j)], dst_ref=rx2.at[0, :, last_piece(j)],
            send_sem=s2_send.at[0, j // AR_CHUNKS, j % AR_CHUNKS], recv_sem=s2_recv.at[0, j // AR_CHUNKS, j % AR_CHUNKS],
            device_id=across, device_id_type=MESH)

    def last_back(j):
        return pltpu.make_async_remote_copy(
            src_ref=hbuf.at[mine(0, half), last_piece(j)], dst_ref=out_hbm.at[mine(0, half), last_piece(j)],
            send_sem=s3_send.at[0, j // AR_CHUNKS, j % AR_CHUNKS], recv_sem=s3_recv.at[0, j // AR_CHUNKS, j % AR_CHUNKS],
            device_id=partner, device_id_type=MESH)

    def last_own(j):
        return pltpu.make_async_copy(hbuf.at[mine(0, half), last_piece(j)], out_hbm.at[mine(0, half), last_piece(j)], out_sem.at[j])

    def last_chip_sum(j):
        last_to_partner(j).wait_recv()

        def add(r):
            own = pbuf[mine(r, 16), last_piece(j)].astype(F32)
            tx2[0, pl.ds(r, 16), last_piece(j)] = (own + rx1[0, pl.ds(r, 16), last_piece(j)].astype(F32)).astype(BF16)
        blocks(0, half, add)
        last_to_across(j).start()

    for c in range(n_last):
        at = c * w_last
        block_c, in_block = at // WIDE, at % WIDE
        if block_c >= 2 and in_block == 0:
            for i in range(d_cut):
                d_square(block_c, i).wait()

        def down(i, carry):
            n = c * per_piece + i
            if block_c < 2:
                landed(2 * n, d_ff)
                landed(2 * n + 1, d_ff)
                y = jnp.dot(act[...], beside(2 * n, 2 * n + 1, d_ff), preferred_element_type=F32)
            else:
                y = None
                for k in range(d_cut):
                    row, rest = k * WIDE, min(WIDE, d_ff - k * WIDE)
                    w = pw[(block_c - 2) * d_cut + k, 0:rest, pl.ds(multiple_of(in_block + i * COLS, COLS), COLS)]
                    z = jnp.dot(act[:, row:row + rest], w, preferred_element_type=F32)
                    y = z if y is None else y + z
            pbuf[:, pl.ds(multiple_of(n * COLS, COLS), COLS)] = y.astype(BF16)
            return carry
        twice(per_piece, down)
        last_to_partner(c).start()
        if c > 1:
            last_chip_sum(c - 2)
    last_chip_sum(n_last - 2)
    last_chip_sum(n_last - 1)

    for j in range(n_last):
        last_to_across(j).wait_recv()

        def add(r):
            both = tx2[0, pl.ds(r, 16), last_piece(j)].astype(F32) + rx2[0, pl.ds(r, 16), last_piece(j)].astype(F32)
            hbuf[mine(r, 16), last_piece(j)] = (res[pl.ds(r, 16), last_piece(j)] + both).astype(BF16)
        blocks(0, half, add)
        last_back(j).start()
        last_own(j).start()
    for j in range(n_last):
        last_to_partner(j).wait_send()
        last_to_across(j).wait_send()
        last_back(j).wait()
        last_own(j).wait()


def rest_of_layer(x_in, mixed, w_o, norm_cross, norm_mlp, enc_mask, cross_k, cross_v, cross_q, cross_o, w_gate, w_up, w_down):
    rows, d_model = x_in.shape
    _, src_len, n_head, d_head = cross_k.shape
    inner = n_head * d_head
    d_ff = w_gate.shape[1]
    half = rows // 2
    flat = (rows * inner, src_len)
    k_flat = cross_k.transpose(0, 2, 3, 1).reshape(flat)
    v_flat = cross_v.transpose(0, 2, 3, 1).reshape(flat)
    square = (d_model // 128, 128)
    return pl.pallas_call(
        functools.partial(cross_kernel, n_head),
        out_shape=jax.ShapeDtypeStruct((rows, d_model), BF16),
        in_specs=[ANY] * 13,
        out_specs=ANY,
        scratch_shapes=[
            pltpu.VMEM((RING, d_model, LANES), BF16),
            pltpu.VMEM((8, WIDE, WIDE), BF16),
            pltpu.VMEM((8, d_model // 2, 512), BF16),
            pltpu.VMEM((rows, inner), BF16),
            pltpu.VMEM((rows, d_model), BF16),
            pltpu.VMEM((rows, d_model), BF16),
            pltpu.VMEM((half, d_model), F32),
            pltpu.VMEM((half, d_model), BF16),
            pltpu.VMEM((2, half, d_model), BF16),
            pltpu.VMEM((2, half, d_model), BF16),
            pltpu.VMEM((2, half, d_model), BF16),
            pltpu.VMEM((rows, inner), F32),
            pltpu.VMEM((rows, inner), F32),
            pltpu.VMEM((GROUP * n_head, src_len), BF16),
            pltpu.VMEM((rows, d_ff), BF16),
            pltpu.VMEM((2,) + square, BF16),
            pltpu.VMEM((2, d_model), F32),
            pltpu.VMEM((rows, src_len), jnp.int32),
            pltpu.SemaphoreType.DMA((RING,)),
            pltpu.SemaphoreType.DMA((8,)),
            pltpu.SemaphoreType.DMA((8,)),
            pltpu.SemaphoreType.DMA((d_model // 512 + 1,)),
            pltpu.SemaphoreType.DMA((4,)),
            pltpu.SemaphoreType.DMA((2, 2, AR_CHUNKS)),
            pltpu.SemaphoreType.DMA((2, 2, AR_CHUNKS)),
            pltpu.SemaphoreType.DMA((2, 2, AR_CHUNKS)),
            pltpu.SemaphoreType.DMA((2, 2, AR_CHUNKS)),
            pltpu.SemaphoreType.DMA((2, 2, AR_CHUNKS)),
            pltpu.SemaphoreType.DMA((2, 2, AR_CHUNKS)),
            pltpu.SemaphoreType.DMA((2 * AR_CHUNKS,)),
        ],
        compiler_params=pltpu.CompilerParams(vmem_limit_bytes=67_000_000, collective_id=0, has_side_effects=True),
        name="rest_part",
    )(x_in, mixed, w_o, norm_cross.reshape(square), norm_mlp.reshape(square), enc_mask, cross_q, k_flat, v_flat, cross_o, w_gate, w_up, w_down)


def solution(mesh):
    def local_layer(x_in, tok_pos, self_k, self_v, cross_k, cross_v, enc_mask, rel_bias, w_q, w_k, w_v, w_o, cross_q, cross_o, w_gate, w_up, w_down, norm_self, norm_cross, norm_mlp):
        mixed, new_self_k, new_self_v = self_attention(x_in, norm_self, tok_pos, rel_bias, w_q, w_k, w_v, self_k, self_v)
        x_out = rest_of_layer(x_in, mixed, w_o, norm_cross, norm_mlp, enc_mask, cross_k, cross_v, cross_q, cross_o, w_gate, w_up, w_down)
        return x_out, new_self_k, new_self_v

    cache_spec = P('dp', None, 'tp', None)
    split_cols = P(None, 'tp')
    split_rows = P('tp', None)
    in_specs = (P('dp', None), P('dp'), cache_spec, cache_spec, cache_spec, cache_spec, P('dp', None), split_cols, split_cols, split_cols, split_cols, split_rows, split_cols, split_rows, split_cols, split_cols, split_rows, P(None), P(None), P(None))
    out_specs = (P('dp', None), cache_spec, cache_spec)
    return jax.shard_map(local_layer, mesh=mesh, in_specs=in_specs, out_specs=out_specs, check_vma=False)
```
